128 devices in a mesh: seq: 32 (over y, z, core), batch: 4 (over x).
Axes of the slice: x: 4, y: 4, z: 4, core: 2. Of those that a mesh axis runs over, the one named last changes fastest.
Arguments:
- queries: bfloat16 [4, 4096, 4096], P('batch', 'seq'), may hold values from -130 to 130
- keys: bfloat16 [4, 4096, 1024], P('batch', 'seq'), may hold values from -4 to 4
- values: bfloat16 [4, 4096, 1024], P('batch', 'seq'), may hold values from -4 to 4
- lengths: int32 [4], P('batch'), may hold values from 2048 to 4096
- block_pos: int32 [4, 32], P('batch'), may hold values from 0 to 31, each once within a row
- w_in: bfloat16 [6144, 1024], replicated, may hold values from -0.078125 to 0.078125
- b_in: float32 [1024], replicated, may hold values from -3 to 3
- output_weight: bfloat16 [1024, 8], replicated, may hold values from -0.1875 to 0.1875
- output_bias: float32 [8], replicated, may hold values from 1 to 2
Outputs:
- grad_w_in: float32 [6144, 1024], P(('seq', 'batch'))
- grad_b_in: float32 [1024], replicated
- output_weight_gradient: float32 [1024, 8], replicated
- output_bias_gradient: float32 [8], replicated
The draws below stay inside these ranges and needn't reach their ends.
Inputs may be any that keep to these rules, and one draw needn't show every extreme that they name: Each row of block_pos names every block 0 to 31 once.
All inputs are finite; a program needn't handle non-finite values.
Results may differ from the reference program's by a relative error of at most 0.0017.
The reference program's roundings to bfloat16 on the way (of `features`, `act`, `resid` and `delta`) count: a program that leaves them out, or rounds other values in their place, can miss the bound.
Values may be sent and summed in bfloat16 or wider, within the bound.
A program may use at most 128 MiB of HBM per device.

```python
import math
import jax
import jax.numpy as jnp
from jax import lax

QUERY_HEADS = 32
KEY_VALUE_HEADS = 8
HEAD_DIMENSION = 128
HIDDEN_UNITS = 1024
SEQ_DEV = 128
KD = 1024
FEAT = 6144
TOKEN_COUNT = 4096
SEQUENCE_COUNT = 4
N_SEQ = 32


def group_keys(key):
    base_offset = jax.random.fold_in(key, 7301)
    return jnp.clip(jax.random.normal(base_offset, (SEQUENCE_COUNT, TOKEN_COUNT, KEY_VALUE_HEADS * HEAD_DIMENSION), jnp.float32), -4.0, 4.0)


def draw_keys(key, part):
    base_offset = group_keys(key)
    return base_offset.astype(jnp.bfloat16)


def draw_queries(key, part):
    fresh = jax.random.fold_in(key, 1709)
    base_offset = jnp.clip(jax.random.normal(fresh, (SEQUENCE_COUNT, TOKEN_COUNT, QUERY_HEADS * HEAD_DIMENSION), jnp.float32), -4.0, 4.0)
    return base_offset.astype(jnp.bfloat16)


def place_ends(entries, stream_key, least, largest):
    index_at = [jax.random.randint(jax.random.fold_in(stream_key, axis), (), 0, length) for axis, length in enumerate(entries.shape)]
    widest = entries.shape.index(max(entries.shape))
    next_to = index_at[:widest] + [(index_at[widest] + 1) % entries.shape[widest]] + index_at[widest + 1:]
    return entries.at[tuple(index_at)].set(least).at[tuple(next_to)].set(largest)


def shard_levels(stream_key, shape, pieces, least, high):
    gain = 1.0
    for dim, blocks in pieces:
        steps = jax.random.uniform(jax.random.fold_in(jax.random.fold_in(stream_key, 6), dim), (blocks,), jnp.float32, least / len(pieces), high / len(pieces))
        gain = gain * jnp.repeat(jnp.exp(steps), shape[dim] // blocks).reshape((-1,) + (1,) * (len(shape) - 1 - dim))
    return gain


def bell_draw(stream_key, dims, scale, most, split=(), kind=jnp.bfloat16):
    array = jax.random.normal(stream_key, dims, jnp.float32) * scale
    if len(split) > 0:
        array = shard_levels(stream_key, dims, split, -0.22, 0.18) * array
    return jnp.clip(array, min=-most, max=most).astype(kind)


def setup_inputs(seed: int = 0) -> dict:
    seeds = jax.random.split(jax.random.key(seed), 10)
    queries = draw_queries(jax.random.fold_in(seeds[9], 71), 0)
    keys = draw_keys(jax.random.fold_in(seeds[9], 71), 0)
    values = bell_draw(seeds[2], (SEQUENCE_COUNT, TOKEN_COUNT, KD), 1.0, 4.0, ((0, 4), (1, 32)))
    lengths = place_ends(jax.random.randint(seeds[3], (SEQUENCE_COUNT,), TOKEN_COUNT // 2, TOKEN_COUNT + 1), jax.random.fold_in(seeds[3], 1), TOKEN_COUNT // 2, TOKEN_COUNT).astype(jnp.int32)
    block_pos = jax.vmap(lambda own: jax.random.permutation(own, N_SEQ))(jax.random.split(seeds[4], SEQUENCE_COUNT)).reshape((SEQUENCE_COUNT, N_SEQ)).astype(jnp.int32)
    w_in = bell_draw(seeds[5], (FEAT, HIDDEN_UNITS), FEAT ** -0.5, 0.078125)
    b_in = bell_draw(seeds[6], (HIDDEN_UNITS,), 0.5, 3.0, (), jnp.float32)
    output_weight = bell_draw(seeds[7], (HIDDEN_UNITS, KEY_VALUE_HEADS), HIDDEN_UNITS ** -0.5, 0.1875)
    output_bias = jnp.clip(jax.random.uniform(seeds[8], (KEY_VALUE_HEADS,), jnp.float32, 1.0, 2.0), 1.0, 2.0)
    return {"queries": queries, "keys": keys, "values": values, "lengths": lengths, "block_pos": block_pos, "w_in": w_in, "b_in": b_in, "output_weight": output_weight, "output_bias": output_bias}


def column_mass(q_rows, k_rows, positions, limit):
    group_index = QUERY_HEADS // KEY_VALUE_HEADS
    scale = 1.0 / math.sqrt(HEAD_DIMENSION)

    def queries_per_group(g, sums):
        g32 = jnp.asarray(g).astype(jnp.int32)
        k_part = lax.dynamic_slice_in_dim(k_rows, g32 * HEAD_DIMENSION, HEAD_DIMENSION, 1).astype(jnp.float32)
        key_live = positions < limit

        def per_block(i, column):
            i32 = jnp.asarray(i).astype(jnp.int32)
            start = i32 * SEQ_DEV
            q_part = lax.dynamic_slice(q_rows, (start, g32 * group_index * HEAD_DIMENSION), (SEQ_DEV, group_index * HEAD_DIMENSION))
            q_part = q_part.astype(jnp.float32).reshape(SEQ_DEV, group_index, HEAD_DIMENSION)
            q_pos = lax.dynamic_slice_in_dim(positions, start, SEQ_DEV)
            allowed = (positions[None, :] <= q_pos[:, None]) & key_live[None, :]
            scores = jnp.einsum('qhd,kd->hqk', q_part, k_part) * scale
            masked = jnp.where(allowed[None], scores, -1e+30)
            top = lax.optimization_barrier(jnp.max(masked, axis=2, keepdims=True))
            weights = jnp.where(allowed[None], jnp.exp(masked - top), 0.0)
            total = lax.optimization_barrier(jnp.sum(weights, axis=2, keepdims=True))
            q_live = (q_pos < limit).astype(jnp.float32)
            share = weights / total * q_live[None, :, None]
            return column + lax.optimization_barrier(jnp.sum(share, axis=(0, 1)))
        column = lax.fori_loop(0, N_SEQ, per_block, jnp.zeros((TOKEN_COUNT,), jnp.float32))
        return lax.dynamic_update_index_in_dim(sums, column, g32, 0)
    return lax.fori_loop(0, KEY_VALUE_HEADS, queries_per_group, jnp.zeros((KEY_VALUE_HEADS, TOKEN_COUNT), jnp.float32))

def reference(queries, keys, values, lengths, block_pos, w_in, b_in, output_weight, output_bias):
    norm = 1.0 / math.sqrt(SEQUENCE_COUNT * TOKEN_COUNT)
    offsets = jnp.arange(SEQ_DEV, dtype=jnp.int32)
    grad_w_in = jnp.zeros((FEAT, HIDDEN_UNITS), jnp.float32)
    grad_b_in = jnp.zeros((HIDDEN_UNITS,), jnp.float32)
    output_weight_gradient = jnp.zeros((HIDDEN_UNITS, KEY_VALUE_HEADS), jnp.float32)
    output_bias_gradient = jnp.zeros((KEY_VALUE_HEADS,), jnp.float32)
    for index in range(SEQUENCE_COUNT):
        q_rows = queries[index]
        k_rows = keys[index]
        v_rows = values[index]
        positions = (block_pos[index][:, None] * SEQ_DEV + offsets[None, :]).reshape(-1).astype(jnp.int32)
        limit = lengths[index]
        live = (positions < limit).astype(jnp.float32)
        mass = column_mass(q_rows, k_rows, positions, limit)
        labels = jnp.log1p(mass).T
        features = jnp.concatenate([q_rows, k_rows, v_rows], axis=1)
        pre = jnp.dot(features, w_in, preferred_element_type=jnp.float32) + b_in
        act = jax.nn.silu(pre).astype(jnp.bfloat16)
        pred = jnp.dot(act, output_weight, preferred_element_type=jnp.float32) + output_bias
        resid = ((pred - labels) * live[:, None] * norm).astype(jnp.bfloat16)
        back = jnp.dot(resid, output_weight.T, preferred_element_type=jnp.float32)
        sig = jax.nn.sigmoid(pre)
        delta = (back * sig * (1.0 + pre * (1.0 - sig))).astype(jnp.bfloat16)
        grad_w_in = grad_w_in + jnp.dot(features.T, delta, preferred_element_type=jnp.float32)
        grad_b_in = grad_b_in + lax.optimization_barrier(jnp.sum(delta.astype(jnp.float32), axis=0))
        output_weight_gradient = output_weight_gradient + jnp.dot(act.T, resid, preferred_element_type=jnp.float32)
        output_bias_gradient = output_bias_gradient + lax.optimization_barrier(jnp.sum(resid.astype(jnp.float32), axis=0))
    return (grad_w_in, grad_b_in, output_weight_gradient, output_bias_gradient)
```

```python
import functools, math
import jax, jax.numpy as jnp
from jax import lax
from jax.experimental import pallas as pl
from jax.experimental.pallas import tpu as pltpu
from jax.sharding import PartitionSpec as P

NEG = -1e30

def attn_body(tq, kc, sub, blocks, rows, scale2, order_ref, limit_ref, q_hbm, k_hbm, out_ref, qs, ks, s_ref, acc_ref, sems):
    total = blocks * rows
    def issue(s, _):
        p = order_ref[s]
        dst = pl.ds(pl.multiple_of(p * rows, rows), rows)
        pltpu.make_async_copy(q_hbm.at[s], qs.at[dst], sems.at[0]).start()
        pltpu.make_async_copy(k_hbm.at[s], ks.at[dst], sems.at[1]).start()
        return 0
    lax.fori_loop(0, blocks, issue, 0)
    acc_ref[...] = jnp.zeros_like(acc_ref)
    for src, dst, i in ((q_hbm, qs, 0), (k_hbm, ks, 1)):
        pltpu.make_async_copy(src, src, sems.at[i]).wait()
    limit = limit_ref[0]
    lanes = 128
    groups = tq // lanes

    def tile(i, _):
        q0 = pl.multiple_of(i * tq, tq)
        q_part = qs[pl.ds(q0, tq), :]

        def scores(r0, mx, masked):
            k_part = ks[pl.ds(r0, kc), :]
            s = lax.dot_general(k_part, q_part, (((1,), (1,)), ((), ())), preferred_element_type=jnp.float32)
            if masked:
                kp = r0 + lax.broadcasted_iota(jnp.int32, (kc, tq), 0)
                qp = q0 + lax.broadcasted_iota(jnp.int32, (kc, tq), 1)
                s = jnp.where(kp <= qp, s, NEG)
            s_ref[pl.ds(r0, kc), :] = s
            return jnp.maximum(mx, jnp.max(s.reshape(kc // 8, 8, tq), axis=0))

        n_full = i * (tq // kc)
        mx = lax.fori_loop(0, n_full, lambda j, m: scores(pl.multiple_of(j * kc, kc), m, False), jnp.full((8, tq), NEG, jnp.float32))
        for d in range(tq // kc):
            mx = scores(pl.multiple_of(q0 + d * kc, kc), mx, True)
        top = jnp.max(mx, axis=0, keepdims=True)
        top8 = jnp.broadcast_to(top, (8, tq))
        n_sub = (i + 1) * (tq // sub)

        def weights(j, l):
            r0 = pl.multiple_of(j * sub, sub)
            s = s_ref[pl.ds(r0, sub), :].reshape(sub // 8, 8, tq)
            w = jnp.exp2((s - top8[None]) * scale2)
            s_ref[pl.ds(r0, sub), :] = w.reshape(sub, tq)
            return l + jnp.sum(w, axis=0)

        l = lax.fori_loop(0, n_sub, weights, jnp.zeros((8, tq), jnp.float32))
        denom = jnp.sum(l, axis=0, keepdims=True)
        qpos = q0 + lax.broadcasted_iota(jnp.int32, (1, tq), 1)
        rec = jnp.where(qpos < limit, 1.0 / denom, 0.0)
        rec8 = jnp.broadcast_to(rec, (8, tq))

        def shares(j, _):
            r0 = pl.multiple_of(j * sub, sub)
            w = s_ref[pl.ds(r0, sub), :].reshape(sub // 8, 8, tq) * rec8[None]
            w = w.reshape(sub, tq)
            tot = w[:, :lanes]
            for g in range(1, groups):
                tot = tot + w[:, g * lanes:(g + 1) * lanes]
            acc_ref[pl.ds(r0, sub), :] += tot
            return 0
        lax.fori_loop(0, n_sub, shares, 0)
        return 0

    lax.fori_loop(0, total // tq, tile, 0)

    def emit(s, _):
        p = order_ref[s]
        part = acc_ref[pl.ds(pl.multiple_of(p * rows, rows), rows), :]
        out_ref[pl.ds(s, 1), :] = jnp.sum(part.T, axis=0, keepdims=True)
        return 0
    lax.fori_loop(0, blocks, emit, 0)


def attention(order, limit, q_all, k_all, tq=512, kc=128, sub=64):
    blocks, rows, head = q_all.shape
    total = blocks * rows
    scale2 = math.log2(math.e) / math.sqrt(head)
    return pl.pallas_call(
        functools.partial(attn_body, tq, kc, sub, blocks, rows, scale2),
        out_shape=jax.ShapeDtypeStruct((blocks, rows), jnp.float32),
        in_specs=[pl.BlockSpec(memory_space=pltpu.SMEM)] * 2 + [pl.BlockSpec(memory_space=pl.ANY)] * 2,
        out_specs=pl.BlockSpec(memory_space=pltpu.VMEM),
        scratch_shapes=[
            pltpu.VMEM((total, head), jnp.bfloat16),
            pltpu.VMEM((total, head), jnp.bfloat16),
            pltpu.VMEM((total, tq), jnp.float32),
            pltpu.VMEM((total, 128), jnp.float32),
            pltpu.SemaphoreType.DMA((2,)),
        ],
        compiler_params=pltpu.CompilerParams(vmem_limit_bytes=48 * 2**20),
        cost_estimate=pl.CostEstimate(flops=total * total * head, bytes_accessed=4 * total * head, transcendentals=total * total // 2),
        name="mass",
    )(order, limit, q_all, k_all)


def on_device(queries, keys, values, lengths, block_pos, w_in, b_in, output_weight, output_bias):
    q_rows, k_rows, v_rows = queries[0], keys[0], values[0]
    rows = q_rows.shape[0]
    heads_kv = output_weight.shape[1]
    head = k_rows.shape[1] // heads_kv
    n = lax.axis_size("seq")
    per = q_rows.shape[1] // k_rows.shape[1]
    total = n * rows
    mine = lax.axis_index("seq")
    q_send = q_rows.reshape(rows, n, head).transpose(1, 0, 2)
    k_send = jnp.repeat(k_rows.reshape(rows, heads_kv, head).transpose(1, 0, 2), per, axis=0)
    both = lax.all_to_all(jnp.concatenate([q_send, k_send], axis=2), "seq", 0, 0, tiled=True)
    mass_own = attention(block_pos[0], lengths, both[:, :, :head], both[:, :, head:], 512, 512, 64)
    features = jnp.concatenate([q_rows, k_rows, v_rows], axis=1)
    cols = features.shape[1] // n
    f_mine = lax.all_to_all(features.reshape(rows, n, cols).transpose(1, 0, 2), "seq", 0, 0, tiled=True).reshape(total, cols)
    pre = jnp.dot(features, w_in, preferred_element_type=jnp.float32) + b_in
    sig = jax.nn.sigmoid(pre)
    act = (pre * sig).astype(jnp.bfloat16)
    slope = sig * (1.0 + pre * (1.0 - sig))
    pred = jnp.dot(act, output_weight, preferred_element_type=jnp.float32) + output_bias
    offsets = jnp.arange(rows, dtype=jnp.int32)
    query_pos = lax.dynamic_index_in_dim(block_pos[0], mine, 0, keepdims=False) * rows + offsets
    query_live = (query_pos < lengths[0]).astype(jnp.float32)
    norm = 1.0 / math.sqrt(lax.axis_size("batch") * total)

    mass = lax.all_to_all(mass_own, "seq", 0, 0, tiled=True)
    mass = jnp.sum(mass.reshape(heads_kv, per, rows), axis=1)
    labels = jnp.log1p(mass).T
    resid = ((pred - labels) * query_live[:, None] * norm).astype(jnp.bfloat16)
    back = lax.dot_general(resid, output_weight, (((1,), (1,)), ((), ())), preferred_element_type=jnp.float32)
    delta = (back * slope).astype(jnp.bfloat16)
    every_delta = lax.all_gather(delta, "seq", axis=0, tiled=True)
    out_term = lax.dot_general(resid, act, (((0,), (0,)), ((), ())), preferred_element_type=jnp.float32)
    small = jnp.concatenate([
        jnp.sum(delta.astype(jnp.float32), axis=0),
        out_term.ravel(),
        jnp.sum(resid.astype(jnp.float32), axis=0)])
    small = lax.psum(small, ("seq", "batch"))
    h = b_in.shape[0]
    grad_b_in = small[:h]
    output_weight_gradient = small[h:h + h * heads_kv].reshape(heads_kv, h).T
    output_bias_gradient = small[h + h * heads_kv:]
    part = lax.dot_general(f_mine, every_delta, (((0,), (0,)), ((), ())), preferred_element_type=jnp.float32)
    grad_w_in = lax.psum_scatter(part, "batch", scatter_dimension=0, tiled=True)
    return (grad_w_in, grad_b_in, output_weight_gradient, output_bias_gradient)


def solution(mesh):
    return jax.shard_map(
        on_device,
        mesh=mesh,
        in_specs=(
            P("batch", "seq", None),
            P("batch", "seq", None),
            P("batch", "seq", None),
            P("batch"),
            P("batch", None),
            P(),
            P(),
            P(),
            P(),
        ),
        out_specs=(P(("seq", "batch"), None), P(), P(), P()),
        check_vma=False,
    )
```

```python
import functools, math
import jax, jax.numpy as jnp
from jax import lax
from jax.experimental import pallas as pl
from jax.experimental.pallas import tpu as pltpu
from jax.sharding import PartitionSpec as P

NEG = -1e30

def attn_body(tq, kc, sub, blocks, rows, scale2, order_ref, limit_ref, q_hbm, k_hbm, out_ref, qs, ks, s_ref, acc_ref, sems):
    total = blocks * rows
    def issue(s, _):
        p = order_ref[s]
        dst = pl.ds(pl.multiple_of(p * rows, rows), rows)
        pltpu.make_async_copy(q_hbm.at[s], qs.at[dst], sems.at[0]).start()
        pltpu.make_async_copy(k_hbm.at[s], ks.at[dst], sems.at[1]).start()
        return 0
    lax.fori_loop(0, blocks, issue, 0)
    acc_ref[...] = jnp.zeros_like(acc_ref)
    for src, dst, i in ((q_hbm, qs, 0), (k_hbm, ks, 1)):
        pltpu.make_async_copy(src, src, sems.at[i]).wait()
    limit = limit_ref[0]
    lanes = 128
    groups = tq // lanes

    def tile(i, _):
        q0 = pl.multiple_of(i * tq, tq)
        q_part = qs[pl.ds(q0, tq), :]

        def scores(r0, mx, masked):
            k_part = ks[pl.ds(r0, kc), :]
            s = lax.dot_general(k_part, q_part, (((1,), (1,)), ((), ())), preferred_element_type=jnp.float32)
            if masked:
                kp = r0 + lax.broadcasted_iota(jnp.int32, (kc, tq), 0)
                qp = q0 + lax.broadcasted_iota(jnp.int32, (kc, tq), 1)
                s = jnp.where(kp <= qp, s, NEG)
            s_ref[pl.ds(r0, kc), :] = s
            return jnp.maximum(mx, jnp.max(s.reshape(kc // 8, 8, tq), axis=0))

        n_full = i * (tq // kc)
        mx = lax.fori_loop(0, n_full, lambda j, m: scores(pl.multiple_of(j * kc, kc), m, False), jnp.full((8, tq), NEG, jnp.float32))
        for d in range(tq // kc):
            mx = scores(pl.multiple_of(q0 + d * kc, kc), mx, True)
        top = jnp.max(mx, axis=0, keepdims=True)
        top8 = jnp.broadcast_to(top, (8, tq))
        n_sub = (i + 1) * (tq // sub)

        def weights(j, l):
            r0 = pl.multiple_of(j * sub, sub)
            s = s_ref[pl.ds(r0, sub), :].reshape(sub // 8, 8, tq)
            w = jnp.exp2((s - top8[None]) * scale2)
            s_ref[pl.ds(r0, sub), :] = w.reshape(sub, tq)
            return l + jnp.sum(w, axis=0)

        l = lax.fori_loop(0, n_sub, weights, jnp.zeros((8, tq), jnp.float32))
        denom = jnp.sum(l, axis=0, keepdims=True)
        qpos = q0 + lax.broadcasted_iota(jnp.int32, (1, tq), 1)
        rec = jnp.where(qpos < limit, 1.0 / denom, 0.0)
        rec8 = jnp.broadcast_to(rec, (8, tq))

        def shares(j, _):
            r0 = pl.multiple_of(j * sub, sub)
            w = s_ref[pl.ds(r0, sub), :].reshape(sub // 8, 8, tq) * rec8[None]
            w = w.reshape(sub, tq)
            tot = w[:, :lanes]
            for g in range(1, groups):
                tot = tot + w[:, g * lanes:(g + 1) * lanes]
            acc_ref[pl.ds(r0, sub), :] += tot
            return 0
        lax.fori_loop(0, n_sub, shares, 0)
        return 0

    lax.fori_loop(0, total // tq, tile, 0)

    def emit(s, _):
        p = order_ref[s]
        part = acc_ref[pl.ds(pl.multiple_of(p * rows, rows), rows), :]
        out_ref[s] = jnp.sum(part.T, axis=0, keepdims=True)
        return 0
    lax.fori_loop(0, blocks, emit, 0)


def attention(order, limit, q_all, k_all, tq=512, kc=128, sub=64):
    blocks, rows, head = q_all.shape
    total = blocks * rows
    scale2 = math.log2(math.e) / math.sqrt(head)
    return pl.pallas_call(
        functools.partial(attn_body, tq, kc, sub, blocks, rows, scale2),
        out_shape=jax.ShapeDtypeStruct((blocks, 1, rows), jnp.float32),
        in_specs=[pl.BlockSpec(memory_space=pltpu.SMEM)] * 2 + [pl.BlockSpec(memory_space=pl.ANY)] * 2,
        out_specs=pl.BlockSpec(memory_space=pltpu.VMEM),
        scratch_shapes=[
            pltpu.VMEM((total, head), jnp.bfloat16),
            pltpu.VMEM((total, head), jnp.bfloat16),
            pltpu.VMEM((total, tq), jnp.float32),
            pltpu.VMEM((total, 128), jnp.float32),
            pltpu.SemaphoreType.DMA((2,)),
        ],
        compiler_params=pltpu.CompilerParams(vmem_limit_bytes=48 * 2**20),
        cost_estimate=pl.CostEstimate(flops=total * total * head, bytes_accessed=4 * total * head, transcendentals=total * total // 2),
        name="mass",
    )(order, limit, q_all, k_all)


MESH = pl.DeviceIdType.MESH


def remote(src, dst, send_sem, recv_sem, device):
    return pltpu.make_async_remote_copy(
        src_ref=src, dst_ref=dst, send_sem=send_sem, recv_sem=recv_sem, device_id=device, device_id_type=MESH
    )


def tail_body(dims, norm, mass_ref, pred_ref, live_ref, w2t_ref, slope_ref, act_ref, f_ref, grad_ref, small_ref,
              mrecv, lab, dl, ft, part, pair, xrecv, sm, smr, zs, ys, xs,
              m_send, m_recv, g_send, g_recv, p_send, p_recv, x_send, x_recv, s_send, s_recv):
    ny, nz, nb = dims
    n = ny * nz * 2
    s, b = lax.axis_index("seq"), lax.axis_index("batch")
    core, c = lax.rem(s, 2), s // 2
    z, y = lax.rem(c, nz), c // nz
    rows, hidden = slope_ref.shape
    chunks, tokens, width = dl.shape
    feats = part.shape[1]
    half = feats // 2
    own_rows = half // nb
    partner = (s + 1 - 2 * core, b)

    barrier = pltpu.get_barrier_semaphore()

    def greet(r, _):
        pl.semaphore_signal(barrier, inc=1, device_id=(lax.rem(s + r, n), b), device_id_type=MESH)
        return 0
    lax.fori_loop(1, n, greet, 0)
    for r in range(1, nb):
        pl.semaphore_signal(barrier, inc=1, device_id=(s, lax.rem(b + r, nb)), device_id_type=MESH)
    pl.semaphore_wait(barrier, n - 1 + nb - 1)

    def mass_copy(r, sender):
        to = lax.rem(s + r, n)
        return remote(mass_ref.at[to], mrecv.at[s], m_send.at[r], m_recv.at[s], (to, b))

    def mass_start(r, _):
        mass_copy(r, s).start()
        return 0
    lax.fori_loop(1, n, mass_start, 0)
    mrecv[s] = mass_ref[s]

    for k in range(tokens // rows):
        ft[:, k * rows:(k + 1) * rows] = f_ref[k * rows:(k + 1) * rows, :].T

    def mass_wait(r, _):
        frm = lax.rem(s + n - r, n)
        got = remote(mass_ref.at[frm], mrecv.at[frm], m_send.at[r], m_recv.at[frm], (frm, b))
        got.wait_recv()
        return 0
    lax.fori_loop(1, n, mass_wait, 0)

    heads = lab.shape[0]
    per = n // heads
    for g in range(heads):
        total = mrecv[per * g]
        for i in range(1, per):
            total = total + mrecv[per * g + i]
        lab[g:g + 1, :] = jnp.log1p(total)
    resid_t = ((pred_ref[...] - lab[...]) * live_ref[...] * norm).astype(jnp.bfloat16)
    resid = resid_t.astype(jnp.float32).T.astype(jnp.bfloat16)
    back = jnp.dot(resid, w2t_ref[...], preferred_element_type=jnp.float32)
    delta = (back * slope_ref[...]).astype(jnp.bfloat16)
    here = pl.ds(pl.multiple_of(c * rows, rows), rows)
    for j in range(chunks):
        dl[j, here, :] = delta[:, j * width:(j + 1) * width]

    wide = rows // 2
    slot = {}

    def number(*key):
        return slot.setdefault(key, len(slot))

    def spot(half_id, a, e):
        return (a * nz + e) if half_id == 0 else (e * nz + a)

    def ring(v, d, size):
        return lax.rem(v + (d + size), size)

    def coords(half_id):
        return (y, z, ny, nz) if half_id == 0 else (z, y, nz, ny)

    def piece(j, block, half_id, quarter):
        r0 = half_id * wide + (quarter * (wide // 2) if quarter is not None else 0)
        size = wide // 2 if quarter is not None else wide
        return dl.at[j, pl.ds(pl.multiple_of(block * rows + r0, wide // 2), size), :]

    def neighbour(half_id, which, d):
        along_y = (half_id == 0) == (which == 0)
        to_y = ring(y, d, ny) if along_y else y
        to_z = z if along_y else ring(z, d, nz)
        return ((to_y * nz + to_z) * 2 + core, b)

    started = []

    def copy(j, half_id, which, da, de, quarter, d):
        a, e, na, ne = coords(half_id)
        block = spot(half_id, ring(a, da, na), ring(e, de, ne))
        ref = piece(j, block, half_id, quarter)
        m = number(j, half_id, which, da, de, quarter, d)
        return remote(ref, ref, g_send.at[m], g_recv.at[m], neighbour(half_id, which, d))

    def send(j, half_id, which, da, de, quarter, d):
        one = copy(j, half_id, which, da, de, quarter, d)
        one.start()
        started.append(one)

    def receive(j, half_id, which, da, de, quarter, d):
        a, e, na, ne = coords(half_id)
        back_a, back_e = (da - d, de) if which == 0 else (da, de - d)
        block = spot(half_id, ring(a, back_a, na), ring(e, back_e, ne))
        ref = piece(j, block, half_id, quarter)
        m = number(j, half_id, which, da, de, quarter, d)
        remote(ref, ref, g_send.at[m], g_recv.at[m], neighbour(half_id, which, -d)).wait_recv()

    def second(j, h, da):
        for d in (1, -1):
            send(j, h, 1, da, 0, None, d)

    def second_pass_on(j, h, da):
        receive(j, h, 1, da, 0, None, 1)
        send(j, h, 1, da, -1, 0, 1)
        receive(j, h, 1, da, 0, None, -1)
        send(j, h, 1, da, 1, 1, -1)

    def second_end(j, h, da):
        receive(j, h, 1, da, -1, 0, 1)
        receive(j, h, 1, da, 1, 1, -1)

    def stage0(j):
        for h in (0, 1):
            for d in (1, -1):
                send(j, h, 0, 0, 0, None, d)
        for h in (0, 1):
            second(j, h, 0)

    def stage1(j):
        for h in (0, 1):
            receive(j, h, 0, 0, 0, None, 1)
            send(j, h, 0, -1, 0, 0, 1)
            second(j, h, -1)
            receive(j, h, 0, 0, 0, None, -1)
            send(j, h, 0, 1, 0, 1, -1)
            second(j, h, 1)

    def stage2(j):
        for h in (0, 1):
            second_pass_on(j, h, 0)
        for h in (0, 1):
            receive(j, h, 0, -1, 0, 0, 1)
            receive(j, h, 0, 1, 0, 1, -1)
            second(j, h, 2)

    def stage3(j):
        for da in (-1, 1):
            for h in (0, 1):
                second_pass_on(j, h, da)

    def stage4(j):
        for h in (0, 1):
            second_pass_on(j, h, 2)

    def stage5(j):
        for da in (0, -1, 1, 2):
            for h in (0, 1):
                second_end(j, h, da)

    def multiply(j):
        part[j] = jnp.dot(ft[...], dl[j], preferred_element_type=jnp.float32)

    def pair_copy(j, of):
        ref = part.at[j, pl.ds(pl.multiple_of((1 - of) * half, half), half), :]
        return remote(ref, pair.at[j], p_send.at[j], p_recv.at[j], partner)

    def pair_start(j):
        one = pair_copy(j, core)
        one.start()
        started.append(one)

    def x_copy(j, r):
        to = lax.rem(b + r, nb)
        ref = pair.at[j, pl.ds(pl.multiple_of(to * own_rows, own_rows), own_rows), :]
        return remote(ref, xrecv.at[j, r - 1], x_send.at[j, r - 1], x_recv.at[j, r - 1], (s, to))

    def x_start(j):
        pair_copy(j, core).wait_recv()
        pair[j] = pair[j] + part[j, pl.ds(pl.multiple_of(core * half, half), half), :]
        for r in (2, 1, 3)[: nb - 1]:
            one = x_copy(j, r)
            one.start()
            started.append(one)

    def x_end(j):
        for r in range(1, nb):
            x_copy(j, r).wait_recv()
        own = pair[j, pl.ds(pl.multiple_of(b * own_rows, own_rows), own_rows), :]
        for r in range(1, nb):
            own = own + xrecv[j, r - 1]
        grad_ref[:, j * width:(j + 1) * width] = own

    def small_start0():
        sw = sm.shape[2]
        out_term = jnp.dot(resid_t, act_ref[...], preferred_element_type=jnp.float32)
        sums = jnp.sum(delta.astype(jnp.float32), axis=0, keepdims=True)
        bias = jnp.sum(resid_t.astype(jnp.float32), axis=1, keepdims=True)
        lanes = 128
        cols = [out_term[:, k * lanes:(k + 1) * lanes] for k in range(hidden // lanes)]
        cols.append(jnp.concatenate([sums[:, k * lanes:(k + 1) * lanes] for k in range(hidden // lanes)], axis=0))
        cols.append(jnp.broadcast_to(bias, (heads, lanes)))
        each = sw // lanes
        for k, value in enumerate(cols):
            sm[k // each, :, (k % each) * lanes:(k % each + 1) * lanes] = value
        one = remote(sm.at[1 - core], smr, s_send.at[0], s_recv.at[0], partner)
        one.start()
        started.append(one)

    def small_hop(level, value, buf, at, size, target):
        buf[at] = value
        for r in range(1, size):
            one = remote(buf.at[at], buf.at[at], s_send.at[level * 3 + r], s_recv.at[level * 3 + r], target(r))
            one.start()
            started.append(one)

    def small_sum(level, buf, at, size, target):
        for r in range(1, size):
            frm = lax.rem(at + size - r, size)
            remote(buf.at[frm], buf.at[frm], s_send.at[level * 3 + r], s_recv.at[level * 3 + r], target(r)).wait_recv()
        total = buf[0]
        for k in range(1, size):
            total = total + buf[k]
        return total

    to_z = lambda r: ((y * nz + lax.rem(z + r, nz)) * 2 + core, b)
    to_y = lambda r: ((lax.rem(y + r, ny) * nz + z) * 2 + core, b)
    to_x = lambda r: (s, lax.rem(b + r, nb))

    def small1():
        remote(sm.at[1 - core], smr, s_send.at[0], s_recv.at[0], partner).wait_recv()
        small_hop(0, sm[core] + smr[...], zs, z, nz, to_z)

    def small2():
        small_hop(1, small_sum(0, zs, z, nz, to_z), ys, y, ny, to_y)

    def small3():
        small_hop(2, small_sum(1, ys, y, ny, to_y), xs, b, nb, to_x)

    def small4():
        sm[core] = small_sum(2, xs, b, nb, to_x)
        one = remote(sm.at[core], small_ref.at[core], s_send.at[10], s_recv.at[10], partner)
        one.start()
        started.append(one)
        small_ref[core] = sm[core]

    def small5():
        remote(sm.at[1 - core], small_ref.at[1 - core], s_send.at[10], s_recv.at[10], partner).wait_recv()

    if chunks == 2:
        stage0(0); small_start0(); stage1(0); stage2(0); stage0(1); stage3(0); small1(); stage1(1); stage4(0)
        stage2(1); stage5(0); small2(); stage3(1)
        multiply(0); pair_start(0); stage4(1); small3()
        x_start(0); stage5(1)
        multiply(1); pair_start(1); small4(); x_end(0); x_start(1); small5(); x_end(1)
    else:
        small = [small1, small2, small3, small4, small5]
        stage0(0); small_start0(); stage1(0); stage2(0)
        for j in range(chunks):
            last = j + 1 == chunks
            if not last:
                stage0(j + 1)
            stage3(j)
            if not last:
                stage1(j + 1)
            stage4(j)
            if not last:
                stage2(j + 1)
            stage5(j)
            if small:
                small.pop(0)()
            multiply(j)
            pair_start(j)
            if small:
                small.pop(0)()
            if j > 0:
                x_end(j - 1)
            x_start(j)
        for one in small:
            one()
        x_end(chunks - 1)

    for one in started:
        one.wait_send()

    def mass_drain(r, _):
        mass_copy(r, s).wait_send()
        return 0
    lax.fori_loop(1, n, mass_drain, 0)


def tail(dims, norm, mass, pred_t, live, w2t, slope, act, f, chunks=2):
    ny, nz, nb = dims
    n = mass.shape[0]
    rows, hidden = slope.shape
    tokens, feats = f.shape
    heads = pred_t.shape[0]
    width = hidden // chunks
    half = feats // 2
    sw = (hidden + 256) // 2
    vm = pltpu.VMEM
    dma = pltpu.SemaphoreType.DMA
    return pl.pallas_call(
        functools.partial(tail_body, dims, norm),
        out_shape=(
            jax.ShapeDtypeStruct((half // nb, hidden), jnp.float32),
            jax.ShapeDtypeStruct((2, heads, sw), jnp.float32),
        ),
        in_specs=[pl.BlockSpec(memory_space=vm)] * 7,
        out_specs=[pl.BlockSpec(memory_space=vm)] * 2,
        scratch_shapes=[
            vm((n, 1, rows), jnp.float32),
            vm((heads, rows), jnp.float32),
            vm((chunks, tokens, width), jnp.bfloat16),
            vm((feats, tokens), jnp.bfloat16),
            vm((chunks, feats, width), jnp.float32),
            vm((chunks, half, width), jnp.float32),
            vm((chunks, nb - 1, half // nb, width), jnp.float32),
            vm((2, heads, sw), jnp.float32),
            vm((heads, sw), jnp.float32),
            vm((nz, heads, sw), jnp.float32),
            vm((ny, heads, sw), jnp.float32),
            vm((nb, heads, sw), jnp.float32),
            dma((n,)), dma((n,)),
            dma((chunks * 40,)), dma((chunks * 40,)),
            dma((chunks,)), dma((chunks,)),
            dma((chunks, nb - 1)), dma((chunks, nb - 1)),
            dma((12,)), dma((12,)),
        ],
        compiler_params=pltpu.CompilerParams(collective_id=3, has_side_effects=True, vmem_limit_bytes=56 * 2**20),
        cost_estimate=pl.CostEstimate(flops=2 * tokens * feats * hidden, bytes_accessed=8 * 2**20, transcendentals=0),
        name="tail",
    )(mass, pred_t, live, w2t, slope, act, f)


def on_device(dims, queries, keys, values, lengths, block_pos, w_in, b_in, output_weight, output_bias):
    q_rows, k_rows, v_rows = queries[0], keys[0], values[0]
    rows = q_rows.shape[0]
    hidden, heads_kv = output_weight.shape
    head = k_rows.shape[1] // heads_kv
    n = lax.axis_size("seq")
    per = q_rows.shape[1] // k_rows.shape[1]
    total = n * rows
    mine = lax.axis_index("seq")
    q_send = q_rows.reshape(rows, n, head).transpose(1, 0, 2)
    k_send = jnp.repeat(k_rows.reshape(rows, heads_kv, head).transpose(1, 0, 2), per, axis=0)
    both = lax.all_to_all(jnp.concatenate([q_send, k_send], axis=2), "seq", 0, 0, tiled=True)
    mass_own = attention(block_pos[0], lengths, both[:, :, :head], both[:, :, head:], 512, 512, 64)
    features = jnp.concatenate([q_rows, k_rows, v_rows], axis=1)
    chips = n // 2
    cols = features.shape[1] // chips
    planes = [[2 * i + core for i in range(chips)] for core in range(2)]
    f_mine = lax.all_to_all(
        features.reshape(rows, chips, cols).transpose(1, 0, 2), "seq", 0, 0, tiled=True, axis_index_groups=planes
    ).reshape(chips * rows, cols)
    pre = jnp.dot(features, w_in, preferred_element_type=jnp.float32) + b_in
    sig = jax.nn.sigmoid(pre)
    act = (pre * sig).astype(jnp.bfloat16)
    slope = sig * (1.0 + pre * (1.0 - sig))
    pred = jnp.dot(act, output_weight, preferred_element_type=jnp.float32) + output_bias
    offsets = jnp.arange(rows, dtype=jnp.int32)
    query_pos = lax.dynamic_index_in_dim(block_pos[0], mine, 0, keepdims=False) * rows + offsets
    query_live = (query_pos < lengths[0]).astype(jnp.float32)
    norm = 1.0 / math.sqrt(lax.axis_size("batch") * total)
    grad_w_in, small = tail(dims, norm, mass_own, pred.T, query_live[None, :], output_weight.T, slope, act, f_mine)
    small = jnp.concatenate([small[0], small[1]], axis=1)
    grad_b_in = small[:, hidden:hidden + 128].reshape(hidden)
    return (grad_w_in, grad_b_in, small[:, :hidden].T, small[:, hidden + 128])


def solution(mesh):
    nb = mesh.shape["batch"]
    ny = nz = math.isqrt(mesh.shape["seq"] // 2)
    return jax.shard_map(
        functools.partial(on_device, (ny, nz, nb)),
        mesh=mesh,
        in_specs=(
            P("batch", "seq", None),
            P("batch", "seq", None),
            P("batch", "seq", None),
            P("batch"),
            P("batch", None),
            P(),
            P(),
            P(),
            P(),
        ),
        out_specs=(P(("seq", "batch"), None), P(), P(), P()),
        check_vma=False,
    )
```

```python
import functools, math
import jax, jax.numpy as jnp
from jax import lax
from jax.experimental import pallas as pl
from jax.experimental.pallas import tpu as pltpu
from jax.sharding import PartitionSpec as P

NEG = -1e30

def attn_body(tq, kc, sub, blocks, rows, scale2, order_ref, limit_ref, q_hbm, k_hbm, out_ref, qs, ks, s_ref, acc_ref, sems):
    total = blocks * rows
    def issue(s, _):
        p = order_ref[s]
        dst = pl.ds(pl.multiple_of(p * rows, rows), rows)
        pltpu.make_async_copy(q_hbm.at[s], qs.at[dst], sems.at[0]).start()
        pltpu.make_async_copy(k_hbm.at[s], ks.at[dst], sems.at[1]).start()
        return 0
    lax.fori_loop(0, blocks, issue, 0)
    acc_ref[...] = jnp.zeros_like(acc_ref)
    for src, dst, i in ((q_hbm, qs, 0), (k_hbm, ks, 1)):
        pltpu.make_async_copy(src, src, sems.at[i]).wait()
    limit = limit_ref[0]
    lanes = 128
    groups = tq // lanes

    def tile(i, _):
        q0 = pl.multiple_of(i * tq, tq)
        q_part = qs[pl.ds(q0, tq), :]

        def scores(r0, mx, masked):
            k_part = ks[pl.ds(r0, kc), :]
            s = lax.dot_general(k_part, q_part, (((1,), (1,)), ((), ())), preferred_element_type=jnp.float32)
            if masked:
                kp = r0 + lax.broadcasted_iota(jnp.int32, (kc, tq), 0)
                qp = q0 + lax.broadcasted_iota(jnp.int32, (kc, tq), 1)
                s = jnp.where(kp <= qp, s, NEG)
            s_ref[pl.ds(r0, kc), :] = s
            return jnp.maximum(mx, jnp.max(s.reshape(kc // 8, 8, tq), axis=0))

        n_full = i * (tq // kc)
        mx = lax.fori_loop(0, n_full, lambda j, m: scores(pl.multiple_of(j * kc, kc), m, False), jnp.full((8, tq), NEG, jnp.float32))
        for d in range(tq // kc):
            mx = scores(pl.multiple_of(q0 + d * kc, kc), mx, True)
        top = jnp.max(mx, axis=0, keepdims=True)
        top8 = jnp.broadcast_to(top, (8, tq))
        n_sub = (i + 1) * (tq // sub)

        def weights(j, l):
            r0 = pl.multiple_of(j * sub, sub)
            s = s_ref[pl.ds(r0, sub), :].reshape(sub // 8, 8, tq)
            w = jnp.exp2((s - top8[None]) * scale2)
            s_ref[pl.ds(r0, sub), :] = w.reshape(sub, tq)
            return l + jnp.sum(w, axis=0)

        l = lax.fori_loop(0, n_sub, weights, jnp.zeros((8, tq), jnp.float32))
        denom = jnp.sum(l, axis=0, keepdims=True)
        qpos = q0 + lax.broadcasted_iota(jnp.int32, (1, tq), 1)
        rec = jnp.where(qpos < limit, 1.0 / denom, 0.0)
        rec8 = jnp.broadcast_to(rec, (8, tq))

        def shares(j, _):
            r0 = pl.multiple_of(j * sub, sub)
            w = s_ref[pl.ds(r0, sub), :].reshape(sub // 8, 8, tq) * rec8[None]
            w = w.reshape(sub, tq)
            tot = w[:, :lanes]
            for g in range(1, groups):
                tot = tot + w[:, g * lanes:(g + 1) * lanes]
            acc_ref[pl.ds(r0, sub), :] += tot
            return 0
        lax.fori_loop(0, n_sub, shares, 0)
        return 0

    lax.fori_loop(0, total // tq, tile, 0)

    def emit(s, _):
        p = order_ref[s]
        part = acc_ref[pl.ds(pl.multiple_of(p * rows, rows), rows), :]
        out_ref[s] = jnp.sum(part.T, axis=0, keepdims=True)
        return 0
    lax.fori_loop(0, blocks, emit, 0)


def attention(order, limit, q_all, k_all, tq=512, kc=128, sub=64):
    blocks, rows, head = q_all.shape
    total = blocks * rows
    scale2 = math.log2(math.e) / math.sqrt(head)
    return pl.pallas_call(
        functools.partial(attn_body, tq, kc, sub, blocks, rows, scale2),
        out_shape=jax.ShapeDtypeStruct((blocks, 1, rows), jnp.float32),
        in_specs=[pl.BlockSpec(memory_space=pltpu.SMEM)] * 2 + [pl.BlockSpec(memory_space=pltpu.HBM)] * 2,
        out_specs=pl.BlockSpec(memory_space=pltpu.VMEM),
        scratch_shapes=[
            pltpu.VMEM((total, head), jnp.bfloat16),
            pltpu.VMEM((total, head), jnp.bfloat16),
            pltpu.VMEM((total, tq), jnp.float32),
            pltpu.VMEM((total, 128), jnp.float32),
            pltpu.SemaphoreType.DMA((2,)),
        ],
        compiler_params=pltpu.CompilerParams(vmem_limit_bytes=48 * 2**20),
        cost_estimate=pl.CostEstimate(flops=total * total * head, bytes_accessed=4 * total * head, transcendentals=total * total // 2),
        name="mass",
    )(order, limit, q_all, k_all)


MESH = pl.DeviceIdType.MESH


def remote(src, dst, send_sem, recv_sem, device):
    return pltpu.make_async_remote_copy(
        src_ref=src, dst_ref=dst, send_sem=send_sem, recv_sem=recv_sem, device_id=device, device_id_type=MESH
    )


def head_body(dims, per, q_ref, k_ref, v_ref, bin_ref, w2t_ref, bias_ref, w_hbm, qa, ka, pred_ref, slope_ref, act_ref,
              stage, wbuf, pre, w_sem, i_send, i_recv, d_send, d_recv, l_sem):
    ny, nz, nb = dims
    chips = ny * nz
    s, b = lax.axis_index("seq"), lax.axis_index("batch")
    core, c = lax.rem(s, 2), s // 2
    z, y = lax.rem(c, nz), c // nz
    partner = (s + 1 - 2 * core, b)
    head = ka.shape[2]
    slots, deep, hidden = wbuf.shape
    steps = w_hbm.shape[0] // deep

    def w_copy(i):
        at = lax.rem(i, slots)
        return pltpu.make_async_copy(w_hbm.at[pl.ds(pl.multiple_of(i * deep, deep), deep), :], wbuf.at[at], w_sem.at[at])

    for i in range(slots):
        w_copy(i).start()

    def chip_at(r, sign):
        dy, dz = r // nz, lax.rem(r, nz)
        return lax.rem(y + sign * dy + ny, ny) * nz + lax.rem(z + sign * dz + nz, nz)

    barrier = pltpu.get_barrier_semaphore()

    def greet(r, _):
        pl.semaphore_signal(barrier, inc=1, device_id=(2 * chip_at(r, 1) + core, b), device_id_type=MESH)
        return 0
    lax.fori_loop(1, chips, greet, 0)
    pl.semaphore_signal(barrier, inc=1, device_id=partner, device_id_type=MESH)
    pl.semaphore_wait(barrier, chips)

    def columns(ref, i):
        return ref.at[:, pl.ds(pl.multiple_of(i * head, head), head)]

    def parts(to):
        return (columns(q_ref, 2 * to + core), columns(q_ref, 2 * to + 1 - core), columns(k_ref, (2 * to) // per))

    def arrivals(frm):
        return (qa.at[2 * frm + core], stage.at[0, frm], stage.at[1, frm])

    def across(i, src, to, frm, dst):
        return remote(src, dst, i_send.at[i, to], i_recv.at[i, frm], (2 * to + core, b))

    def send(r, _):
        to = chip_at(r, 1)
        for i in (1, 2, 0):
            across(i, parts(to)[i], to, c, arrivals(c)[i]).start()
        return 0
    lax.fori_loop(1, chips, send, 0)

    def over(i, src, at):
        dst = (qa.at[2 * at + core], ka.at[2 * at + core])[i]
        return remote(src, dst, d_send.at[i, at], d_recv.at[i, at], partner)

    def keep(src, at):
        return pltpu.make_async_copy(src, ka.at[2 * at + core], l_sem.at[at])

    own_q, other_q, own_k = parts(c)
    over(0, other_q, c).start()
    over(1, own_k, c).start()
    keep(own_k, c).start()
    own_copy = pltpu.make_async_copy(own_q, qa.at[2 * c + core], l_sem.at[chips])
    own_copy.start()

    pre[...] = jnp.broadcast_to(bin_ref[...], pre.shape)

    def multiply(i, x):
        w_copy(i).wait()
        pre[...] += jnp.dot(x, wbuf[lax.rem(i, slots)], preferred_element_type=jnp.float32)

    def refill(i):
        @pl.when(i + slots < steps)
        def _():
            w_copy(i + slots).start()

    base = 0
    for ref in (q_ref, k_ref, v_ref):
        def step(i, _, ref=ref, base=base):
            multiply(base + i, ref[:, pl.ds(pl.multiple_of(i * deep, deep), deep)])
            refill(base + i)
            return 0
        count = ref.shape[1] // deep
        lax.fori_loop(0, count, step, 0)
        base += count
    p = pre[...]
    sig = jax.nn.sigmoid(p)
    act = (p * sig).astype(jnp.bfloat16)
    act_ref[...] = act
    slope_ref[...] = sig * (1.0 + p * (1.0 - sig))
    out = lax.dot_general(w2t_ref[...], act, (((1,), (1,)), ((), ())), preferred_element_type=jnp.float32)
    for g in range(pred_ref.shape[0]):
        pred_ref[g:g + 1, :] = out[g:g + 1, :] + bias_ref[g]

    def pass_on(r, _):
        frm = chip_at(r, -1)
        for i in (1, 2):
            across(i, parts(frm)[i], frm, frm, arrivals(frm)[i]).wait_recv()
            over(i - 1, stage.at[i - 1, frm], frm).start()
        keep(stage.at[1, frm], frm).start()
        return 0
    lax.fori_loop(1, chips, pass_on, 0)

    def settle(r, _):
        frm = chip_at(r, -1)
        to = chip_at(r, 1)
        across(0, parts(frm)[0], frm, frm, arrivals(frm)[0]).wait_recv()
        for i in range(3):
            across(i, parts(to)[i], to, c, arrivals(c)[i]).wait_send()
        return 0
    lax.fori_loop(1, chips, settle, 0)

    def settle_over(at, _):
        for i in range(2):
            dst = (qa.at[2 * at + 1 - core], ka.at[2 * at + 1 - core])[i]
            remote(stage.at[i, at], dst, d_send.at[i, at], d_recv.at[i, at], partner).wait()
        keep(stage.at[1, at], at).wait()
        return 0
    lax.fori_loop(0, chips, settle_over, 0)
    own_copy.wait()


def head(dims, q, k, v, b_in, w2t, bias, w_in, slots=3, deep=512):
    ny, nz, nb = dims
    rows, hidden = q.shape[0], w_in.shape[1]
    heads = w2t.shape[0]
    size = k.shape[1] // heads
    chips = ny * nz
    n = 2 * chips
    vm, anywhere = pltpu.VMEM, pltpu.HBM
    dma = pltpu.SemaphoreType.DMA
    block = lambda space: pl.BlockSpec(memory_space=space)
    return pl.pallas_call(
        functools.partial(head_body, dims, q.shape[1] // k.shape[1]),
        out_shape=(
            jax.ShapeDtypeStruct((n, rows, size), jnp.bfloat16),
            jax.ShapeDtypeStruct((n, rows, size), jnp.bfloat16),
            jax.ShapeDtypeStruct((heads, rows), jnp.float32),
            jax.ShapeDtypeStruct((rows, hidden), jnp.float32),
            jax.ShapeDtypeStruct((rows, hidden), jnp.bfloat16),
        ),
        in_specs=[block(vm)] * 5 + [block(pltpu.SMEM), block(anywhere)],
        out_specs=[block(anywhere)] * 2 + [block(vm)] * 3,
        scratch_shapes=[
            vm((2, chips, rows, size), jnp.bfloat16),
            vm((slots, deep, hidden), jnp.bfloat16),
            vm((rows, hidden), jnp.float32),
            dma((slots,)),
            dma((3, chips)), dma((3, chips)),
            dma((2, chips)), dma((2, chips)),
            dma((chips + 1,)),
        ],
        compiler_params=pltpu.CompilerParams(collective_id=1, has_side_effects=True, vmem_limit_bytes=56 * 2**20),
        cost_estimate=pl.CostEstimate(flops=2 * rows * w_in.shape[0] * hidden, bytes_accessed=16 * 2**20, transcendentals=0),
        name="head",
    )(q, k, v, b_in, w2t, bias, w_in)


def tail_body(dims, norm, order_ref, limit_ref, mass_ref, pred_ref, w2t_ref, slope_ref, act_ref, f_ref, grad_ref, small_ref,
              mrecv, lab, dl, ft, part, pair, xrecv, sm, smr, zs, ys, xs,
              m_send, m_recv, g_send, g_recv, p_send, p_recv, x_send, x_recv, s_send, s_recv):
    ny, nz, nb = dims
    n = ny * nz * 2
    s, b = lax.axis_index("seq"), lax.axis_index("batch")
    core, c = lax.rem(s, 2), s // 2
    z, y = lax.rem(c, nz), c // nz
    rows, hidden = slope_ref.shape
    chunks, tokens, width = dl.shape
    feats = part.shape[1]
    half = feats // 2
    own_rows = half // nb
    partner = (s + 1 - 2 * core, b)

    barrier = pltpu.get_barrier_semaphore()

    def greet(r, _):
        pl.semaphore_signal(barrier, inc=1, device_id=(lax.rem(s + r, n), b), device_id_type=MESH)
        return 0
    lax.fori_loop(1, n, greet, 0)
    for r in range(1, nb):
        pl.semaphore_signal(barrier, inc=1, device_id=(s, lax.rem(b + r, nb)), device_id_type=MESH)
    pl.semaphore_wait(barrier, n - 1 + nb - 1)

    def mass_copy(r, sender):
        to = lax.rem(s + r, n)
        return remote(mass_ref.at[to], mrecv.at[s], m_send.at[r], m_recv.at[s], (to, b))

    def mass_start(r, _):
        mass_copy(r, s).start()
        return 0
    lax.fori_loop(1, n, mass_start, 0)
    mrecv[s] = mass_ref[s]

    for k in range(tokens // rows):
        ft[:, k * rows:(k + 1) * rows] = f_ref[k * rows:(k + 1) * rows, :].T

    def mass_wait(r, _):
        frm = lax.rem(s + n - r, n)
        got = remote(mass_ref.at[frm], mrecv.at[frm], m_send.at[r], m_recv.at[frm], (frm, b))
        got.wait_recv()
        return 0
    lax.fori_loop(1, n, mass_wait, 0)

    heads = lab.shape[0]
    per = n // heads
    for g in range(heads):
        total = mrecv[per * g]
        for i in range(1, per):
            total = total + mrecv[per * g + i]
        lab[g:g + 1, :] = jnp.log1p(total)
    position = order_ref[s] * rows + lax.broadcasted_iota(jnp.int32, (1, rows), 1)
    live = jnp.where(position < limit_ref[0], 1.0, 0.0)
    resid_t = ((pred_ref[...] - lab[...]) * live * norm).astype(jnp.bfloat16)
    resid = resid_t.astype(jnp.float32).T.astype(jnp.bfloat16)
    back = jnp.dot(resid, w2t_ref[...], preferred_element_type=jnp.float32)
    delta = (back * slope_ref[...]).astype(jnp.bfloat16)
    here = pl.ds(pl.multiple_of(c * rows, rows), rows)
    for j in range(chunks):
        dl[j, here, :] = delta[:, j * width:(j + 1) * width]

    wide = rows // 2
    slot = {}

    def number(*key):
        return slot.setdefault(key, len(slot))

    def spot(half_id, a, e):
        return (a * nz + e) if half_id == 0 else (e * nz + a)

    def ring(v, d, size):
        return lax.rem(v + (d + size), size)

    def coords(half_id):
        return (y, z, ny, nz) if half_id == 0 else (z, y, nz, ny)

    def piece(j, block, half_id, quarter):
        r0 = half_id * wide + (quarter * (wide // 2) if quarter is not None else 0)
        size = wide // 2 if quarter is not None else wide
        return dl.at[j, pl.ds(pl.multiple_of(block * rows + r0, wide // 2), size), :]

    def neighbour(half_id, which, d):
        along_y = (half_id == 0) == (which == 0)
        to_y = ring(y, d, ny) if along_y else y
        to_z = z if along_y else ring(z, d, nz)
        return ((to_y * nz + to_z) * 2 + core, b)

    started = []

    def copy(j, half_id, which, da, de, quarter, d):
        a, e, na, ne = coords(half_id)
        block = spot(half_id, ring(a, da, na), ring(e, de, ne))
        ref = piece(j, block, half_id, quarter)
        m = number(j, half_id, which, da, de, quarter, d)
        return remote(ref, ref, g_send.at[m], g_recv.at[m], neighbour(half_id, which, d))

    def send(j, half_id, which, da, de, quarter, d):
        one = copy(j, half_id, which, da, de, quarter, d)
        one.start()
        started.append(one)

    def receive(j, half_id, which, da, de, quarter, d):
        a, e, na, ne = coords(half_id)
        back_a, back_e = (da - d, de) if which == 0 else (da, de - d)
        block = spot(half_id, ring(a, back_a, na), ring(e, back_e, ne))
        ref = piece(j, block, half_id, quarter)
        m = number(j, half_id, which, da, de, quarter, d)
        remote(ref, ref, g_send.at[m], g_recv.at[m], neighbour(half_id, which, -d)).wait_recv()

    def second(j, h, da):
        for d in (1, -1):
            send(j, h, 1, da, 0, None, d)

    def second_pass_on(j, h, da):
        receive(j, h, 1, da, 0, None, 1)
        send(j, h, 1, da, -1, 0, 1)
        receive(j, h, 1, da, 0, None, -1)
        send(j, h, 1, da, 1, 1, -1)

    def second_end(j, h, da):
        receive(j, h, 1, da, -1, 0, 1)
        receive(j, h, 1, da, 1, 1, -1)

    def stage0(j):
        for h in (0, 1):
            for d in (1, -1):
                send(j, h, 0, 0, 0, None, d)
        for h in (0, 1):
            second(j, h, 0)

    def stage1(j):
        for h in (0, 1):
            receive(j, h, 0, 0, 0, None, 1)
            send(j, h, 0, -1, 0, 0, 1)
            second(j, h, -1)
            receive(j, h, 0, 0, 0, None, -1)
            send(j, h, 0, 1, 0, 1, -1)
            second(j, h, 1)

    def stage2(j):
        for h in (0, 1):
            second_pass_on(j, h, 0)
        for h in (0, 1):
            receive(j, h, 0, -1, 0, 0, 1)
            receive(j, h, 0, 1, 0, 1, -1)
            second(j, h, 2)

    def stage3(j):
        for da in (-1, 1):
            for h in (0, 1):
                second_pass_on(j, h, da)

    def stage4(j):
        for h in (0, 1):
            second_pass_on(j, h, 2)

    def stage5(j):
        for da in (0, -1, 1, 2):
            for h in (0, 1):
                second_end(j, h, da)

    def multiply(j):
        part[j] = jnp.dot(ft[...], dl[j], preferred_element_type=jnp.float32)

    def pair_copy(j, of):
        ref = part.at[j, pl.ds(pl.multiple_of((1 - of) * half, half), half), :]
        return remote(ref, pair.at[j], p_send.at[j], p_recv.at[j], partner)

    def pair_start(j):
        one = pair_copy(j, core)
        one.start()
        started.append(one)

    def x_copy(j, r):
        to = lax.rem(b + r, nb)
        ref = pair.at[j, pl.ds(pl.multiple_of(to * own_rows, own_rows), own_rows), :]
        return remote(ref, xrecv.at[j, r - 1], x_send.at[j, r - 1], x_recv.at[j, r - 1], (s, to))

    def x_start(j):
        pair_copy(j, core).wait_recv()
        pair[j] = pair[j] + part[j, pl.ds(pl.multiple_of(core * half, half), half), :]
        for r in (2, 1, 3)[: nb - 1]:
            one = x_copy(j, r)
            one.start()
            started.append(one)

    def x_end(j):
        for r in range(1, nb):
            x_copy(j, r).wait_recv()
        own = pair[j, pl.ds(pl.multiple_of(b * own_rows, own_rows), own_rows), :]
        for r in range(1, nb):
            own = own + xrecv[j, r - 1]
        grad_ref[:, j * width:(j + 1) * width] = own

    def small_start0():
        sw = sm.shape[2]
        out_term = jnp.dot(resid_t, act_ref[...], preferred_element_type=jnp.float32)
        sums = jnp.sum(delta.astype(jnp.float32), axis=0, keepdims=True)
        bias = jnp.sum(resid_t.astype(jnp.float32), axis=1, keepdims=True)
        lanes = 128
        cols = [out_term[:, k * lanes:(k + 1) * lanes] for k in range(hidden // lanes)]
        cols.append(jnp.concatenate([sums[:, k * lanes:(k + 1) * lanes] for k in range(hidden // lanes)], axis=0))
        cols.append(jnp.broadcast_to(bias, (heads, lanes)))
        each = sw // lanes
        for k, value in enumerate(cols):
            sm[k // each, :, (k % each) * lanes:(k % each + 1) * lanes] = value
        one = remote(sm.at[1 - core], smr, s_send.at[0], s_recv.at[0], partner)
        one.start()
        started.append(one)

    def small_hop(level, value, buf, at, size, target):
        buf[at] = value
        for r in range(1, size):
            one = remote(buf.at[at], buf.at[at], s_send.at[level * 3 + r], s_recv.at[level * 3 + r], target(r))
            one.start()
            started.append(one)

    def small_sum(level, buf, at, size, target):
        for r in range(1, size):
            frm = lax.rem(at + size - r, size)
            remote(buf.at[frm], buf.at[frm], s_send.at[level * 3 + r], s_recv.at[level * 3 + r], target(r)).wait_recv()
        total = buf[0]
        for k in range(1, size):
            total = total + buf[k]
        return total

    to_z = lambda r: ((y * nz + lax.rem(z + r, nz)) * 2 + core, b)
    to_y = lambda r: ((lax.rem(y + r, ny) * nz + z) * 2 + core, b)
    to_x = lambda r: (s, lax.rem(b + r, nb))

    def small1():
        remote(sm.at[1 - core], smr, s_send.at[0], s_recv.at[0], partner).wait_recv()
        small_hop(0, sm[core] + smr[...], zs, z, nz, to_z)

    def small2():
        small_hop(1, small_sum(0, zs, z, nz, to_z), ys, y, ny, to_y)

    def small3():
        small_hop(2, small_sum(1, ys, y, ny, to_y), xs, b, nb, to_x)

    def small4():
        sm[core] = small_sum(2, xs, b, nb, to_x)
        one = remote(sm.at[core], small_ref.at[core], s_send.at[10], s_recv.at[10], partner)
        one.start()
        started.append(one)
        small_ref[core] = sm[core]

    def small5():
        remote(sm.at[1 - core], small_ref.at[1 - core], s_send.at[10], s_recv.at[10], partner).wait_recv()

    if chunks == 2:
        stage0(0); small_start0(); stage1(0); stage2(0); stage0(1); stage3(0); small1(); stage1(1); stage4(0)
        stage2(1); stage5(0); small2(); stage3(1)
        multiply(0); pair_start(0); stage4(1); small3()
        x_start(0); stage5(1)
        multiply(1); pair_start(1); small4(); x_end(0); x_start(1); small5(); x_end(1)
    else:
        small = [small1, small2, small3, small4, small5]
        stage0(0); small_start0(); stage1(0); stage2(0)
        for j in range(chunks):
            last = j + 1 == chunks
            if not last:
                stage0(j + 1)
            stage3(j)
            if not last:
                stage1(j + 1)
            stage4(j)
            if not last:
                stage2(j + 1)
            stage5(j)
            if small:
                small.pop(0)()
            multiply(j)
            pair_start(j)
            if small:
                small.pop(0)()
            if j > 0:
                x_end(j - 1)
            x_start(j)
        for one in small:
            one()
        x_end(chunks - 1)

    for one in started:
        one.wait_send()

    def mass_drain(r, _):
        mass_copy(r, s).wait_send()
        return 0
    lax.fori_loop(1, n, mass_drain, 0)


def tail(dims, norm, order, limit, mass, pred_t, w2t, slope, act, f, chunks=2):
    ny, nz, nb = dims
    n = mass.shape[0]
    rows, hidden = slope.shape
    tokens, feats = f.shape
    heads = pred_t.shape[0]
    width = hidden // chunks
    half = feats // 2
    sw = (hidden + 256) // 2
    vm = pltpu.VMEM
    dma = pltpu.SemaphoreType.DMA
    return pl.pallas_call(
        functools.partial(tail_body, dims, norm),
        out_shape=(
            jax.ShapeDtypeStruct((half // nb, hidden), jnp.float32),
            jax.ShapeDtypeStruct((2, heads, sw), jnp.float32),
        ),
        in_specs=[pl.BlockSpec(memory_space=pltpu.SMEM)] * 2 + [pl.BlockSpec(memory_space=vm)] * 6,
        out_specs=[pl.BlockSpec(memory_space=vm)] * 2,
        scratch_shapes=[
            vm((n, 1, rows), jnp.float32),
            vm((heads, rows), jnp.float32),
            vm((chunks, tokens, width), jnp.bfloat16),
            vm((feats, tokens), jnp.bfloat16),
            vm((chunks, feats, width), jnp.float32),
            vm((chunks, half, width), jnp.float32),
            vm((chunks, nb - 1, half // nb, width), jnp.float32),
            vm((2, heads, sw), jnp.float32),
            vm((heads, sw), jnp.float32),
            vm((nz, heads, sw), jnp.float32),
            vm((ny, heads, sw), jnp.float32),
            vm((nb, heads, sw), jnp.float32),
            dma((n,)), dma((n,)),
            dma((chunks * 40,)), dma((chunks * 40,)),
            dma((chunks,)), dma((chunks,)),
            dma((chunks, nb - 1)), dma((chunks, nb - 1)),
            dma((12,)), dma((12,)),
        ],
        compiler_params=pltpu.CompilerParams(collective_id=3, has_side_effects=True, vmem_limit_bytes=56 * 2**20),
        cost_estimate=pl.CostEstimate(flops=2 * tokens * feats * hidden, bytes_accessed=8 * 2**20, transcendentals=0),
        name="tail",
    )(order, limit, mass, pred_t, w2t, slope, act, f)


def on_device(dims, queries, keys, values, lengths, block_pos, w_in, b_in, output_weight, output_bias):
    q_rows, k_rows, v_rows = queries[0], keys[0], values[0]
    rows = q_rows.shape[0]
    hidden, heads_kv = output_weight.shape
    n = lax.axis_size("seq")
    total = n * rows
    w2t = output_weight.T
    q_all, k_all, pred_t, slope, act = head(
        dims, q_rows, k_rows, v_rows, b_in[None, :], w2t, output_bias, w_in
    )
    features = jnp.concatenate([q_rows, k_rows, v_rows], axis=1)
    chips = n // 2
    cols = features.shape[1] // chips
    f_send = features.reshape(rows, chips, cols).transpose(1, 0, 2)
    f_send, pred_t = lax.optimization_barrier((f_send, pred_t))
    planes = [[2 * i + core for i in range(chips)] for core in range(2)]
    f_mine = lax.all_to_all(
        f_send, "seq", 0, 0, tiled=True, axis_index_groups=planes
    ).reshape(chips * rows, cols)
    mass_own = attention(block_pos[0], lengths, q_all, k_all, 512, 512, 64)
    norm = 1.0 / math.sqrt(lax.axis_size("batch") * total)
    grad_w_in, small = tail(dims, norm, block_pos[0], lengths, mass_own, pred_t, w2t, slope, act, f_mine)
    small = jnp.concatenate([small[0], small[1]], axis=1)
    grad_b_in = small[:, hidden:hidden + 128].reshape(hidden)
    return (grad_w_in, grad_b_in, small[:, :hidden].T, small[:, hidden + 128])


def solution(mesh):
    nb = mesh.shape["batch"]
    ny = nz = math.isqrt(mesh.shape["seq"] // 2)
    return jax.shard_map(
        functools.partial(on_device, (ny, nz, nb)),
        mesh=mesh,
        in_specs=(
            P("batch", "seq", None),
            P("batch", "seq", None),
            P("batch", "seq", None),
            P("batch"),
            P("batch", None),
            P(),
            P(),
            P(),
            P(),
        ),
        out_specs=(P(("seq", "batch"), None), P(), P(), P()),
        check_vma=False,
    )
```

```python
import functools, math
import jax, jax.numpy as jnp
from jax import lax
from jax.experimental import pallas as pl
from jax.experimental.pallas import tpu as pltpu
from jax.sharding import PartitionSpec as P
NEG = -1e30

def attn_core(tq, sub, total, scale2, limit, qs, ks, s_ref, acc_ref):
    lanes = 128
    groups = tq // lanes
    nt = total // tq
    eights = lambda x: x.reshape(x.shape[0] // 8, 8, tq)

    def at(j, n=tq):
        return pl.ds(pl.multiple_of(j * n, n), n)

    def scores(i, j, mx, masked):
        s = lax.dot_general(ks[at(j), :], qs[at(i), :], (((1,), (1,)), ((), ())), preferred_element_type=jnp.float32)
        if masked:
            kp = lax.broadcasted_iota(jnp.int32, (tq, tq), 0)
            qp = lax.broadcasted_iota(jnp.int32, (tq, tq), 1)
            s = jnp.where(kp <= qp, s, NEG)
        s_ref[lax.rem(i, 3), at(j), :] = s
        return jnp.maximum(mx, jnp.max(eights(s), axis=0))

    def weights(i, j, l, top):
        for u in range(tq // sub):
            here = pl.ds(pl.multiple_of(j * tq + u * sub, sub), sub)
            w = jnp.exp2((eights(s_ref[lax.rem(i, 3), here, :]) - top[None]) * scale2)
            s_ref[lax.rem(i, 3), here, :] = w.reshape(sub, tq)
            l = l + jnp.sum(w, axis=0)
        return l

    def shares(i, j, rec):
        for u in range(tq // sub):
            here = pl.ds(pl.multiple_of(j * tq + u * sub, sub), sub)
            w = (eights(s_ref[lax.rem(i, 3), here, :]) * rec[None]).reshape(sub, tq)
            tot = w[:, :lanes]
            for g in range(1, groups):
                tot = tot + w[:, g * lanes:(g + 1) * lanes]
            acc_ref[here, :] += tot

    none = jnp.full((8, tq), NEG, jnp.float32)
    zero = jnp.zeros((8, tq), jnp.float32)

    def spread_top(mx):
        return jnp.broadcast_to(jnp.max(mx, axis=0, keepdims=True), (8, tq))

    def spread_rec(i, l):
        pos = i * tq + lax.broadcasted_iota(jnp.int32, (1, tq), 1)
        rec = jnp.where(pos < limit, 1.0 / jnp.sum(l, axis=0, keepdims=True), 0.0)
        return jnp.broadcast_to(rec, (8, tq))

    def step(i, top, rec, with_scores=True, with_weights=True, with_shares=True):
        def each(j, carry):
            mx, l = carry
            if with_scores:
                mx = scores(i, j, mx, False)
            if with_weights:
                l = weights(i + 1, j, l, top)
            if with_shares:
                shares(i + 2, j, rec)
            return mx, l
        mx, l = lax.fori_loop(0, i, each, (none, zero))
        if with_scores:
            mx = scores(i, i, mx, True)
        if with_weights:
            for d in (0, 1):
                if with_scores or d:
                    l = weights(i + 1, i + d, l, top)
        if with_shares:
            for d in (0, 1, 2):
                if with_scores or with_weights and d or d == 2:
                    shares(i + 2, i + d, rec)
        return mx, l

    last = nt - 1
    mx, _ = step(last, none, none, True, False, False)
    mx, l = step(last - 1, spread_top(mx), none, True, True, False)

    def generic(t, carry):
        top, rec = carry
        i = last - t
        mx, l = step(i, top, rec)
        return spread_top(mx), spread_rec(i + 1, l)
    top, rec = lax.fori_loop(2, nt, generic, (spread_top(mx), spread_rec(last, l)))
    _, l = step(-1, top, rec, False, True, True)
    step(-2, none, spread_rec(0, l), False, False, True)


def attn_body(tq, sub, blocks, rows, scale2, order_ref, limit_ref, q_hbm, k_hbm, out_ref, qs, ks, s_ref, acc_ref, sems):
    total = blocks * rows
    def issue(s, _):
        p = order_ref[s]
        dst = pl.ds(pl.multiple_of(p * rows, rows), rows)
        pltpu.make_async_copy(q_hbm.at[s], qs.at[dst], sems.at[0]).start()
        pltpu.make_async_copy(k_hbm.at[s], ks.at[dst], sems.at[1]).start()
        return 0
    lax.fori_loop(0, blocks, issue, 0)
    acc_ref[...] = jnp.zeros_like(acc_ref)
    for src, dst, i in ((q_hbm, qs, 0), (k_hbm, ks, 1)):
        pltpu.make_async_copy(src, src, sems.at[i]).wait()
    attn_core(tq, sub, total, scale2, limit_ref[0], qs, ks, s_ref, acc_ref)

    def emit(s, _):
        p = order_ref[s]
        part = acc_ref[pl.ds(pl.multiple_of(p * rows, rows), rows), :]
        out_ref[s] = jnp.sum(part.T, axis=0, keepdims=True)
        return 0
    lax.fori_loop(0, blocks, emit, 0)


def attention(order, limit, q_all, k_all, tq=512, sub=64):
    blocks, rows, head = q_all.shape
    total = blocks * rows
    scale2 = math.log2(math.e) / math.sqrt(head)
    return pl.pallas_call(
        functools.partial(attn_body, tq, sub, blocks, rows, scale2),
        out_shape=jax.ShapeDtypeStruct((blocks, 1, rows), jnp.float32),
        in_specs=[pl.BlockSpec(memory_space=pltpu.SMEM)] * 2 + [pl.BlockSpec(memory_space=pltpu.HBM)] * 2,
        out_specs=pl.BlockSpec(memory_space=pltpu.VMEM),
        scratch_shapes=[
            pltpu.VMEM((total, head), jnp.bfloat16),
            pltpu.VMEM((total, head), jnp.bfloat16),
            pltpu.VMEM((3, total, tq), jnp.float32),
            pltpu.VMEM((total, 128), jnp.float32),
            pltpu.SemaphoreType.DMA((2,)),
        ],
        compiler_params=pltpu.CompilerParams(vmem_limit_bytes=56 * 2**20),
        cost_estimate=pl.CostEstimate(flops=total * total * head, bytes_accessed=4 * total * head, transcendentals=total * total // 2),
        name="mass",
    )(order, limit, q_all, k_all)


MESH = pl.DeviceIdType.MESH


def remote(src, dst, send_sem, recv_sem, device):
    return pltpu.make_async_remote_copy(
        src_ref=src, dst_ref=dst, send_sem=send_sem, recv_sem=recv_sem, device_id=device, device_id_type=MESH
    )


def head_body(dims, per, q_ref, k_ref, v_ref, bin_ref, w2t_ref, bias_ref, w_hbm, qa, ka, pred_ref, slope_ref, act_ref,
              stage, wbuf, pre, w_sem, i_send, i_recv, d_send, d_recv, l_sem):
    ny, nz, nb = dims
    chips = ny * nz
    s, b = lax.axis_index("seq"), lax.axis_index("batch")
    core, c = lax.rem(s, 2), s // 2
    z, y = lax.rem(c, nz), c // nz
    partner = (s + 1 - 2 * core, b)
    head = ka.shape[2]
    slots, deep, hidden = wbuf.shape
    steps = w_hbm.shape[0] // deep

    def w_copy(i):
        at = lax.rem(i, slots)
        return pltpu.make_async_copy(w_hbm.at[pl.ds(pl.multiple_of(i * deep, deep), deep), :], wbuf.at[at], w_sem.at[at])

    for i in range(slots):
        w_copy(i).start()

    def chip_at(r, sign):
        dy, dz = r // nz, lax.rem(r, nz)
        return lax.rem(y + sign * dy + ny, ny) * nz + lax.rem(z + sign * dz + nz, nz)

    barrier = pltpu.get_barrier_semaphore()

    def greet(r, _):
        pl.semaphore_signal(barrier, inc=1, device_id=(2 * chip_at(r, 1) + core, b), device_id_type=MESH)
        return 0
    lax.fori_loop(1, chips, greet, 0)
    pl.semaphore_signal(barrier, inc=1, device_id=partner, device_id_type=MESH)
    pl.semaphore_wait(barrier, chips)

    def columns(ref, i):
        return ref.at[:, pl.ds(pl.multiple_of(i * head, head), head)]

    def parts(to):
        return (columns(q_ref, 2 * to + core), columns(q_ref, 2 * to + 1 - core), columns(k_ref, (2 * to) // per))

    def arrivals(frm):
        return (qa.at[2 * frm + core], stage.at[0, frm], stage.at[1, frm])

    def across(i, src, to, frm, dst):
        return remote(src, dst, i_send.at[i, to], i_recv.at[i, frm], (2 * to + core, b))

    def send(r, _):
        to = chip_at(r, 1)
        for i in (1, 2, 0):
            across(i, parts(to)[i], to, c, arrivals(c)[i]).start()
        return 0
    lax.fori_loop(1, chips, send, 0)

    def over(i, src, at):
        dst = (qa.at[2 * at + core], ka.at[2 * at + core])[i]
        return remote(src, dst, d_send.at[i, at], d_recv.at[i, at], partner)

    def keep(src, at):
        return pltpu.make_async_copy(src, ka.at[2 * at + core], l_sem.at[at])

    own_q, other_q, own_k = parts(c)
    over(0, other_q, c).start()
    over(1, own_k, c).start()
    keep(own_k, c).start()
    own_copy = pltpu.make_async_copy(own_q, qa.at[2 * c + core], l_sem.at[chips])
    own_copy.start()

    pre[...] = jnp.broadcast_to(bin_ref[...], pre.shape)

    def multiply(i, x):
        w_copy(i).wait()
        pre[...] += jnp.dot(x, wbuf[lax.rem(i, slots)], preferred_element_type=jnp.float32)

    def refill(i):
        @pl.when(i + slots < steps)
        def _():
            w_copy(i + slots).start()

    base = 0
    for ref in (q_ref, k_ref, v_ref):
        def step(i, _, ref=ref, base=base):
            multiply(base + i, ref[:, pl.ds(pl.multiple_of(i * deep, deep), deep)])
            refill(base + i)
            return 0
        count = ref.shape[1] // deep
        lax.fori_loop(0, count, step, 0)
        base += count
    p = pre[...]
    sig = jax.nn.sigmoid(p)
    act = (p * sig).astype(jnp.bfloat16)
    act_ref[...] = act
    slope_ref[...] = sig * (1.0 + p * (1.0 - sig))
    out = lax.dot_general(w2t_ref[...], act, (((1,), (1,)), ((), ())), preferred_element_type=jnp.float32)
    for g in range(pred_ref.shape[0]):
        pred_ref[g:g + 1, :] = out[g:g + 1, :] + bias_ref[g]

    def pass_on(r, _):
        frm = chip_at(r, -1)
        for i in (1, 2):
            across(i, parts(frm)[i], frm, frm, arrivals(frm)[i]).wait_recv()
            over(i - 1, stage.at[i - 1, frm], frm).start()
        keep(stage.at[1, frm], frm).start()
        return 0
    lax.fori_loop(1, chips, pass_on, 0)

    def settle(r, _):
        frm = chip_at(r, -1)
        to = chip_at(r, 1)
        across(0, parts(frm)[0], frm, frm, arrivals(frm)[0]).wait_recv()
        for i in range(3):
            across(i, parts(to)[i], to, c, arrivals(c)[i]).wait_send()
        return 0
    lax.fori_loop(1, chips, settle, 0)

    def settle_over(at, _):
        for i in range(2):
            dst = (qa.at[2 * at + 1 - core], ka.at[2 * at + 1 - core])[i]
            remote(stage.at[i, at], dst, d_send.at[i, at], d_recv.at[i, at], partner).wait()
        keep(stage.at[1, at], at).wait()
        return 0
    lax.fori_loop(0, chips, settle_over, 0)
    own_copy.wait()


def head(dims, q, k, v, b_in, w2t, bias, w_in, slots=3, deep=512):
    ny, nz, nb = dims
    rows, hidden = q.shape[0], w_in.shape[1]
    heads = w2t.shape[0]
    size = k.shape[1] // heads
    chips = ny * nz
    n = 2 * chips
    vm, anywhere = pltpu.VMEM, pltpu.HBM
    dma = pltpu.SemaphoreType.DMA
    block = lambda space: pl.BlockSpec(memory_space=space)
    return pl.pallas_call(
        functools.partial(head_body, dims, q.shape[1] // k.shape[1]),
        out_shape=(
            jax.ShapeDtypeStruct((n, rows, size), jnp.bfloat16),
            jax.ShapeDtypeStruct((n, rows, size), jnp.bfloat16),
            jax.ShapeDtypeStruct((heads, rows), jnp.float32),
            jax.ShapeDtypeStruct((rows, hidden), jnp.float32),
            jax.ShapeDtypeStruct((rows, hidden), jnp.bfloat16),
        ),
        in_specs=[block(vm)] * 5 + [block(pltpu.SMEM), block(anywhere)],
        out_specs=[block(anywhere)] * 2 + [block(vm)] * 3,
        scratch_shapes=[
            vm((2, chips, rows, size), jnp.bfloat16),
            vm((slots, deep, hidden), jnp.bfloat16),
            vm((rows, hidden), jnp.float32),
            dma((slots,)),
            dma((3, chips)), dma((3, chips)),
            dma((2, chips)), dma((2, chips)),
            dma((chips + 1,)),
        ],
        compiler_params=pltpu.CompilerParams(collective_id=1, has_side_effects=True, vmem_limit_bytes=56 * 2**20),
        cost_estimate=pl.CostEstimate(flops=2 * rows * w_in.shape[0] * hidden, bytes_accessed=16 * 2**20, transcendentals=0),
        name="head",
    )(q, k, v, b_in, w2t, bias, w_in)


def tail_body(dims, norm, order_ref, limit_ref, mass_ref, pred_ref, w2t_ref, slope_ref, act_ref, f_ref, grad_ref, ow_ref, b_ref, bias_ref,
              mrecv, lab, dl, ft, part, pair, xrecv, sm, small, smr, zs, ys, xs,
              m_send, m_recv, g_send, g_recv, p_send, p_recv, x_send, x_recv, s_send, s_recv):
    ny, nz, nb = dims
    n = ny * nz * 2
    s, b = lax.axis_index("seq"), lax.axis_index("batch")
    core, c = lax.rem(s, 2), s // 2
    z, y = lax.rem(c, nz), c // nz
    rows, hidden = slope_ref.shape
    chunks, tokens = len(dl), dl[0].shape[0]
    feats = part[0].shape[0]
    begin = [sum(d.shape[1] for d in dl[:j]) for j in range(chunks + 1)]
    half = feats // 2
    own_rows = half // nb
    partner = (s + 1 - 2 * core, b)

    barrier = pltpu.get_barrier_semaphore()

    def greet(r, _):
        pl.semaphore_signal(barrier, inc=1, device_id=(lax.rem(s + r, n), b), device_id_type=MESH)
        return 0
    lax.fori_loop(1, n, greet, 0)
    for r in range(1, nb):
        pl.semaphore_signal(barrier, inc=1, device_id=(s, lax.rem(b + r, nb)), device_id_type=MESH)
    pl.semaphore_wait(barrier, n - 1 + nb - 1)

    def mass_copy(r, sender):
        to = lax.rem(s + r, n)
        return remote(mass_ref.at[to], mrecv.at[s], m_send.at[r], m_recv.at[s], (to, b))

    def mass_start(r, _):
        mass_copy(r, s).start()
        return 0
    lax.fori_loop(1, n, mass_start, 0)
    mrecv[s] = mass_ref[s]

    for k in range(tokens // rows):
        ft[:, k * rows:(k + 1) * rows] = f_ref[k * rows:(k + 1) * rows, :].T

    def mass_wait(r, _):
        frm = lax.rem(s + n - r, n)
        got = remote(mass_ref.at[frm], mrecv.at[frm], m_send.at[r], m_recv.at[frm], (frm, b))
        got.wait_recv()
        return 0
    lax.fori_loop(1, n, mass_wait, 0)

    heads = lab.shape[0]
    per = n // heads
    for g in range(heads):
        total = mrecv[per * g]
        for i in range(1, per):
            total = total + mrecv[per * g + i]
        lab[g:g + 1, :] = jnp.log1p(total)
    position = order_ref[s] * rows + lax.broadcasted_iota(jnp.int32, (1, rows), 1)
    live = jnp.where(position < limit_ref[0], 1.0, 0.0)
    resid_t = ((pred_ref[...] - lab[...]) * live * norm).astype(jnp.bfloat16)
    resid = resid_t.astype(jnp.float32).T.astype(jnp.bfloat16)
    back = jnp.dot(resid, w2t_ref[...], preferred_element_type=jnp.float32)
    delta = (back * slope_ref[...]).astype(jnp.bfloat16)
    here = pl.ds(pl.multiple_of(c * rows, rows), rows)
    for j in range(chunks):
        dl[j][here, :] = delta[:, begin[j]:begin[j + 1]]

    wide = rows // 2
    slot = {}

    def number(*key):
        return slot.setdefault(key, len(slot))

    def spot(half_id, a, e):
        return (a * nz + e) if half_id == 0 else (e * nz + a)

    def ring(v, d, size):
        return lax.rem(v + (d + size), size)

    def coords(half_id):
        return (y, z, ny, nz) if half_id == 0 else (z, y, nz, ny)

    def piece(j, block, half_id, quarter):
        r0 = half_id * wide + (quarter * (wide // 2) if quarter is not None else 0)
        size = wide // 2 if quarter is not None else wide
        return dl[j].at[pl.ds(pl.multiple_of(block * rows + r0, wide // 2), size), :]

    def neighbour(half_id, which, d):
        along_y = (half_id == 0) == (which == 0)
        to_y = ring(y, d, ny) if along_y else y
        to_z = z if along_y else ring(z, d, nz)
        return ((to_y * nz + to_z) * 2 + core, b)

    started = []

    def copy(j, half_id, which, da, de, quarter, d):
        a, e, na, ne = coords(half_id)
        block = spot(half_id, ring(a, da, na), ring(e, de, ne))
        ref = piece(j, block, half_id, quarter)
        m = number(j, half_id, which, da, de, quarter, d)
        return remote(ref, ref, g_send.at[m], g_recv.at[m], neighbour(half_id, which, d))

    def send(j, half_id, which, da, de, quarter, d):
        one = copy(j, half_id, which, da, de, quarter, d)
        one.start()
        started.append(one)

    def receive(j, half_id, which, da, de, quarter, d):
        a, e, na, ne = coords(half_id)
        back_a, back_e = (da - d, de) if which == 0 else (da, de - d)
        block = spot(half_id, ring(a, back_a, na), ring(e, back_e, ne))
        ref = piece(j, block, half_id, quarter)
        m = number(j, half_id, which, da, de, quarter, d)
        remote(ref, ref, g_send.at[m], g_recv.at[m], neighbour(half_id, which, -d)).wait_recv()

    def second(j, h, da):
        for d in (1, -1):
            send(j, h, 1, da, 0, None, d)

    def second_pass_on(j, h, da):
        receive(j, h, 1, da, 0, None, 1)
        send(j, h, 1, da, -1, 0, 1)
        receive(j, h, 1, da, 0, None, -1)
        send(j, h, 1, da, 1, 1, -1)

    def second_end(j, h, da):
        receive(j, h, 1, da, -1, 0, 1)
        receive(j, h, 1, da, 1, 1, -1)

    def stage0(j):
        for h in (0, 1):
            for d in (1, -1):
                send(j, h, 0, 0, 0, None, d)
        for h in (0, 1):
            second(j, h, 0)

    def stage1(j):
        for h in (0, 1):
            receive(j, h, 0, 0, 0, None, 1)
            send(j, h, 0, -1, 0, 0, 1)
            second(j, h, -1)
            receive(j, h, 0, 0, 0, None, -1)
            send(j, h, 0, 1, 0, 1, -1)
            second(j, h, 1)

    def stage2(j):
        for h in (0, 1):
            second_pass_on(j, h, 0)
        for h in (0, 1):
            receive(j, h, 0, -1, 0, 0, 1)
            receive(j, h, 0, 1, 0, 1, -1)
            second(j, h, 2)

    def stage3(j):
        for da in (-1, 1):
            for h in (0, 1):
                second_pass_on(j, h, da)

    def stage4(j):
        for h in (0, 1):
            second_pass_on(j, h, 2)

    def stage5(j):
        for da in (0, -1, 1, 2):
            for h in (0, 1):
                second_end(j, h, da)

    def multiply(j):
        part[j][...] = jnp.dot(ft[...], dl[j][...], preferred_element_type=jnp.float32)

    def pair_copy(j, of):
        ref = part[j].at[pl.ds(pl.multiple_of((1 - of) * half, half), half), :]
        return remote(ref, pair[j], p_send.at[j], p_recv.at[j], partner)

    def pair_start(j):
        one = pair_copy(j, core)
        one.start()
        started.append(one)

    def x_copy(j, r):
        to = lax.rem(b + r, nb)
        ref = pair[j].at[pl.ds(pl.multiple_of(to * own_rows, own_rows), own_rows), :]
        return remote(ref, xrecv[j].at[r - 1], x_send.at[j, r - 1], x_recv.at[j, r - 1], (s, to))

    def x_start(j):
        pair_copy(j, core).wait_recv()
        pair[j][...] = pair[j][...] + part[j][pl.ds(pl.multiple_of(core * half, half), half), :]
        for r in (2, 1, 3)[: nb - 1]:
            one = x_copy(j, r)
            one.start()
            started.append(one)

    def x_end(j):
        for r in range(1, nb):
            x_copy(j, r).wait_recv()
        own = pair[j][pl.ds(pl.multiple_of(b * own_rows, own_rows), own_rows), :]
        for r in range(1, nb):
            own = own + xrecv[j][r - 1]
        grad_ref[:, begin[j]:begin[j + 1]] = own

    def small_start0():
        sw = sm.shape[2]
        out_term = jnp.dot(resid_t, act_ref[...], preferred_element_type=jnp.float32)
        sums = jnp.sum(delta.astype(jnp.float32), axis=0, keepdims=True)
        bias = jnp.sum(resid.astype(jnp.float32), axis=0, keepdims=True)
        lanes = 128
        cols = [out_term[:, k * lanes:(k + 1) * lanes] for k in range(hidden // lanes)]
        cols.append(jnp.concatenate([sums[:, k * lanes:(k + 1) * lanes] for k in range(hidden // lanes)], axis=0))
        cols.append(jnp.zeros((heads, lanes), jnp.float32))
        each = sw // lanes
        for k, value in enumerate(cols):
            sm[k // each, :, (k % each) * lanes:(k % each + 1) * lanes] = value
        at = (len(cols) - 1) % each * lanes
        sm[1, 0:1, at:at + heads] = bias
        one = remote(sm.at[1 - core], smr, s_send.at[0], s_recv.at[0], partner)
        one.start()
        started.append(one)

    def small_hop(level, value, buf, at, size, target):
        buf[at] = value
        for r in range(1, size):
            one = remote(buf.at[at], buf.at[at], s_send.at[level * 3 + r], s_recv.at[level * 3 + r], target(r))
            one.start()
            started.append(one)

    def small_sum(level, buf, at, size, target):
        for r in range(1, size):
            frm = lax.rem(at + size - r, size)
            remote(buf.at[frm], buf.at[frm], s_send.at[level * 3 + r], s_recv.at[level * 3 + r], target(r)).wait_recv()
        total = buf[0]
        for k in range(1, size):
            total = total + buf[k]
        return total

    to_z = lambda r: ((y * nz + lax.rem(z + r, nz)) * 2 + core, b)
    to_y = lambda r: ((lax.rem(y + r, ny) * nz + z) * 2 + core, b)
    to_x = lambda r: (s, lax.rem(b + r, nb))

    def small1():
        remote(sm.at[1 - core], smr, s_send.at[0], s_recv.at[0], partner).wait_recv()
        small_hop(0, sm[core] + smr[...], zs, z, nz, to_z)

    def small2():
        small_hop(1, small_sum(0, zs, z, nz, to_z), ys, y, ny, to_y)

    def small3():
        small_hop(2, small_sum(1, ys, y, ny, to_y), xs, b, nb, to_x)

    def small4():
        sm[core] = small_sum(2, xs, b, nb, to_x)
        one = remote(sm.at[core], small.at[core], s_send.at[10], s_recv.at[10], partner)
        one.start()
        started.append(one)
        small[core] = sm[core]

    def small5():
        remote(sm.at[1 - core], small.at[1 - core], s_send.at[10], s_recv.at[10], partner).wait_recv()
        sw = small.shape[2]
        ow_ref[:, :sw] = small[0]
        ow_ref[:, sw:] = small[1, :, :hidden - sw]
        b_ref[...] = small[1, :, hidden - sw:hidden - sw + 128]
        bias_ref[...] = small[1, 0:1, hidden - sw + 128:hidden - sw + 128 + heads]

    stage0(0); small_start0(); stage1(0); stage2(0); stage0(1); stage3(0); small1(); stage1(1); stage4(0)
    stage2(1); stage5(0); small2(); stage3(1)
    multiply(0); pair_start(0); stage4(1); small3()
    x_start(0); stage5(1)
    multiply(1); pair_start(1); small4(); x_end(0); x_start(1); small5(); x_end(1)

    for one in started:
        one.wait_send()

    def mass_drain(r, _):
        mass_copy(r, s).wait_send()
        return 0
    lax.fori_loop(1, n, mass_drain, 0)


def tail(dims, norm, order, limit, mass, pred_t, w2t, slope, act, f, widths=(640, 384)):
    ny, nz, nb = dims
    n = mass.shape[0]
    rows, hidden = slope.shape
    tokens, feats = f.shape
    heads = pred_t.shape[0]
    chunks = len(widths)
    half = feats // 2
    sw = (hidden + 256) // 2
    vm = pltpu.VMEM
    dma = pltpu.SemaphoreType.DMA
    return pl.pallas_call(
        functools.partial(tail_body, dims, norm),
        out_shape=(
            jax.ShapeDtypeStruct((half // nb, hidden), jnp.float32),
            jax.ShapeDtypeStruct((heads, hidden), jnp.float32),
            jax.ShapeDtypeStruct((heads, 128), jnp.float32),
            jax.ShapeDtypeStruct((1, heads), jnp.float32),
        ),
        in_specs=[pl.BlockSpec(memory_space=pltpu.SMEM)] * 2 + [pl.BlockSpec(memory_space=vm)] * 6,
        out_specs=[pl.BlockSpec(memory_space=vm)] * 4,
        scratch_shapes=[
            vm((n, 1, rows), jnp.float32),
            vm((heads, rows), jnp.float32),
            tuple(vm((tokens, w), jnp.bfloat16) for w in widths),
            vm((feats, tokens), jnp.bfloat16),
            tuple(vm((feats, w), jnp.float32) for w in widths),
            tuple(vm((half, w), jnp.float32) for w in widths),
            tuple(vm((nb - 1, half // nb, w), jnp.float32) for w in widths),
            vm((2, heads, sw), jnp.float32),
            vm((2, heads, sw), jnp.float32),
            vm((heads, sw), jnp.float32),
            vm((nz, heads, sw), jnp.float32),
            vm((ny, heads, sw), jnp.float32),
            vm((nb, heads, sw), jnp.float32),
            dma((n,)), dma((n,)),
            dma((chunks * 40,)), dma((chunks * 40,)),
            dma((chunks,)), dma((chunks,)),
            dma((chunks, nb - 1)), dma((chunks, nb - 1)),
            dma((12,)), dma((12,)),
        ],
        compiler_params=pltpu.CompilerParams(collective_id=3, has_side_effects=True, vmem_limit_bytes=56 * 2**20),
        cost_estimate=pl.CostEstimate(flops=2 * tokens * feats * hidden, bytes_accessed=8 * 2**20, transcendentals=0),
        name="tail",
    )(order, limit, mass, pred_t, w2t, slope, act, f)


def on_device(dims, queries, keys, values, lengths, block_pos, w_in, b_in, output_weight, output_bias):
    q_rows, k_rows, v_rows = queries[0], keys[0], values[0]
    rows = q_rows.shape[0]
    hidden, heads_kv = output_weight.shape
    n = lax.axis_size("seq")
    total = n * rows
    w2t = output_weight.T
    q_all, k_all, pred_t, slope, act = head(
        dims, q_rows, k_rows, v_rows, b_in[None, :], w2t, output_bias, w_in
    )
    features = jnp.concatenate([q_rows, k_rows, v_rows], axis=1)
    chips = n // 2
    cols = features.shape[1] // chips
    f_send = features.reshape(rows, chips, cols).transpose(1, 0, 2)
    f_send, pred_t = lax.optimization_barrier((f_send, pred_t))
    planes = [[2 * i + core for i in range(chips)] for core in range(2)]
    f_mine = lax.all_to_all(
        f_send, "seq", 0, 0, tiled=True, axis_index_groups=planes
    ).reshape(chips * rows, cols)
    mass_own = attention(block_pos[0], lengths, q_all, k_all, 512, 128)
    norm = 1.0 / math.sqrt(lax.axis_size("batch") * total)
    grad_w_in, ow, gb, bias = tail(dims, norm, block_pos[0], lengths, mass_own, pred_t, w2t, slope, act, f_mine)
    return (grad_w_in, gb.reshape(hidden), ow.T, bias.reshape(heads_kv))


def solution(mesh):
    nb = mesh.shape["batch"]
    ny = nz = math.isqrt(mesh.shape["seq"] // 2)
    return jax.shard_map(
        functools.partial(on_device, (ny, nz, nb)),
        mesh=mesh,
        in_specs=(
            P("batch", "seq", None),
            P("batch", "seq", None),
            P("batch", "seq", None),
            P("batch"),
            P("batch", None),
            P(),
            P(),
            P(),
            P(),
        ),
        out_specs=(P(("seq", "batch"), None), P(), P(), P()),
        check_vma=False,
    )
```

```python
import functools
import math

import jax
import jax.numpy as jnp
from jax import lax
from jax.experimental import pallas as pl
from jax.experimental.pallas import tpu as pltpu
from jax.sharding import PartitionSpec as P

NEG = -1e30
MESH = pl.DeviceIdType.MESH


def remote(src, dst, send_sem, recv_sem, device):
    return pltpu.make_async_remote_copy(
        src_ref=src, dst_ref=dst, send_sem=send_sem, recv_sem=recv_sem, device_id=device, device_id_type=MESH
    )


def attn_core(tq, sub, total, scale2, limit, qs, ks, s_ref, acc_ref):
    lanes = 128
    groups = tq // lanes
    nt = total // tq
    eights = lambda x: x.reshape(x.shape[0] // 8, 8, tq)

    def at(j, n=tq):
        return pl.ds(pl.multiple_of(j * n, n), n)

    def scores(i, j, mx, masked):
        s = lax.dot_general(ks[at(j), :], qs[at(i), :], (((1,), (1,)), ((), ())), preferred_element_type=jnp.float32)
        if masked:
            kp = lax.broadcasted_iota(jnp.int32, (tq, tq), 0)
            qp = lax.broadcasted_iota(jnp.int32, (tq, tq), 1)
            s = jnp.where(kp <= qp, s, NEG)
        s_ref[lax.rem(i, 3), at(j), :] = s
        return jnp.maximum(mx, jnp.max(eights(s), axis=0))

    def weights(i, j, l, top):
        for u in range(tq // sub):
            here = pl.ds(pl.multiple_of(j * tq + u * sub, sub), sub)
            w = jnp.exp2((eights(s_ref[lax.rem(i, 3), here, :]) - top[None]) * scale2)
            s_ref[lax.rem(i, 3), here, :] = w.reshape(sub, tq)
            l = l + jnp.sum(w, axis=0)
        return l

    def shares(i, j, rec):
        for u in range(tq // sub):
            here = pl.ds(pl.multiple_of(j * tq + u * sub, sub), sub)
            w = (eights(s_ref[lax.rem(i, 3), here, :]) * rec[None]).reshape(sub, tq)
            tot = w[:, :lanes]
            for g in range(1, groups):
                tot = tot + w[:, g * lanes:(g + 1) * lanes]
            acc_ref[j * (tq // sub) + u] += tot

    none = jnp.full((8, tq), NEG, jnp.float32)
    zero = jnp.zeros((8, tq), jnp.float32)

    def spread_top(mx):
        return jnp.broadcast_to(jnp.max(mx, axis=0, keepdims=True), (8, tq))

    def spread_rec(i, l):
        pos = i * tq + lax.broadcasted_iota(jnp.int32, (1, tq), 1)
        rec = jnp.where(pos < limit, 1.0 / jnp.sum(l, axis=0, keepdims=True), 0.0)
        return jnp.broadcast_to(rec, (8, tq))

    def step(i, top, rec, with_scores=True, with_weights=True, with_shares=True):
        def each(j, carry):
            mx, l = carry
            if with_scores:
                mx = scores(i, j, mx, False)
            if with_weights:
                l = weights(i + 1, j, l, top)
            if with_shares:
                shares(i + 2, j, rec)
            return mx, l
        mx, l = lax.fori_loop(0, i, each, (none, zero))
        if with_scores:
            mx = scores(i, i, mx, True)
        if with_weights:
            for d in (0, 1):
                if with_scores or d:
                    l = weights(i + 1, i + d, l, top)
        if with_shares:
            for d in (0, 1, 2):
                if with_scores or with_weights and d or d == 2:
                    shares(i + 2, i + d, rec)
        return mx, l

    last = nt - 1
    mx, _ = step(last, none, none, True, False, False)
    mx, l = step(last - 1, spread_top(mx), none, True, True, False)

    def generic(t, carry):
        top, rec = carry
        i = last - t
        mx, l = step(i, top, rec)
        return spread_top(mx), spread_rec(i + 1, l)
    top, rec = lax.fori_loop(2, nt, generic, (spread_top(mx), spread_rec(last, l)))
    _, l = step(-1, top, rec, False, True, True)
    step(-2, none, spread_rec(0, l), False, False, True)


def whole_body(dims, norm, per, tq, sub, order_ref, inv_ref, limit_ref, bias_ref, q_hbm, k_hbm, v_hbm, w_hbm, bin_ref, w2t_ref, out_ref,
               feat, qa, ka, stage, wbuf, pre, pred_ref, slope_ref, act_ref, qs, ks, s_ref, acc_ref, mass_ref, f_ref,
               mrecv, lab, dl, ft, part, pair, xrecv, sm, small, smr, zs, ys, xs,
               w_sem, in_sem, i_send, i_recv, d_send, d_recv, f_send, f_recv,
               m_send, m_recv, g_send, g_recv, p_send, p_recv, x_send, x_recv, s_send, s_recv):
    ny, nz, nb = dims
    chips = ny * nz
    n = chips * 2
    s, b = lax.axis_index("seq"), lax.axis_index("batch")
    core, c = lax.rem(s, 2), s // 2
    z, y = lax.rem(c, nz), c // nz
    rows, hidden = slope_ref.shape
    head = ka.shape[2]
    q_cols, k_cols = q_hbm.shape[1], k_hbm.shape[1]
    slots, deep = wbuf.shape[:2]
    steps = w_hbm.shape[0] // deep
    chunks, tokens = len(dl), dl[0].shape[0]
    feats = part[0].shape[0]
    begin = [sum(d.shape[1] for d in dl[:j]) for j in range(chunks + 1)]
    half = feats // 2
    own_rows = half // nb
    partner = (s + 1 - 2 * core, b)

    barrier = pltpu.get_barrier_semaphore()

    def greet(r, _):
        pl.semaphore_signal(barrier, inc=1, device_id=(lax.rem(s + r, n), b), device_id_type=MESH)
        return 0
    lax.fori_loop(1, n, greet, 0)
    for r in range(1, nb):
        pl.semaphore_signal(barrier, inc=1, device_id=(s, lax.rem(b + r, nb)), device_id_type=MESH)

    inputs = []
    at = 0
    for i, ref in enumerate((q_hbm, k_hbm, v_hbm)):
        inputs.append(pltpu.make_async_copy(ref, feat.at[:, at:at + ref.shape[1]], in_sem.at[i]))
        at += ref.shape[1]
    for one in inputs:
        one.start()

    def w_copy(i):
        at = lax.rem(i, slots)
        return pltpu.make_async_copy(w_hbm.at[pl.ds(pl.multiple_of(i * deep, deep), deep), :], wbuf.at[at], w_sem.at[at])

    for i in range(slots):
        w_copy(i).start()
    acc_ref[...] = jnp.zeros_like(acc_ref)
    pre[...] = jnp.broadcast_to(bin_ref[...], pre.shape)
    for one in inputs:
        one.wait()

    def chip_at(r, sign):
        dy, dz = r // nz, lax.rem(r, nz)
        return lax.rem(y + sign * dy + ny, ny) * nz + lax.rem(z + sign * dz + nz, nz)

    def columns(i):
        return pl.ds(pl.multiple_of(i * head, head), head)

    def parts(to):
        return (columns(2 * to + core), columns(2 * to + 1 - core), columns(q_cols // head + (2 * to) // per))

    own_q, other_q, own_k = parts(c)
    qa[s] = feat[:, own_q]
    ka[s] = feat[:, own_k]
    mine = pl.ds(pl.multiple_of(c * feats, feats), feats)
    f_ref[c] = feat[:, mine]
    pl.semaphore_wait(barrier, n - 1 + nb - 1)

    def arrivals(frm):
        return (qa.at[2 * frm + core], stage.at[frm], ka.at[2 * frm + core])

    def across(i, to, frm):
        return remote(feat.at[:, parts(to)[i]], arrivals(frm)[i], i_send.at[i, to], i_recv.at[i, frm], (2 * to + core, b))

    def send(r, _):
        to = chip_at(r, 1)
        for i in (1, 2, 0):
            across(i, to, c).start()
        return 0
    lax.fori_loop(1, chips, send, 0)

    def over(i, src, at, whose):
        dst = (qa.at[2 * at + whose], ka.at[2 * at + whose])[i]
        return remote(src, dst, d_send.at[i, at], d_recv.at[i, at], partner)

    over(0, feat.at[:, other_q], c, core).start()
    over(1, feat.at[:, own_k], c, core).start()

    def step(i, _):
        w_copy(i).wait()
        x = feat[:, pl.ds(pl.multiple_of(i * deep, deep), deep)]
        pre[...] += jnp.dot(x, wbuf[lax.rem(i, slots)], preferred_element_type=jnp.float32)

        @pl.when(i + slots < steps)
        def _():
            w_copy(i + slots).start()
        return 0
    lax.fori_loop(0, steps, step, 0)
    p = pre[...]
    sig = jax.nn.sigmoid(p)
    act = (p * sig).astype(jnp.bfloat16)
    act_ref[...] = act
    slope_ref[...] = sig * (1.0 + p * (1.0 - sig))
    out = lax.dot_general(w2t_ref[...], act, (((1,), (1,)), ((), ())), preferred_element_type=jnp.float32)
    for g in range(pred_ref.shape[0]):
        pred_ref[g:g + 1, :] = out[g:g + 1, :] + bias_ref[g]

    def pass_on(r, _):
        frm = chip_at(r, -1)
        across(1, frm, frm).wait_recv()
        over(0, stage.at[frm], frm, core).start()
        across(2, frm, frm).wait_recv()
        over(1, ka.at[2 * frm + core], frm, core).start()
        return 0
    lax.fori_loop(1, chips, pass_on, 0)

    def settle(r, _):
        frm, to = chip_at(r, -1), chip_at(r, 1)
        across(0, frm, frm).wait_recv()
        for i in range(3):
            across(i, to, c).wait_send()
        return 0
    lax.fori_loop(1, chips, settle, 0)

    def settle_over(at, _):
        over(0, stage.at[at], at, 1 - core).wait()
        over(1, ka.at[2 * at + core], at, 1 - core).wait()
        return 0
    lax.fori_loop(0, chips, settle_over, 0)

    def f_copy(to, frm):
        cut = pl.ds(pl.multiple_of(to * feats, feats), feats)
        return remote(feat.at[:, cut], f_ref.at[frm], f_send.at[to], f_recv.at[frm], (2 * to + core, b))

    def f_start(r, _):
        f_copy(chip_at(r, 1), c).start()
        return 0
    lax.fori_loop(1, chips, f_start, 0)

    def sort(at, _):
        here = pl.ds(pl.multiple_of(at * rows, rows), rows)
        qs[here, :] = qa[inv_ref[at]]
        ks[here, :] = ka[inv_ref[at]]
        return 0
    lax.fori_loop(0, n, sort, 0)

    scale2 = math.log2(math.e) / math.sqrt(head)
    attn_core(tq, sub, n * rows, scale2, limit_ref[0], qs, ks, s_ref, acc_ref)

    def emit(at, _):
        block = acc_ref[order_ref[at]]
        mass_ref[at] = jnp.sum(block.T, axis=0, keepdims=True)
        return 0
    lax.fori_loop(0, n, emit, 0)

    def mass_copy(r, sender):
        to = lax.rem(s + r, n)
        return remote(mass_ref.at[to], mrecv.at[s], m_send.at[r], m_recv.at[s], (to, b))

    def mass_start(r, _):
        mass_copy(r, s).start()
        return 0
    lax.fori_loop(1, n, mass_start, 0)
    mrecv[s] = mass_ref[s]

    def f_wait(r, _):
        frm = chip_at(r, -1)
        f_copy(frm, frm).wait_recv()
        f_copy(chip_at(r, 1), c).wait_send()
        return 0
    lax.fori_loop(1, chips, f_wait, 0)
    for k in range(tokens // rows):
        ft[:, k * rows:(k + 1) * rows] = f_ref[k].T

    def mass_wait(r, _):
        frm = lax.rem(s + n - r, n)
        got = remote(mass_ref.at[frm], mrecv.at[frm], m_send.at[r], m_recv.at[frm], (frm, b))
        got.wait_recv()
        return 0
    lax.fori_loop(1, n, mass_wait, 0)

    heads = lab.shape[0]
    per = n // heads
    for g in range(heads):
        total = mrecv[per * g]
        for i in range(1, per):
            total = total + mrecv[per * g + i]
        lab[g:g + 1, :] = jnp.log1p(total)
    position = order_ref[s] * rows + lax.broadcasted_iota(jnp.int32, (1, rows), 1)
    live = jnp.where(position < limit_ref[0], 1.0, 0.0)
    resid_t = ((pred_ref[...] - lab[...]) * live * norm).astype(jnp.bfloat16)
    resid = resid_t.astype(jnp.float32).T.astype(jnp.bfloat16)
    back = jnp.dot(resid, w2t_ref[...], preferred_element_type=jnp.float32)
    delta = (back * slope_ref[...]).astype(jnp.bfloat16)
    here = pl.ds(pl.multiple_of(c * rows, rows), rows)
    for j in range(chunks):
        dl[j][here, :] = delta[:, begin[j]:begin[j + 1]]

    wide = rows // 2
    slot = {}

    def number(*key):
        return slot.setdefault(key, len(slot))

    def spot(half_id, a, e):
        return (a * nz + e) if half_id == 0 else (e * nz + a)

    def ring(v, d, size):
        return lax.rem(v + (d + size), size)

    def coords(half_id):
        return (y, z, ny, nz) if half_id == 0 else (z, y, nz, ny)

    def piece(j, block, half_id, quarter):
        r0 = half_id * wide + (quarter * (wide // 2) if quarter is not None else 0)
        size = wide // 2 if quarter is not None else wide
        return dl[j].at[pl.ds(pl.multiple_of(block * rows + r0, wide // 2), size), :]

    def neighbour(half_id, which, d):
        along_y = (half_id == 0) == (which == 0)
        to_y = ring(y, d, ny) if along_y else y
        to_z = z if along_y else ring(z, d, nz)
        return ((to_y * nz + to_z) * 2 + core, b)

    started = []

    def copy(j, half_id, which, da, de, quarter, d):
        a, e, na, ne = coords(half_id)
        block = spot(half_id, ring(a, da, na), ring(e, de, ne))
        ref = piece(j, block, half_id, quarter)
        m = number(j, half_id, which, da, de, quarter, d)
        return remote(ref, ref, g_send.at[m], g_recv.at[m], neighbour(half_id, which, d))

    def send(j, half_id, which, da, de, quarter, d):
        one = copy(j, half_id, which, da, de, quarter, d)
        one.start()
        started.append(one)

    def receive(j, half_id, which, da, de, quarter, d):
        a, e, na, ne = coords(half_id)
        back_a, back_e = (da - d, de) if which == 0 else (da, de - d)
        block = spot(half_id, ring(a, back_a, na), ring(e, back_e, ne))
        ref = piece(j, block, half_id, quarter)
        m = number(j, half_id, which, da, de, quarter, d)
        remote(ref, ref, g_send.at[m], g_recv.at[m], neighbour(half_id, which, -d)).wait_recv()

    def second(j, h, da):
        for d in (1, -1):
            send(j, h, 1, da, 0, None, d)

    def second_pass_on(j, h, da):
        receive(j, h, 1, da, 0, None, 1)
        send(j, h, 1, da, -1, 0, 1)
        receive(j, h, 1, da, 0, None, -1)
        send(j, h, 1, da, 1, 1, -1)

    def second_end(j, h, da):
        receive(j, h, 1, da, -1, 0, 1)
        receive(j, h, 1, da, 1, 1, -1)

    def stage0(j):
        for h in (0, 1):
            for d in (1, -1):
                send(j, h, 0, 0, 0, None, d)
        for h in (0, 1):
            second(j, h, 0)

    def stage1(j):
        for h in (0, 1):
            receive(j, h, 0, 0, 0, None, 1)
            send(j, h, 0, -1, 0, 0, 1)
            second(j, h, -1)
            receive(j, h, 0, 0, 0, None, -1)
            send(j, h, 0, 1, 0, 1, -1)
            second(j, h, 1)

    def stage2(j):
        for h in (0, 1):
            second_pass_on(j, h, 0)
        for h in (0, 1):
            receive(j, h, 0, -1, 0, 0, 1)
            receive(j, h, 0, 1, 0, 1, -1)
            second(j, h, 2)

    def stage3(j):
        for da in (-1, 1):
            for h in (0, 1):
                second_pass_on(j, h, da)

    def stage4(j):
        for h in (0, 1):
            second_pass_on(j, h, 2)

    def stage5(j):
        for da in (0, -1, 1, 2):
            for h in (0, 1):
                second_end(j, h, da)

    def multiply(j):
        part[j][...] = jnp.dot(ft[...], dl[j][...], preferred_element_type=jnp.float32)

    def pair_copy(j, of):
        ref = part[j].at[pl.ds(pl.multiple_of((1 - of) * half, half), half), :]
        return remote(ref, pair[j], p_send.at[j], p_recv.at[j], partner)

    def pair_start(j):
        one = pair_copy(j, core)
        one.start()
        started.append(one)

    def x_copy(j, r):
        to = lax.rem(b + r, nb)
        ref = pair[j].at[pl.ds(pl.multiple_of(to * own_rows, own_rows), own_rows), :]
        return remote(ref, xrecv[j].at[r - 1], x_send.at[j, r - 1], x_recv.at[j, r - 1], (s, to))

    def x_start(j):
        pair_copy(j, core).wait_recv()
        pair[j][...] = pair[j][...] + part[j][pl.ds(pl.multiple_of(core * half, half), half), :]
        for r in (2, 1, 3)[: nb - 1]:
            one = x_copy(j, r)
            one.start()
            started.append(one)

    def x_end(j):
        for r in range(1, nb):
            x_copy(j, r).wait_recv()
        own = pair[j][pl.ds(pl.multiple_of(b * own_rows, own_rows), own_rows), :]
        for r in range(1, nb):
            own = own + xrecv[j][r - 1]
        out_ref[:own_rows, begin[j]:begin[j + 1]] = own

    def small_start0():
        sw = sm.shape[2]
        out_term = jnp.dot(resid_t, act_ref[...], preferred_element_type=jnp.float32)
        sums = jnp.sum(delta.astype(jnp.float32), axis=0, keepdims=True)
        bias = jnp.sum(resid.astype(jnp.float32), axis=0, keepdims=True)
        lanes = 128
        cols = [out_term[:, k * lanes:(k + 1) * lanes] for k in range(hidden // lanes)]
        cols.append(jnp.concatenate([sums[:, k * lanes:(k + 1) * lanes] for k in range(hidden // lanes)], axis=0))
        cols.append(jnp.zeros((heads, lanes), jnp.float32))
        each = sw // lanes
        for k, value in enumerate(cols):
            sm[k // each, :, (k % each) * lanes:(k % each + 1) * lanes] = value
        at = (len(cols) - 1) % each * lanes
        sm[1, 0:1, at:at + heads] = bias
        one = remote(sm.at[1 - core], smr, s_send.at[0], s_recv.at[0], partner)
        one.start()
        started.append(one)

    def small_hop(level, value, buf, at, size, target):
        buf[at] = value
        for r in range(1, size):
            one = remote(buf.at[at], buf.at[at], s_send.at[level * 3 + r], s_recv.at[level * 3 + r], target(r))
            one.start()
            started.append(one)

    def small_sum(level, buf, at, size, target):
        for r in range(1, size):
            frm = lax.rem(at + size - r, size)
            remote(buf.at[frm], buf.at[frm], s_send.at[level * 3 + r], s_recv.at[level * 3 + r], target(r)).wait_recv()
        total = buf[0]
        for k in range(1, size):
            total = total + buf[k]
        return total

    to_z = lambda r: ((y * nz + lax.rem(z + r, nz)) * 2 + core, b)
    to_y = lambda r: ((lax.rem(y + r, ny) * nz + z) * 2 + core, b)
    to_x = lambda r: (s, lax.rem(b + r, nb))

    def small1():
        remote(sm.at[1 - core], smr, s_send.at[0], s_recv.at[0], partner).wait_recv()
        small_hop(0, sm[core] + smr[...], zs, z, nz, to_z)

    def small2():
        small_hop(1, small_sum(0, zs, z, nz, to_z), ys, y, ny, to_y)

    def small3():
        small_hop(2, small_sum(1, ys, y, ny, to_y), xs, b, nb, to_x)

    def small4():
        sm[core] = small_sum(2, xs, b, nb, to_x)
        one = remote(sm.at[core], small.at[core], s_send.at[10], s_recv.at[10], partner)
        one.start()
        started.append(one)
        small[core] = sm[core]

    def small5():
        remote(sm.at[1 - core], small.at[1 - core], s_send.at[10], s_recv.at[10], partner).wait_recv()
        sw = small.shape[2]
        out_ref[own_rows:own_rows + heads, :sw] = small[0]
        out_ref[own_rows:own_rows + heads, sw:] = small[1, :, :hidden - sw]
        base = own_rows + heads
        lanes = 128
        for k in range(hidden // lanes):
            out_ref[base:base + 1, k * lanes:(k + 1) * lanes] = small[1, k:k + 1, hidden - sw:hidden - sw + lanes]
        out_ref[base + 1:base + 2, :lanes] = small[1, 0:1, hidden - sw + lanes:hidden - sw + 2 * lanes]

    stage0(0); small_start0(); stage1(0); stage2(0); stage0(1); stage3(0); small1(); stage1(1); stage4(0)
    stage2(1); stage5(0); small2(); stage3(1)
    multiply(0); pair_start(0); stage4(1); small3()
    x_start(0); stage5(1)
    multiply(1); pair_start(1); small4(); x_end(0); x_start(1); small5(); x_end(1)

    for one in started:
        one.wait_send()

    def mass_drain(r, _):
        mass_copy(r, s).wait_send()
        return 0
    lax.fori_loop(1, n, mass_drain, 0)


def whole(dims, norm, order, inverse, limit, bias, q, k, v, w_in, b_in, w2t, tq=512, sub=128, widths=(640, 384), slots=3, deep=512):
    ny, nz, nb = dims
    rows, hidden = q.shape[0], w_in.shape[1]
    heads = w2t.shape[0]
    size = k.shape[1] // heads
    chips = ny * nz
    n = 2 * chips
    tokens = chips * rows
    columns = w_in.shape[0]
    feats = columns // chips
    half = feats // 2
    chunks = len(widths)
    sw = (hidden + 256) // 2
    vm, dma = pltpu.VMEM, pltpu.SemaphoreType.DMA
    block = lambda space: pl.BlockSpec(memory_space=space)
    f32, bf16 = jnp.float32, jnp.bfloat16
    return pl.pallas_call(
        functools.partial(whole_body, dims, norm, q.shape[1] // k.shape[1], tq, sub),
        out_shape=jax.ShapeDtypeStruct((half // nb + 16, hidden), f32),
        in_specs=[block(pltpu.SMEM)] * 4 + [block(pltpu.HBM)] * 4 + [block(vm)] * 2,
        out_specs=block(vm),
        scratch_shapes=[
            vm((rows, columns), bf16),
            vm((n, rows, size), bf16),
            vm((n, rows, size), bf16),
            vm((chips, rows, size), bf16),
            vm((slots, deep, hidden), bf16),
            vm((rows, hidden), f32),
            vm((heads, rows), f32),
            vm((rows, hidden), f32),
            vm((rows, hidden), bf16),
            vm((n * rows, size), bf16),
            vm((n * rows, size), bf16),
            vm((3, n * rows, tq), f32),
            vm((n, rows, 128), f32),
            vm((n, 1, rows), f32),
            vm((chips, rows, feats), bf16),
            vm((n, 1, rows), f32),
            vm((heads, rows), f32),
            tuple(vm((tokens, w), bf16) for w in widths),
            vm((feats, tokens), bf16),
            tuple(vm((feats, w), f32) for w in widths),
            tuple(vm((half, w), f32) for w in widths),
            tuple(vm((nb - 1, half // nb, w), f32) for w in widths),
            vm((2, heads, sw), f32),
            vm((2, heads, sw), f32),
            vm((heads, sw), f32),
            vm((nz, heads, sw), f32),
            vm((ny, heads, sw), f32),
            vm((nb, heads, sw), f32),
            dma((slots,)), dma((3,)),
            dma((3, chips)), dma((3, chips)),
            dma((2, chips)), dma((2, chips)),
            dma((chips,)), dma((chips,)),
            dma((n,)), dma((n,)),
            dma((chunks * 40,)), dma((chunks * 40,)),
            dma((chunks,)), dma((chunks,)),
            dma((chunks, nb - 1)), dma((chunks, nb - 1)),
            dma((12,)), dma((12,)),
        ],
        compiler_params=pltpu.CompilerParams(collective_id=1, has_side_effects=True, vmem_limit_bytes=60 * 2**20),
        name="whole",
    )(order, inverse, limit, bias, q, k, v, w_in, b_in, w2t)


def on_device(dims, queries, keys, values, lengths, block_pos, w_in, b_in, output_weight, output_bias):
    hidden, heads = output_weight.shape
    total = lax.axis_size("seq") * queries.shape[1]
    norm = 1.0 / math.sqrt(lax.axis_size("batch") * total)
    order = block_pos[0]
    stored = jnp.arange(order.shape[0], dtype=jnp.int32)
    inverse = jnp.sum(jnp.where(order[None, :] == stored[:, None], stored[None, :], 0), axis=1)
    out = whole(
        dims, norm, order, inverse, lengths, output_bias, queries[0], keys[0], values[0], w_in, b_in[None, :], output_weight.T
    )
    own = out.shape[0] - 16
    return (out[:own], out[own + heads], out[own:own + heads].T, out[own + heads + 1, :heads])


def solution(mesh):
    nb = mesh.shape["batch"]
    ny = nz = math.isqrt(mesh.shape["seq"] // 2)
    return jax.shard_map(
        functools.partial(on_device, (ny, nz, nb)),
        mesh=mesh,
        in_specs=(
            P("batch", "seq", None),
            P("batch", "seq", None),
            P("batch", "seq", None),
            P("batch"),
            P("batch", None),
            P(),
            P(),
            P(),
            P(),
        ),
        out_specs=(P(("seq", "batch"), None), P(), P(), P()),
        check_vma=False,
    )
```

```python
import functools
import math

import jax
import jax.numpy as jnp
from jax import lax
from jax.experimental import pallas as pl
from jax.experimental.pallas import tpu as pltpu
from jax.sharding import PartitionSpec as P

NEG = -1e30
MESH = pl.DeviceIdType.MESH


def remote(src, dst, send_sem, recv_sem, device):
    return pltpu.make_async_remote_copy(
        src_ref=src, dst_ref=dst, send_sem=send_sem, recv_sem=recv_sem, device_id=device, device_id_type=MESH
    )


def attn_core(tq, sub, total, scale2, limit, qs, ks, bufs, acc_ref, done=None):
    lanes = 128
    groups = tq // lanes
    nt = total // tq
    eights = lambda x: x.reshape(x.shape[0] // 8, 8, tq)

    def at(j, n=tq):
        return pl.ds(pl.multiple_of(j * n, n), n)

    def scores(i, j, mx, masked):
        s = lax.dot_general(ks[at(j), :], qs[at(i), :], (((1,), (1,)), ((), ())), preferred_element_type=jnp.float32)
        if masked:
            kp = lax.broadcasted_iota(jnp.int32, (tq, tq), 0)
            qp = lax.broadcasted_iota(jnp.int32, (tq, tq), 1)
            s = jnp.where(kp <= qp, s, NEG)
        bufs[i % 3][at(j), :] = s
        return jnp.maximum(mx, jnp.max(eights(s), axis=0))

    def weights(i, j, l, top):
        buf = bufs[i % 3]
        for u in range(tq // sub):
            here = pl.ds(pl.multiple_of(j * tq + u * sub, sub), sub)
            w = jnp.exp2((eights(buf[here, :]) - top[None]) * scale2)
            buf[here, :] = w.reshape(sub, tq)
            l = l + jnp.sum(w, axis=0)
        return l

    def shares(i, j, rec):
        buf = bufs[i % 3]
        for u in range(tq // sub):
            here = pl.ds(pl.multiple_of(j * tq + u * sub, sub), sub)
            w = (eights(buf[here, :]) * rec[None]).reshape(sub, tq)
            tot = w[:, :lanes]
            for g in range(1, groups):
                tot = tot + w[:, g * lanes:(g + 1) * lanes]
            acc_ref[j * (tq // sub) + u] += tot

    def spread_top(mx):
        return jnp.broadcast_to(jnp.max(mx, axis=0, keepdims=True), (8, tq))

    def spread_rec(i, l):
        pos = i * tq + lax.broadcasted_iota(jnp.int32, (1, tq), 1)
        rec = jnp.where(pos < limit, 1.0 / jnp.sum(l, axis=0, keepdims=True), 0.0)
        return jnp.broadcast_to(rec, (8, tq))

    top = rec = None
    for i in range(nt - 1, -3, -1):
        first, second, third = i >= 0, 0 <= i + 1 < nt, i + 2 < nt

        def each(j, carry, i=i, first=first, second=second, third=third, top=top, rec=rec):
            mx, l = carry
            if first:
                mx = scores(i, j, mx, False)
            if second:
                l = weights(i + 1, j, l, top)
            if third:
                shares(i + 2, j, rec)
            return mx, l

        mx = jnp.full((8, tq), NEG, jnp.float32)
        l = jnp.zeros((8, tq), jnp.float32)
        if i > 0:
            mx, l = lax.fori_loop(0, i, each, (mx, l))
        if first:
            mx = scores(i, i, mx, True)
        for d in (0, 1, 2):
            if second and d < 2 and i + d >= 0:
                l = weights(i + 1, i + d, l, top)
            if third and i + d >= 0:
                shares(i + 2, i + d, rec)
        if third and done is not None:
            done(i + 2)
        top, rec = spread_top(mx), spread_rec(i + 1, l)


def whole_body(dims, norm, per, tq, sub, order_ref, inv_ref, limit_ref, bias_ref, q_hbm, k_hbm, v_hbm, w_hbm, bin_ref, w2t_ref, out_ref,
               feat, qa, ka, stage, wbuf, pre, pred_ref, slope_ref, act_ref, qs, ks, bufs, acc_ref, msort, mass_ref, f_ref,
               mrecv, lab, dl, ft, part, pair, xrecv, sm, small, smr, zs, ys, xs,
               w_sem, in_sem, i_send, i_recv, d_send, d_recv, f_send, f_recv,
               m_send, m_recv, g_send, g_recv, p_send, p_recv, x_send, x_recv, s_send, s_recv):
    ny, nz, nb = dims
    chips = ny * nz
    n = chips * 2
    s, b = lax.axis_index("seq"), lax.axis_index("batch")
    core, c = lax.rem(s, 2), s // 2
    z, y = lax.rem(c, nz), c // nz
    rows, hidden = slope_ref.shape
    head = ka.shape[2]
    q_cols, k_cols = q_hbm.shape[1], k_hbm.shape[1]
    slots, deep = wbuf.shape[:2]
    steps = w_hbm.shape[0] // deep
    chunks, tokens = len(dl), dl[0].shape[0]
    feats = part[0].shape[0]
    begin = [sum(d.shape[1] for d in dl[:j]) for j in range(chunks + 1)]
    half = feats // 2
    own_rows = half // nb
    partner = (s + 1 - 2 * core, b)

    barrier = pltpu.get_barrier_semaphore()

    def greet(r, _):
        pl.semaphore_signal(barrier, inc=1, device_id=(lax.rem(s + r, n), b), device_id_type=MESH)
        return 0
    lax.fori_loop(1, n, greet, 0)
    for r in range(1, nb):
        pl.semaphore_signal(barrier, inc=1, device_id=(s, lax.rem(b + r, nb)), device_id_type=MESH)

    inputs = []
    at = 0
    for i, ref in enumerate((q_hbm, k_hbm, v_hbm)):
        inputs.append(pltpu.make_async_copy(ref, feat.at[:, at:at + ref.shape[1]], in_sem.at[i]))
        at += ref.shape[1]
    for one in inputs:
        one.start()

    def w_copy(i):
        at = lax.rem(i, slots)
        return pltpu.make_async_copy(w_hbm.at[pl.ds(pl.multiple_of(i * deep, deep), deep), :], wbuf.at[at], w_sem.at[at])

    for i in range(slots):
        w_copy(i).start()
    acc_ref[...] = jnp.zeros_like(acc_ref)
    pre[...] = jnp.broadcast_to(bin_ref[...], pre.shape)
    for one in inputs:
        one.wait()

    hops = lambda d: -min(d[0], ny - d[0]) - min(d[1], nz - d[1])
    away = sorted(((dy, dz) for dy in range(ny) for dz in range(nz) if dy or dz), key=hops)

    def chip_at(d, sign):
        dy, dz = d
        return lax.rem(y + sign * dy + ny, ny) * nz + lax.rem(z + sign * dz + nz, nz)

    def columns(i):
        return pl.ds(pl.multiple_of(i * head, head), head)

    def parts(to):
        return (columns(2 * to + core), columns(2 * to + 1 - core), columns(q_cols // head + (2 * to) // per))

    own_q, other_q, own_k = parts(c)
    qa[s] = feat[:, own_q]
    ka[s] = feat[:, own_k]
    mine = pl.ds(pl.multiple_of(c * feats, feats), feats)
    f_ref[c] = feat[:, mine]
    pl.semaphore_wait(barrier, n - 1 + nb - 1)

    def arrivals(frm):
        return (qa.at[2 * frm + core], stage.at[frm], ka.at[2 * frm + core])

    def across(i, to, frm):
        return remote(feat.at[:, parts(to)[i]], arrivals(frm)[i], i_send.at[i, to], i_recv.at[i, frm], (2 * to + core, b))

    for some in ((1, 2), (0,)):
        for d in away:
            for i in some:
                across(i, chip_at(d, 1), c).start()

    def over(i, src, at, whose):
        dst = (qa.at[2 * at + whose], ka.at[2 * at + whose])[i]
        return remote(src, dst, d_send.at[i, at], d_recv.at[i, at], partner)

    over(0, feat.at[:, other_q], c, core).start()
    over(1, feat.at[:, own_k], c, core).start()

    def step(i, _):
        w_copy(i).wait()
        x = feat[:, pl.ds(pl.multiple_of(i * deep, deep), deep)]
        pre[...] += jnp.dot(x, wbuf[lax.rem(i, slots)], preferred_element_type=jnp.float32)

        @pl.when(i + slots < steps)
        def _():
            w_copy(i + slots).start()
        return 0
    lax.fori_loop(0, steps, step, 0)
    p = pre[...]
    sig = jax.nn.sigmoid(p)
    act = (p * sig).astype(jnp.bfloat16)
    act_ref[...] = act
    slope_ref[...] = sig * (1.0 + p * (1.0 - sig))
    out = lax.dot_general(w2t_ref[...], act, (((1,), (1,)), ((), ())), preferred_element_type=jnp.float32)
    for g in range(pred_ref.shape[0]):
        pred_ref[g:g + 1, :] = out[g:g + 1, :] + bias_ref[g]

    for d in away:
        frm = chip_at(d, -1)
        across(1, frm, frm).wait_recv()
        over(0, stage.at[frm], frm, core).start()
        across(2, frm, frm).wait_recv()
        over(1, ka.at[2 * frm + core], frm, core).start()

    def all_others(r):
        return lax.rem(c + r, chips)

    def settle(r, _):
        across(0, all_others(r), all_others(r)).wait_recv()
        for i in range(3):
            across(i, all_others(r), c).wait_send()
        return 0
    lax.fori_loop(1, chips, settle, 0)

    def settle_over(at, _):
        over(0, stage.at[at], at, 1 - core).wait()
        over(1, ka.at[2 * at + core], at, 1 - core).wait()
        return 0
    lax.fori_loop(0, chips, settle_over, 0)

    def f_copy(to, frm):
        cut = pl.ds(pl.multiple_of(to * feats, feats), feats)
        return remote(feat.at[:, cut], f_ref.at[frm], f_send.at[to], f_recv.at[frm], (2 * to + core, b))

    for d in away:
        f_copy(chip_at(d, 1), c).start()

    def sort(at, _):
        here = pl.ds(pl.multiple_of(at * rows, rows), rows)
        qs[here, :] = qa[inv_ref[at]]
        ks[here, :] = ka[inv_ref[at]]
        return 0
    lax.fori_loop(0, n, sort, 0)

    scale2 = math.log2(math.e) / math.sqrt(head)

    def done(i):
        for u in range(i * (tq // rows), (i + 1) * (tq // rows)):
            msort[u] = jnp.sum(acc_ref[u].T, axis=0, keepdims=True)

    attn_core(tq, sub, n * rows, scale2, limit_ref[0], qs, ks, bufs, acc_ref, done)

    def emit(at, _):
        mass_ref[at] = msort[order_ref[at]]
        return 0
    lax.fori_loop(0, n, emit, 0)

    def mass_copy(r, sender):
        to = lax.rem(s + r, n)
        return remote(mass_ref.at[to], mrecv.at[s], m_send.at[r], m_recv.at[s], (to, b))

    def mass_start(r, _):
        mass_copy(r, s).start()
        return 0
    lax.fori_loop(1, n, mass_start, 0)
    mrecv[s] = mass_ref[s]

    def f_wait(r, _):
        f_copy(all_others(r), all_others(r)).wait_recv()
        f_copy(all_others(r), c).wait_send()
        return 0
    lax.fori_loop(1, chips, f_wait, 0)
    for k in range(tokens // rows):
        ft[:, k * rows:(k + 1) * rows] = f_ref[k].T

    def mass_wait(r, _):
        frm = lax.rem(s + n - r, n)
        got = remote(mass_ref.at[frm], mrecv.at[frm], m_send.at[r], m_recv.at[frm], (frm, b))
        got.wait_recv()
        return 0
    lax.fori_loop(1, n, mass_wait, 0)

    heads = lab.shape[0]
    per = n // heads
    for g in range(heads):
        total = mrecv[per * g]
        for i in range(1, per):
            total = total + mrecv[per * g + i]
        lab[g:g + 1, :] = jnp.log1p(total)
    position = order_ref[s] * rows + lax.broadcasted_iota(jnp.int32, (1, rows), 1)
    live = jnp.where(position < limit_ref[0], 1.0, 0.0)
    resid_t = ((pred_ref[...] - lab[...]) * live * norm).astype(jnp.bfloat16)
    resid = resid_t.astype(jnp.float32).T.astype(jnp.bfloat16)
    back = jnp.dot(resid, w2t_ref[...], preferred_element_type=jnp.float32)
    delta = (back * slope_ref[...]).astype(jnp.bfloat16)
    here = pl.ds(pl.multiple_of(c * rows, rows), rows)
    for j in range(chunks):
        dl[j][here, :] = delta[:, begin[j]:begin[j + 1]]

    wide = rows // 2
    slot = {}

    def number(*key):
        return slot.setdefault(key, len(slot))

    def spot(half_id, a, e):
        return (a * nz + e) if half_id == 0 else (e * nz + a)

    def ring(v, d, size):
        return lax.rem(v + (d + size), size)

    def coords(half_id):
        return (y, z, ny, nz) if half_id == 0 else (z, y, nz, ny)

    def piece(j, block, half_id, quarter):
        r0 = half_id * wide + (quarter * (wide // 2) if quarter is not None else 0)
        size = wide // 2 if quarter is not None else wide
        return dl[j].at[pl.ds(pl.multiple_of(block * rows + r0, wide // 2), size), :]

    def neighbour(half_id, which, d):
        along_y = (half_id == 0) == (which == 0)
        to_y = ring(y, d, ny) if along_y else y
        to_z = z if along_y else ring(z, d, nz)
        return ((to_y * nz + to_z) * 2 + core, b)

    started = []

    def copy(j, half_id, which, da, de, quarter, d):
        a, e, na, ne = coords(half_id)
        block = spot(half_id, ring(a, da, na), ring(e, de, ne))
        ref = piece(j, block, half_id, quarter)
        m = number(j, half_id, which, da, de, quarter, d)
        return remote(ref, ref, g_send.at[m], g_recv.at[m], neighbour(half_id, which, d))

    def send(j, half_id, which, da, de, quarter, d):
        one = copy(j, half_id, which, da, de, quarter, d)
        one.start()
        started.append(one)

    def receive(j, half_id, which, da, de, quarter, d):
        a, e, na, ne = coords(half_id)
        back_a, back_e = (da - d, de) if which == 0 else (da, de - d)
        block = spot(half_id, ring(a, back_a, na), ring(e, back_e, ne))
        ref = piece(j, block, half_id, quarter)
        m = number(j, half_id, which, da, de, quarter, d)
        remote(ref, ref, g_send.at[m], g_recv.at[m], neighbour(half_id, which, -d)).wait_recv()

    def second(j, h, da):
        for d in (1, -1):
            send(j, h, 1, da, 0, None, d)

    def second_pass_on(j, h, da):
        receive(j, h, 1, da, 0, None, 1)
        send(j, h, 1, da, -1, 0, 1)
        receive(j, h, 1, da, 0, None, -1)
        send(j, h, 1, da, 1, 1, -1)

    def second_end(j, h, da):
        receive(j, h, 1, da, -1, 0, 1)
        receive(j, h, 1, da, 1, 1, -1)

    def stage0(j):
        for h in (0, 1):
            for d in (1, -1):
                send(j, h, 0, 0, 0, None, d)
        for h in (0, 1):
            second(j, h, 0)

    def stage1(j):
        for h in (0, 1):
            receive(j, h, 0, 0, 0, None, 1)
            send(j, h, 0, -1, 0, 0, 1)
            second(j, h, -1)
            receive(j, h, 0, 0, 0, None, -1)
            send(j, h, 0, 1, 0, 1, -1)
            second(j, h, 1)

    def stage2(j):
        for h in (0, 1):
            second_pass_on(j, h, 0)
        for h in (0, 1):
            receive(j, h, 0, -1, 0, 0, 1)
            receive(j, h, 0, 1, 0, 1, -1)
            second(j, h, 2)

    def stage3(j):
        for da in (-1, 1):
            for h in (0, 1):
                second_pass_on(j, h, da)

    def stage4(j):
        for h in (0, 1):
            second_pass_on(j, h, 2)

    def stage5(j):
        for da in (0, -1, 1, 2):
            for h in (0, 1):
                second_end(j, h, da)

    def multiply(j):
        part[j][...] = jnp.dot(ft[...], dl[j][...], preferred_element_type=jnp.float32)

    def pair_copy(j, of):
        ref = part[j].at[pl.ds(pl.multiple_of((1 - of) * half, half), half), :]
        return remote(ref, pair[j], p_send.at[j], p_recv.at[j], partner)

    def pair_start(j):
        one = pair_copy(j, core)
        one.start()
        started.append(one)

    def x_copy(j, r):
        to = lax.rem(b + r, nb)
        ref = pair[j].at[pl.ds(pl.multiple_of(to * own_rows, own_rows), own_rows), :]
        return remote(ref, xrecv[j].at[r - 1], x_send.at[j, r - 1], x_recv.at[j, r - 1], (s, to))

    def x_start(j):
        pair_copy(j, core).wait_recv()
        pair[j][...] = pair[j][...] + part[j][pl.ds(pl.multiple_of(core * half, half), half), :]
        for r in (2, 1, 3)[: nb - 1]:
            one = x_copy(j, r)
            one.start()
            started.append(one)

    def x_end(j):
        for r in range(1, nb):
            x_copy(j, r).wait_recv()
        own = pair[j][pl.ds(pl.multiple_of(b * own_rows, own_rows), own_rows), :]
        for r in range(1, nb):
            own = own + xrecv[j][r - 1]
        out_ref[:own_rows, begin[j]:begin[j + 1]] = own

    def small_start0():
        sw = sm.shape[2]
        out_term = jnp.dot(resid_t, act_ref[...], preferred_element_type=jnp.float32)
        sums = jnp.sum(delta.astype(jnp.float32), axis=0, keepdims=True)
        bias = jnp.sum(resid.astype(jnp.float32), axis=0, keepdims=True)
        lanes = 128
        cols = [out_term[:, k * lanes:(k + 1) * lanes] for k in range(hidden // lanes)]
        cols.append(jnp.concatenate([sums[:, k * lanes:(k + 1) * lanes] for k in range(hidden // lanes)], axis=0))
        cols.append(jnp.zeros((heads, lanes), jnp.float32))
        each = sw // lanes
        for k, value in enumerate(cols):
            sm[k // each, :, (k % each) * lanes:(k % each + 1) * lanes] = value
        at = (len(cols) - 1) % each * lanes
        sm[1, 0:1, at:at + heads] = bias
        one = remote(sm.at[1 - core], smr, s_send.at[0], s_recv.at[0], partner)
        one.start()
        started.append(one)

    def small_hop(level, value, buf, at, size, target):
        buf[at] = value
        for r in range(1, size):
            one = remote(buf.at[at], buf.at[at], s_send.at[level * 3 + r], s_recv.at[level * 3 + r], target(r))
            one.start()
            started.append(one)

    def small_sum(level, buf, at, size, target):
        for r in range(1, size):
            frm = lax.rem(at + size - r, size)
            remote(buf.at[frm], buf.at[frm], s_send.at[level * 3 + r], s_recv.at[level * 3 + r], target(r)).wait_recv()
        total = buf[0]
        for k in range(1, size):
            total = total + buf[k]
        return total

    to_z = lambda r: ((y * nz + lax.rem(z + r, nz)) * 2 + core, b)
    to_y = lambda r: ((lax.rem(y + r, ny) * nz + z) * 2 + core, b)
    to_x = lambda r: (s, lax.rem(b + r, nb))

    def small1():
        remote(sm.at[1 - core], smr, s_send.at[0], s_recv.at[0], partner).wait_recv()
        small_hop(0, sm[core] + smr[...], zs, z, nz, to_z)

    def small2():
        small_hop(1, small_sum(0, zs, z, nz, to_z), ys, y, ny, to_y)

    def small3():
        small_hop(2, small_sum(1, ys, y, ny, to_y), xs, b, nb, to_x)

    def small4():
        sm[core] = small_sum(2, xs, b, nb, to_x)
        one = remote(sm.at[core], small.at[core], s_send.at[10], s_recv.at[10], partner)
        one.start()
        started.append(one)
        small[core] = sm[core]

    def small5():
        remote(sm.at[1 - core], small.at[1 - core], s_send.at[10], s_recv.at[10], partner).wait_recv()
        sw = small.shape[2]
        out_ref[own_rows:own_rows + heads, :sw] = small[0]
        out_ref[own_rows:own_rows + heads, sw:] = small[1, :, :hidden - sw]
        base = own_rows + heads
        lanes = 128
        for k in range(hidden // lanes):
            out_ref[base:base + 1, k * lanes:(k + 1) * lanes] = small[1, k:k + 1, hidden - sw:hidden - sw + lanes]
        out_ref[base + 1:base + 2, :lanes] = small[1, 0:1, hidden - sw + lanes:hidden - sw + 2 * lanes]

    stage0(0)
    stage0(1)
    small_start0()
    stage1(0)
    stage2(0)
    stage1(1)
    small1()
    stage3(0)
    stage2(1)
    stage4(0)
    small2()
    stage3(1)
    stage5(0)
    multiply(0)
    pair_start(0)
    stage4(1)
    small3()
    x_start(0)
    stage5(1)
    multiply(1)
    pair_start(1)
    small4()
    x_start(1)
    x_end(0)
    small5()
    x_end(1)

    for one in started:
        one.wait_send()

    def mass_drain(r, _):
        mass_copy(r, s).wait_send()
        return 0
    lax.fori_loop(1, n, mass_drain, 0)


def whole(dims, norm, order, inverse, limit, bias, q, k, v, w_in, b_in, w2t, tq=512, sub=128, widths=(512, 512), slots=3, deep=512):
    ny, nz, nb = dims
    rows, hidden = q.shape[0], w_in.shape[1]
    heads = w2t.shape[0]
    size = k.shape[1] // heads
    chips = ny * nz
    n = 2 * chips
    tokens = chips * rows
    columns = w_in.shape[0]
    feats = columns // chips
    half = feats // 2
    chunks = len(widths)
    sw = (hidden + 256) // 2
    vm, dma = pltpu.VMEM, pltpu.SemaphoreType.DMA
    block = lambda space: pl.BlockSpec(memory_space=space)
    f32, bf16 = jnp.float32, jnp.bfloat16
    return pl.pallas_call(
        functools.partial(whole_body, dims, norm, q.shape[1] // k.shape[1], tq, sub),
        out_shape=jax.ShapeDtypeStruct((half // nb + 16, hidden), f32),
        in_specs=[block(pltpu.SMEM)] * 4 + [block(pltpu.HBM)] * 4 + [block(vm)] * 2,
        out_specs=block(vm),
        scratch_shapes=[
            vm((rows, columns), bf16),
            vm((n, rows, size), bf16),
            vm((n, rows, size), bf16),
            vm((chips, rows, size), bf16),
            vm((slots, deep, hidden), bf16),
            vm((rows, hidden), f32),
            vm((heads, rows), f32),
            vm((rows, hidden), f32),
            vm((rows, hidden), bf16),
            vm((n * rows, size), bf16),
            vm((n * rows, size), bf16),
            tuple(vm((n * rows, tq), f32) for _ in range(3)),
            vm((n, rows, 128), f32),
            vm((n, 1, rows), f32),
            vm((n, 1, rows), f32),
            vm((chips, rows, feats), bf16),
            vm((n, 1, rows), f32),
            vm((heads, rows), f32),
            tuple(vm((tokens, w), bf16) for w in widths),
            vm((feats, tokens), bf16),
            tuple(vm((feats, w), f32) for w in widths),
            tuple(vm((half, w), f32) for w in widths),
            tuple(vm((nb - 1, half // nb, w), f32) for w in widths),
            vm((2, heads, sw), f32),
            vm((2, heads, sw), f32),
            vm((heads, sw), f32),
            vm((nz, heads, sw), f32),
            vm((ny, heads, sw), f32),
            vm((nb, heads, sw), f32),
            dma((slots,)), dma((3,)),
            dma((3, chips)), dma((3, chips)),
            dma((2, chips)), dma((2, chips)),
            dma((chips,)), dma((chips,)),
            dma((n,)), dma((n,)),
            dma((chunks * 40,)), dma((chunks * 40,)),
            dma((chunks,)), dma((chunks,)),
            dma((chunks, nb - 1)), dma((chunks, nb - 1)),
            dma((12,)), dma((12,)),
        ],
        compiler_params=pltpu.CompilerParams(collective_id=1, has_side_effects=True, vmem_limit_bytes=60 * 2**20),
        name="whole",
    )(order, inverse, limit, bias, q, k, v, w_in, b_in, w2t)


def apart_body(own, heads, out_ref, grad_ref, ow_ref, gb_ref, bias_ref):
    grad_ref[...] = out_ref[:own]
    ow_ref[...] = out_ref[own:own + heads]
    gb_ref[...] = out_ref[own + heads:own + heads + 1]
    bias_ref[...] = out_ref[own + heads + 1:own + heads + 2, :heads]


def apart(own, heads, out):
    hidden = out.shape[1]
    shapes = ((own, hidden), (heads, hidden), (1, hidden), (1, heads))
    return pl.pallas_call(
        functools.partial(apart_body, own, heads),
        out_shape=tuple(jax.ShapeDtypeStruct(one, jnp.float32) for one in shapes),
        in_specs=[pl.BlockSpec(memory_space=pltpu.VMEM)],
        out_specs=[pl.BlockSpec(memory_space=pltpu.VMEM)] * 4,
        name="apart",
    )(out)


def on_device(dims, queries, keys, values, lengths, block_pos, w_in, b_in, output_weight, output_bias):
    hidden, heads = output_weight.shape
    total = lax.axis_size("seq") * queries.shape[1]
    norm = 1.0 / math.sqrt(lax.axis_size("batch") * total)
    order = block_pos[0]
    stored = jnp.arange(order.shape[0], dtype=jnp.int32)
    inverse = jnp.sum(jnp.where(order[None, :] == stored[:, None], stored[None, :], 0), axis=1)
    out = whole(
        dims, norm, order, inverse, lengths, output_bias, queries[0], keys[0], values[0], w_in, b_in[None, :], output_weight.T
    )
    own = out.shape[0] - 16
    grad, ow, gb, bias = apart(own, heads, out)
    return (grad, gb.reshape(hidden), ow.T, bias.reshape(heads))


def solution(mesh):
    nb = mesh.shape["batch"]
    ny = nz = math.isqrt(mesh.shape["seq"] // 2)
    return jax.shard_map(
        functools.partial(on_device, (ny, nz, nb)),
        mesh=mesh,
        in_specs=(
            P("batch", "seq", None),
            P("batch", "seq", None),
            P("batch", "seq", None),
            P("batch"),
            P("batch", None),
            P(),
            P(),
            P(),
            P(),
        ),
        out_specs=(P(("seq", "batch"), None), P(), P(), P()),
        check_vma=False,
    )
```

```python
import functools
import math

import jax
import jax.numpy as jnp
from jax import lax
from jax.experimental import pallas as pl
from jax.experimental.pallas import tpu as pltpu
from jax.sharding import PartitionSpec as P

NEG = -1e30
MESH = pl.DeviceIdType.MESH


def remote(src, dst, send_sem, recv_sem, device):
    return pltpu.make_async_remote_copy(
        src_ref=src, dst_ref=dst, send_sem=send_sem, recv_sem=recv_sem, device_id=device, device_id_type=MESH
    )


def attn_core(tq, sub, total, scale2, limit, qs, ks, bufs, acc_ref, done=None):
    lanes = 128
    groups = tq // lanes
    nt = total // tq
    eights = lambda x: x.reshape(x.shape[0] // 8, 8, tq)

    def at(j, n=tq):
        return pl.ds(pl.multiple_of(j * n, n), n)

    def scores(i, j, mx, masked):
        s = lax.dot_general(ks[at(j), :], qs[at(i), :], (((1,), (1,)), ((), ())), preferred_element_type=jnp.float32)
        if masked:
            kp = lax.broadcasted_iota(jnp.int32, (tq, tq), 0)
            qp = lax.broadcasted_iota(jnp.int32, (tq, tq), 1)
            s = jnp.where(kp <= qp, s, NEG)
        bufs[i % 3][at(j), :] = s
        return jnp.maximum(mx, jnp.max(eights(s), axis=0))

    def weights(i, j, l, top):
        buf = bufs[i % 3]
        for u in range(tq // sub):
            here = pl.ds(pl.multiple_of(j * tq + u * sub, sub), sub)
            w = jnp.exp2((eights(buf[here, :]) - top[None]) * scale2)
            buf[here, :] = w.reshape(sub, tq)
            l = l + jnp.sum(w, axis=0)
        return l

    def shares(i, j, rec):
        buf = bufs[i % 3]
        for u in range(tq // sub):
            here = pl.ds(pl.multiple_of(j * tq + u * sub, sub), sub)
            w = (eights(buf[here, :]) * rec[None]).reshape(sub, tq)
            tot = w[:, :lanes]
            for g in range(1, groups):
                tot = tot + w[:, g * lanes:(g + 1) * lanes]
            acc_ref[j * (tq // sub) + u] += tot

    def spread_top(mx):
        return jnp.broadcast_to(jnp.max(mx, axis=0, keepdims=True), (8, tq))

    def spread_rec(i, l):
        pos = i * tq + lax.broadcasted_iota(jnp.int32, (1, tq), 1)
        rec = jnp.where(pos < limit, 1.0 / jnp.sum(l, axis=0, keepdims=True), 0.0)
        return jnp.broadcast_to(rec, (8, tq))

    top = rec = None
    for i in range(nt - 1, -3, -1):
        first, second, third = i >= 0, 0 <= i + 1 < nt, i + 2 < nt

        def each(j, carry, i=i, first=first, second=second, third=third, top=top, rec=rec):
            mx, l = carry
            if first:
                mx = scores(i, j, mx, False)
            if second:
                l = weights(i + 1, j, l, top)
            if third:
                shares(i + 2, j, rec)
            return mx, l

        mx = jnp.full((8, tq), NEG, jnp.float32)
        l = jnp.zeros((8, tq), jnp.float32)
        if i > 0:
            mx, l = lax.fori_loop(0, i, each, (mx, l))
        if first:
            mx = scores(i, i, mx, True)
        for d in (0, 1, 2):
            if second and d < 2 and i + d >= 0:
                l = weights(i + 1, i + d, l, top)
            if third and i + d >= 0:
                shares(i + 2, i + d, rec)
        if third and done is not None:
            done(i + 2)
        top, rec = spread_top(mx), spread_rec(i + 1, l)


def whole_body(dims, norm, per, tq, sub, order_ref, bias_ref, limit_ref, q_hbm, k_hbm, v_hbm, w_hbm, bin_ref, w2t_ref, out_ref,
               feat, qa, ka, stage, wbuf, pre, pred_ref, slope_ref, act_ref, qs, ks, bufs, acc_ref, msort, mass_ref, f_ref,
               mrecv, lab, dl, ft, part, pair, xrecv, sm, small, smr, zs, ys, xs,
               w_sem, in_sem, i_send, i_recv, d_send, d_recv, f_send, f_recv,
               m_send, m_recv, g_send, g_recv, p_send, p_recv, x_send, x_recv, s_send, s_recv):
    ny, nz, nb = dims
    chips = ny * nz
    n = chips * 2
    s, b = lax.axis_index("seq"), lax.axis_index("batch")
    core, c = lax.rem(s, 2), s // 2
    z, y = lax.rem(c, nz), c // nz
    rows, hidden = slope_ref.shape
    head = ka.shape[2]
    q_cols, k_cols = q_hbm.shape[1], k_hbm.shape[1]
    slots, deep = wbuf.shape[:2]
    steps = w_hbm.shape[0] // deep
    chunks, tokens = len(dl), dl[0].shape[0]
    feats = part[0].shape[0]
    begin = [sum(d.shape[1] for d in dl[:j]) for j in range(chunks + 1)]
    half = feats // 2
    own_rows = half // nb
    partner = (s + 1 - 2 * core, b)

    barrier = pltpu.get_barrier_semaphore()

    def greet(r, _):
        pl.semaphore_signal(barrier, inc=1, device_id=(lax.rem(s + r, n), b), device_id_type=MESH)
        return 0
    lax.fori_loop(1, n, greet, 0)
    for r in range(1, nb):
        pl.semaphore_signal(barrier, inc=1, device_id=(s, lax.rem(b + r, nb)), device_id_type=MESH)

    inputs = []
    at = 0
    for i, ref in enumerate((q_hbm, k_hbm, v_hbm)):
        inputs.append(pltpu.make_async_copy(ref, feat.at[:, at:at + ref.shape[1]], in_sem.at[i]))
        at += ref.shape[1]
    for one in inputs:
        one.start()

    def w_copy(i):
        at = lax.rem(i, slots)
        return pltpu.make_async_copy(w_hbm.at[pl.ds(pl.multiple_of(i * deep, deep), deep), :], wbuf.at[at], w_sem.at[at])

    for i in range(slots):
        w_copy(i).start()
    acc_ref[...] = jnp.zeros_like(acc_ref)
    pre[...] = jnp.broadcast_to(bin_ref[...], pre.shape)
    for one in inputs:
        one.wait()

    hops = lambda d: -min(d[0], ny - d[0]) - min(d[1], nz - d[1])
    away = sorted(((dy, dz) for dy in range(ny) for dz in range(nz) if dy or dz), key=hops)

    def chip_at(d, sign):
        dy, dz = d
        return lax.rem(y + sign * dy + ny, ny) * nz + lax.rem(z + sign * dz + nz, nz)

    def columns(i):
        return pl.ds(pl.multiple_of(i * head, head), head)

    def parts(to):
        return (columns(2 * to + core), columns(2 * to + 1 - core), columns(q_cols // head + (2 * to) // per))

    own_q, other_q, own_k = parts(c)
    qa[s] = feat[:, own_q]
    ka[s] = feat[:, own_k]
    mine = pl.ds(pl.multiple_of(c * feats, feats), feats)
    f_ref[c] = feat[:, mine]
    pl.semaphore_wait(barrier, n - 1 + nb - 1)

    def arrivals(frm):
        return (qa.at[2 * frm + core], stage.at[frm], ka.at[2 * frm + core])

    def across(i, to, frm):
        return remote(feat.at[:, parts(to)[i]], arrivals(frm)[i], i_send.at[i, to], i_recv.at[i, frm], (2 * to + core, b))

    for some in ((1, 2), (0,)):
        for d in away:
            for i in some:
                across(i, chip_at(d, 1), c).start()

    def over(i, src, at, whose):
        dst = (qa.at[2 * at + whose], ka.at[2 * at + whose])[i]
        return remote(src, dst, d_send.at[i, at], d_recv.at[i, at], partner)

    over(0, feat.at[:, other_q], c, core).start()
    over(1, feat.at[:, own_k], c, core).start()

    def step(i, _):
        w_copy(i).wait()
        x = feat[:, pl.ds(pl.multiple_of(i * deep, deep), deep)]
        pre[...] += jnp.dot(x, wbuf[lax.rem(i, slots)], preferred_element_type=jnp.float32)

        @pl.when(i + slots < steps)
        def _():
            w_copy(i + slots).start()
        return 0
    lax.fori_loop(0, steps, step, 0)
    p = pre[...]
    sig = jax.nn.sigmoid(p)
    act = (p * sig).astype(jnp.bfloat16)
    act_ref[...] = act
    slope_ref[...] = sig * (1.0 + p * (1.0 - sig))
    out = lax.dot_general(w2t_ref[...], act, (((1,), (1,)), ((), ())), preferred_element_type=jnp.float32)
    for g in range(pred_ref.shape[0]):
        pred_ref[g:g + 1, :] = out[g:g + 1, :] + bias_ref[g]

    for d in away:
        frm = chip_at(d, -1)
        across(1, frm, frm).wait_recv()
        over(0, stage.at[frm], frm, core).start()
        across(2, frm, frm).wait_recv()
        over(1, ka.at[2 * frm + core], frm, core).start()

    def all_others(r):
        return lax.rem(c + r, chips)

    def settle(r, _):
        across(0, all_others(r), all_others(r)).wait_recv()
        for i in range(3):
            across(i, all_others(r), c).wait_send()
        return 0
    lax.fori_loop(1, chips, settle, 0)

    def settle_over(at, _):
        over(0, stage.at[at], at, 1 - core).wait()
        over(1, ka.at[2 * at + core], at, 1 - core).wait()
        return 0
    lax.fori_loop(0, chips, settle_over, 0)

    def f_copy(to, frm):
        cut = pl.ds(pl.multiple_of(to * feats, feats), feats)
        return remote(feat.at[:, cut], f_ref.at[frm], f_send.at[to], f_recv.at[frm], (2 * to + core, b))

    for d in away:
        f_copy(chip_at(d, 1), c).start()

    def sort(at, _):
        stored = jnp.int32(0)
        for k in range(1, n):
            stored = stored + k * jnp.maximum(1 - jnp.abs(order_ref[k] - at), 0)
        here = pl.ds(pl.multiple_of(at * rows, rows), rows)
        stored = jnp.minimum(stored, n - 1)
        qs[here, :] = qa[stored]
        ks[here, :] = ka[stored]
        return 0
    lax.fori_loop(0, n, sort, 0)

    scale2 = math.log2(math.e) / math.sqrt(head)

    def done(i):
        for u in range(i * (tq // rows), (i + 1) * (tq // rows)):
            msort[u] = jnp.sum(acc_ref[u].T, axis=0, keepdims=True)

    attn_core(tq, sub, n * rows, scale2, limit_ref[...], qs, ks, bufs, acc_ref, done)

    def emit(at, _):
        mass_ref[at] = msort[order_ref[at]]
        return 0
    lax.fori_loop(0, n, emit, 0)

    def mass_copy(r, sender):
        to = lax.rem(s + r, n)
        return remote(mass_ref.at[to], mrecv.at[s], m_send.at[r], m_recv.at[s], (to, b))

    def mass_start(r, _):
        mass_copy(r, s).start()
        return 0
    lax.fori_loop(1, n, mass_start, 0)
    mrecv[s] = mass_ref[s]

    def f_wait(r, _):
        f_copy(all_others(r), all_others(r)).wait_recv()
        f_copy(all_others(r), c).wait_send()
        return 0
    lax.fori_loop(1, chips, f_wait, 0)
    for k in range(tokens // rows):
        ft[:, k * rows:(k + 1) * rows] = f_ref[k].T

    def mass_wait(r, _):
        frm = lax.rem(s + n - r, n)
        got = remote(mass_ref.at[frm], mrecv.at[frm], m_send.at[r], m_recv.at[frm], (frm, b))
        got.wait_recv()
        return 0
    lax.fori_loop(1, n, mass_wait, 0)

    heads = lab.shape[0]
    per = n // heads
    for g in range(heads):
        total = mrecv[per * g]
        for i in range(1, per):
            total = total + mrecv[per * g + i]
        lab[g:g + 1, :] = jnp.log1p(total)
    position = order_ref[s] * rows + lax.broadcasted_iota(jnp.int32, (1, rows), 1)
    live = jnp.where(position < limit_ref[...], 1.0, 0.0)
    resid_t = ((pred_ref[...] - lab[...]) * live * norm).astype(jnp.bfloat16)
    resid = resid_t.astype(jnp.float32).T.astype(jnp.bfloat16)
    back = jnp.dot(resid, w2t_ref[...], preferred_element_type=jnp.float32)
    delta = (back * slope_ref[...]).astype(jnp.bfloat16)
    here = pl.ds(pl.multiple_of(c * rows, rows), rows)
    for j in range(chunks):
        dl[j][here, :] = delta[:, begin[j]:begin[j + 1]]

    wide = rows // 2
    slot = {}

    def number(*key):
        return slot.setdefault(key, len(slot))

    def spot(half_id, a, e):
        return (a * nz + e) if half_id == 0 else (e * nz + a)

    def ring(v, d, size):
        return lax.rem(v + (d + size), size)

    def coords(half_id):
        return (y, z, ny, nz) if half_id == 0 else (z, y, nz, ny)

    def piece(j, block, half_id, quarter):
        r0 = half_id * wide + (quarter * (wide // 2) if quarter is not None else 0)
        size = wide // 2 if quarter is not None else wide
        return dl[j].at[pl.ds(pl.multiple_of(block * rows + r0, wide // 2), size), :]

    def neighbour(half_id, which, d):
        along_y = (half_id == 0) == (which == 0)
        to_y = ring(y, d, ny) if along_y else y
        to_z = z if along_y else ring(z, d, nz)
        return ((to_y * nz + to_z) * 2 + core, b)

    started = []

    def copy(j, half_id, which, da, de, quarter, d):
        a, e, na, ne = coords(half_id)
        block = spot(half_id, ring(a, da, na), ring(e, de, ne))
        ref = piece(j, block, half_id, quarter)
        m = number(j, half_id, which, da, de, quarter, d)
        return remote(ref, ref, g_send.at[m], g_recv.at[m], neighbour(half_id, which, d))

    def send(j, half_id, which, da, de, quarter, d):
        one = copy(j, half_id, which, da, de, quarter, d)
        one.start()
        started.append(one)

    def receive(j, half_id, which, da, de, quarter, d):
        a, e, na, ne = coords(half_id)
        back_a, back_e = (da - d, de) if which == 0 else (da, de - d)
        block = spot(half_id, ring(a, back_a, na), ring(e, back_e, ne))
        ref = piece(j, block, half_id, quarter)
        m = number(j, half_id, which, da, de, quarter, d)
        remote(ref, ref, g_send.at[m], g_recv.at[m], neighbour(half_id, which, -d)).wait_recv()

    def second(j, h, da):
        for d in (1, -1):
            send(j, h, 1, da, 0, None, d)

    def second_pass_on(j, h, da):
        receive(j, h, 1, da, 0, None, 1)
        send(j, h, 1, da, -1, 0, 1)
        receive(j, h, 1, da, 0, None, -1)
        send(j, h, 1, da, 1, 1, -1)

    def second_end(j, h, da):
        receive(j, h, 1, da, -1, 0, 1)
        receive(j, h, 1, da, 1, 1, -1)

    def stage0(j):
        for h in (0, 1):
            for d in (1, -1):
                send(j, h, 0, 0, 0, None, d)
        for h in (0, 1):
            second(j, h, 0)

    def stage1(j):
        for h in (0, 1):
            receive(j, h, 0, 0, 0, None, 1)
            send(j, h, 0, -1, 0, 0, 1)
            second(j, h, -1)
            receive(j, h, 0, 0, 0, None, -1)
            send(j, h, 0, 1, 0, 1, -1)
            second(j, h, 1)

    def stage2(j):
        for h in (0, 1):
            second_pass_on(j, h, 0)
        for h in (0, 1):
            receive(j, h, 0, -1, 0, 0, 1)
            receive(j, h, 0, 1, 0, 1, -1)
            second(j, h, 2)

    def stage3(j):
        for da in (-1, 1):
            for h in (0, 1):
                second_pass_on(j, h, da)

    def stage4(j):
        for h in (0, 1):
            second_pass_on(j, h, 2)

    def stage5(j):
        for da in (0, -1, 1, 2):
            for h in (0, 1):
                second_end(j, h, da)

    def multiply(j):
        part[j][...] = jnp.dot(ft[...], dl[j][...], preferred_element_type=jnp.float32)

    def pair_copy(j, of):
        ref = part[j].at[pl.ds(pl.multiple_of((1 - of) * half, half), half), :]
        return remote(ref, pair[j], p_send.at[j], p_recv.at[j], partner)

    def pair_start(j):
        one = pair_copy(j, core)
        one.start()
        started.append(one)

    def x_copy(j, r):
        to = lax.rem(b + r, nb)
        ref = pair[j].at[pl.ds(pl.multiple_of(to * own_rows, own_rows), own_rows), :]
        return remote(ref, xrecv[j].at[r - 1], x_send.at[j, r - 1], x_recv.at[j, r - 1], (s, to))

    def x_start(j):
        pair_copy(j, core).wait_recv()
        pair[j][...] = pair[j][...] + part[j][pl.ds(pl.multiple_of(core * half, half), half), :]
        for r in (2, 1, 3)[: nb - 1]:
            one = x_copy(j, r)
            one.start()
            started.append(one)

    def x_end(j):
        for r in range(1, nb):
            x_copy(j, r).wait_recv()
        own = pair[j][pl.ds(pl.multiple_of(b * own_rows, own_rows), own_rows), :]
        for r in range(1, nb):
            own = own + xrecv[j][r - 1]
        out_ref[:own_rows, begin[j]:begin[j + 1]] = own

    def small_start0():
        sw = sm.shape[2]
        out_term = jnp.dot(resid_t, act_ref[...], preferred_element_type=jnp.float32)
        sums = jnp.sum(delta.astype(jnp.float32), axis=0, keepdims=True)
        bias = jnp.sum(resid.astype(jnp.float32), axis=0, keepdims=True)
        lanes = 128
        cols = [out_term[:, k * lanes:(k + 1) * lanes] for k in range(hidden // lanes)]
        cols.append(jnp.concatenate([sums[:, k * lanes:(k + 1) * lanes] for k in range(hidden // lanes)], axis=0))
        cols.append(jnp.zeros((heads, lanes), jnp.float32))
        each = sw // lanes
        for k, value in enumerate(cols):
            sm[k // each, :, (k % each) * lanes:(k % each + 1) * lanes] = value
        at = (len(cols) - 1) % each * lanes
        sm[1, 0:1, at:at + heads] = bias
        one = remote(sm.at[1 - core], smr, s_send.at[0], s_recv.at[0], partner)
        one.start()
        started.append(one)

    def small_hop(level, value, buf, at, size, target):
        buf[at] = value
        for r in range(1, size):
            one = remote(buf.at[at], buf.at[at], s_send.at[level * 3 + r], s_recv.at[level * 3 + r], target(r))
            one.start()
            started.append(one)

    def small_sum(level, buf, at, size, target):
        for r in range(1, size):
            frm = lax.rem(at + size - r, size)
            remote(buf.at[frm], buf.at[frm], s_send.at[level * 3 + r], s_recv.at[level * 3 + r], target(r)).wait_recv()
        total = buf[0]
        for k in range(1, size):
            total = total + buf[k]
        return total

    to_z = lambda r: ((y * nz + lax.rem(z + r, nz)) * 2 + core, b)
    to_y = lambda r: ((lax.rem(y + r, ny) * nz + z) * 2 + core, b)
    to_x = lambda r: (s, lax.rem(b + r, nb))

    def small1():
        remote(sm.at[1 - core], smr, s_send.at[0], s_recv.at[0], partner).wait_recv()
        small_hop(0, sm[core] + smr[...], zs, z, nz, to_z)

    def small2():
        small_hop(1, small_sum(0, zs, z, nz, to_z), ys, y, ny, to_y)

    def small3():
        small_hop(2, small_sum(1, ys, y, ny, to_y), xs, b, nb, to_x)

    def small4():
        sm[core] = small_sum(2, xs, b, nb, to_x)
        one = remote(sm.at[core], small.at[core], s_send.at[10], s_recv.at[10], partner)
        one.start()
        started.append(one)
        small[core] = sm[core]

    def small5():
        remote(sm.at[1 - core], small.at[1 - core], s_send.at[10], s_recv.at[10], partner).wait_recv()
        sw = small.shape[2]
        out_ref[own_rows:own_rows + heads, :sw] = small[0]
        out_ref[own_rows:own_rows + heads, sw:] = small[1, :, :hidden - sw]
        base = own_rows + heads
        lanes = 128
        for k in range(hidden // lanes):
            out_ref[base:base + 1, k * lanes:(k + 1) * lanes] = small[1, k:k + 1, hidden - sw:hidden - sw + lanes]
        out_ref[base + 1:base + 2, :lanes] = small[1, 0:1, hidden - sw + lanes:hidden - sw + 2 * lanes]

    stage0(0)
    stage0(1)
    small_start0()
    stage1(0)
    stage2(0)
    stage1(1)
    small1()
    stage3(0)
    stage2(1)
    stage4(0)
    small2()
    stage3(1)
    stage5(0)
    multiply(0)
    pair_start(0)
    stage4(1)
    small3()
    x_start(0)
    stage5(1)
    multiply(1)
    pair_start(1)
    small4()
    x_start(1)
    x_end(0)
    small5()
    x_end(1)

    for one in started:
        one.wait_send()

    def mass_drain(r, _):
        mass_copy(r, s).wait_send()
        return 0
    lax.fori_loop(1, n, mass_drain, 0)


def whole(dims, norm, order, bias, limit, q, k, v, w_in, b_in, w2t, tq=512, sub=128, widths=(512, 512), slots=3, deep=512):
    ny, nz, nb = dims
    rows, hidden = q.shape[0], w_in.shape[1]
    heads = w2t.shape[0]
    size = k.shape[1] // heads
    chips = ny * nz
    n = 2 * chips
    tokens = chips * rows
    columns = w_in.shape[0]
    feats = columns // chips
    half = feats // 2
    chunks = len(widths)
    sw = (hidden + 256) // 2
    vm, dma = pltpu.VMEM, pltpu.SemaphoreType.DMA
    block = lambda space: pl.BlockSpec(memory_space=space)
    f32, bf16 = jnp.float32, jnp.bfloat16
    return pl.pallas_call(
        functools.partial(whole_body, dims, norm, q.shape[1] // k.shape[1], tq, sub),
        out_shape=jax.ShapeDtypeStruct((half // nb + 16, hidden), f32),
        in_specs=[block(pltpu.SMEM)] * 2 + [block(vm)] + [block(pltpu.HBM)] * 4 + [block(vm)] * 2,
        out_specs=block(vm),
        scratch_shapes=[
            vm((rows, columns), bf16),
            vm((n, rows, size), bf16),
            vm((n, rows, size), bf16),
            vm((chips, rows, size), bf16),
            vm((slots, deep, hidden), bf16),
            vm((rows, hidden), f32),
            vm((heads, rows), f32),
            vm((rows, hidden), f32),
            vm((rows, hidden), bf16),
            vm((n * rows, size), bf16),
            vm((n * rows, size), bf16),
            tuple(vm((n * rows, tq), f32) for _ in range(3)),
            vm((n, rows, 128), f32),
            vm((n, 1, rows), f32),
            vm((n, 1, rows), f32),
            vm((chips, rows, feats), bf16),
            vm((n, 1, rows), f32),
            vm((heads, rows), f32),
            tuple(vm((tokens, w), bf16) for w in widths),
            vm((feats, tokens), bf16),
            tuple(vm((feats, w), f32) for w in widths),
            tuple(vm((half, w), f32) for w in widths),
            tuple(vm((nb - 1, half // nb, w), f32) for w in widths),
            vm((2, heads, sw), f32),
            vm((2, heads, sw), f32),
            vm((heads, sw), f32),
            vm((nz, heads, sw), f32),
            vm((ny, heads, sw), f32),
            vm((nb, heads, sw), f32),
            dma((slots,)), dma((3,)),
            dma((3, chips)), dma((3, chips)),
            dma((2, chips)), dma((2, chips)),
            dma((chips,)), dma((chips,)),
            dma((n,)), dma((n,)),
            dma((chunks * 40,)), dma((chunks * 40,)),
            dma((chunks,)), dma((chunks,)),
            dma((chunks, nb - 1)), dma((chunks, nb - 1)),
            dma((12,)), dma((12,)),
        ],
        compiler_params=pltpu.CompilerParams(collective_id=1, has_side_effects=True, vmem_limit_bytes=60 * 2**20),
        name="whole",
    )(order, bias, limit, q, k, v, w_in, b_in, w2t)


def apart_body(own, heads, out_ref, grad_ref, ow_ref, gb_ref, bias_ref):
    grad_ref[...] = out_ref[:own]
    ow_ref[...] = out_ref[own:own + heads]
    gb_ref[...] = out_ref[own + heads:own + heads + 1]
    bias_ref[...] = out_ref[own + heads + 1:own + heads + 2, :heads]


def apart(own, heads, out):
    hidden = out.shape[1]
    shapes = ((own, hidden), (heads, hidden), (1, hidden), (1, heads))
    return pl.pallas_call(
        functools.partial(apart_body, own, heads),
        out_shape=tuple(jax.ShapeDtypeStruct(one, jnp.float32) for one in shapes),
        in_specs=[pl.BlockSpec(memory_space=pltpu.VMEM)],
        out_specs=[pl.BlockSpec(memory_space=pltpu.VMEM)] * 4,
        name="apart",
    )(out)


def on_device(dims, queries, keys, values, lengths, block_pos, w_in, b_in, output_weight, output_bias):
    hidden, heads = output_weight.shape
    total = lax.axis_size("seq") * queries.shape[1]
    norm = 1.0 / math.sqrt(lax.axis_size("batch") * total)
    out = whole(
        dims, norm, block_pos[0], output_bias, lengths[None, :], queries[0], keys[0], values[0], w_in, b_in[None, :], output_weight.T
    )
    own = out.shape[0] - 16
    grad, ow, gb, bias = apart(own, heads, out)
    return (grad, gb.reshape(hidden), ow.T, bias.reshape(heads))


def solution(mesh):
    nb = mesh.shape["batch"]
    ny = nz = math.isqrt(mesh.shape["seq"] // 2)
    return jax.shard_map(
        functools.partial(on_device, (ny, nz, nb)),
        mesh=mesh,
        in_specs=(
            P("batch", "seq", None),
            P("batch", "seq", None),
            P("batch", "seq", None),
            P("batch"),
            P("batch", None),
            P(),
            P(),
            P(),
            P(),
        ),
        out_specs=(P(("seq", "batch"), None), P(), P(), P()),
        check_vma=False,
    )
```

```python
import functools
import math

import jax
import jax.numpy as jnp
from jax import lax
from jax.experimental import pallas as pl
from jax.experimental.pallas import tpu as pltpu
from jax.sharding import PartitionSpec as P

NEG = -1e30
MESH = pl.DeviceIdType.MESH


def remote(src, dst, send_sem, recv_sem, device):
    return pltpu.make_async_remote_copy(
        src_ref=src, dst_ref=dst, send_sem=send_sem, recv_sem=recv_sem, device_id=device, device_id_type=MESH
    )


def attn_core(tq, sub, total, scale2, limit, qs, ks, bufs, acc_ref, done=None):
    lanes = 128
    groups = tq // lanes
    nt = total // tq
    eights = lambda x: x.reshape(x.shape[0] // 8, 8, tq)

    def at(j, n=tq):
        return pl.ds(pl.multiple_of(j * n, n), n)

    def scores(i, j, mx, masked):
        s = lax.dot_general(ks[at(j), :], qs[at(i), :], (((1,), (1,)), ((), ())), preferred_element_type=jnp.float32)
        if masked:
            kp = lax.broadcasted_iota(jnp.int32, (tq, tq), 0)
            qp = lax.broadcasted_iota(jnp.int32, (tq, tq), 1)
            s = jnp.where(kp <= qp, s, NEG)
        bufs[i % 3][at(j), :] = s
        return jnp.maximum(mx, jnp.max(eights(s), axis=0))

    def weights(i, j, l, top):
        buf = bufs[i % 3]
        for u in range(tq // sub):
            here = pl.ds(pl.multiple_of(j * tq + u * sub, sub), sub)
            w = jnp.exp2((eights(buf[here, :]) - top[None]) * scale2)
            buf[here, :] = w.reshape(sub, tq)
            l = l + jnp.sum(w, axis=0)
        return l

    def shares(i, j, rec):
        buf = bufs[i % 3]
        for u in range(tq // sub):
            here = pl.ds(pl.multiple_of(j * tq + u * sub, sub), sub)
            w = (eights(buf[here, :]) * rec[None]).reshape(sub, tq)
            tot = w[:, :lanes]
            for g in range(1, groups):
                tot = tot + w[:, g * lanes:(g + 1) * lanes]
            acc_ref[j * (tq // sub) + u] += tot

    def spread_top(mx):
        return jnp.broadcast_to(jnp.max(mx, axis=0, keepdims=True), (8, tq))

    def spread_rec(i, l):
        pos = i * tq + lax.broadcasted_iota(jnp.int32, (1, tq), 1)
        rec = jnp.where(pos < limit, 1.0 / jnp.sum(l, axis=0, keepdims=True), 0.0)
        return jnp.broadcast_to(rec, (8, tq))

    top = rec = None
    for i in range(nt - 1, -3, -1):
        first, second, third = i >= 0, 0 <= i + 1 < nt, i + 2 < nt

        def each(j, carry, i=i, first=first, second=second, third=third, top=top, rec=rec):
            mx, l = carry
            if first:
                mx = scores(i, j, mx, False)
            if second:
                l = weights(i + 1, j, l, top)
            if third:
                shares(i + 2, j, rec)
            return mx, l

        mx = jnp.full((8, tq), NEG, jnp.float32)
        l = jnp.zeros((8, tq), jnp.float32)
        if i > 0:
            mx, l = lax.fori_loop(0, i, each, (mx, l))
        if first:
            mx = scores(i, i, mx, True)
        for d in (0, 1, 2):
            if second and d < 2 and i + d >= 0:
                l = weights(i + 1, i + d, l, top)
            if third and i + d >= 0:
                shares(i + 2, i + d, rec)
        if third and done is not None:
            done(i + 2)
        top, rec = spread_top(mx), spread_rec(i + 1, l)


def whole_body(dims, norm, per, tq, sub, order_ref, bias_ref, limit_ref, q_hbm, k_hbm, v_hbm, w_hbm, bin_ref, w2t_ref, out_ref,
               feat, qa, ka, stage, wbuf, pre, pred_ref, slope_ref, act_ref, inv, qs, ks, bufs, acc_ref, msort, mass_ref, f_ref,
               mrecv, lab, dl, ft, part, pair, xrecv, sm, small, smr, zs, ys, xs,
               w_sem, in_sem, i_send, i_recv, d_send, d_recv, f_send, f_recv,
               m_send, m_recv, g_send, g_recv, p_send, p_recv, x_send, x_recv, s_send, s_recv):
    ny, nz, nb = dims
    chips = ny * nz
    n = chips * 2
    s, b = lax.axis_index("seq"), lax.axis_index("batch")
    core, c = lax.rem(s, 2), s // 2
    z, y = lax.rem(c, nz), c // nz
    rows, hidden = slope_ref.shape
    head = ka.shape[2]
    q_cols, k_cols = q_hbm.shape[1], k_hbm.shape[1]
    slots, deep = wbuf.shape[:2]
    steps = w_hbm.shape[0] // deep
    chunks, tokens = len(dl), dl[0].shape[0]
    feats = part[0].shape[0]
    begin = [sum(d.shape[1] for d in dl[:j]) for j in range(chunks + 1)]
    half = feats // 2
    own_rows = half // nb
    partner = (s + 1 - 2 * core, b)

    barrier = pltpu.get_barrier_semaphore()

    def greet(r, _):
        pl.semaphore_signal(barrier, inc=1, device_id=(lax.rem(s + r, n), b), device_id_type=MESH)
        return 0
    lax.fori_loop(1, n, greet, 0)
    for r in range(1, nb):
        pl.semaphore_signal(barrier, inc=1, device_id=(s, lax.rem(b + r, nb)), device_id_type=MESH)

    inputs = []
    at = 0
    for i, ref in enumerate((q_hbm, k_hbm, v_hbm)):
        inputs.append(pltpu.make_async_copy(ref, feat.at[:, at:at + ref.shape[1]], in_sem.at[i]))
        at += ref.shape[1]
    for one in inputs:
        one.start()

    def w_copy(i):
        at = lax.rem(i, slots)
        return pltpu.make_async_copy(w_hbm.at[pl.ds(pl.multiple_of(i * deep, deep), deep), :], wbuf.at[at], w_sem.at[at])

    for i in range(slots):
        w_copy(i).start()
    acc_ref[...] = jnp.zeros_like(acc_ref)
    pre[...] = jnp.broadcast_to(bin_ref[...], pre.shape)
    for one in inputs:
        one.wait()

    hops = lambda d: -min(d[0], ny - d[0]) - min(d[1], nz - d[1])
    away = sorted(((dy, dz) for dy in range(ny) for dz in range(nz) if dy or dz), key=hops)

    def chip_at(d, sign):
        dy, dz = d
        return lax.rem(y + sign * dy + ny, ny) * nz + lax.rem(z + sign * dz + nz, nz)

    def columns(i):
        return pl.ds(pl.multiple_of(i * head, head), head)

    def parts(to):
        return (columns(2 * to + core), columns(2 * to + 1 - core), columns(q_cols // head + (2 * to) // per))

    own_q, other_q, own_k = parts(c)
    qa[s] = feat[:, own_q]
    ka[s] = feat[:, own_k]
    mine = pl.ds(pl.multiple_of(c * feats, feats), feats)
    f_ref[c] = feat[:, mine]
    pl.semaphore_wait(barrier, n - 1 + nb - 1)

    def arrivals(frm):
        return (qa.at[2 * frm + core], stage.at[frm], ka.at[2 * frm + core])

    def across(i, to, frm):
        return remote(feat.at[:, parts(to)[i]], arrivals(frm)[i], i_send.at[i, to], i_recv.at[i, frm], (2 * to + core, b))

    for some in ((1,), (2,), (0,)):
        for d in away:
            for i in some:
                across(i, chip_at(d, 1), c).start()

    def over(i, src, at, whose):
        dst = (qa.at[2 * at + whose], ka.at[2 * at + whose])[i]
        return remote(src, dst, d_send.at[i, at], d_recv.at[i, at], partner)

    over(0, feat.at[:, other_q], c, core).start()
    over(1, feat.at[:, own_k], c, core).start()

    def find(at, _):
        stored = jnp.int32(0)
        for k in range(1, n):
            stored = stored + k * jnp.maximum(1 - jnp.abs(order_ref[k] - at), 0)
        inv[at] = jnp.minimum(stored, n - 1)
        return 0
    lax.fori_loop(0, n, find, 0)

    def step(i, _):
        w_copy(i).wait()
        x = feat[:, pl.ds(pl.multiple_of(i * deep, deep), deep)]
        pre[...] += jnp.dot(x, wbuf[lax.rem(i, slots)], preferred_element_type=jnp.float32)

        @pl.when(i + slots < steps)
        def _():
            w_copy(i + slots).start()
        return 0
    lax.fori_loop(0, steps, step, 0)
    p = pre[...]
    sig = jax.nn.sigmoid(p)
    act = (p * sig).astype(jnp.bfloat16)
    act_ref[...] = act
    slope_ref[...] = sig * (1.0 + p * (1.0 - sig))
    out = lax.dot_general(w2t_ref[...], act, (((1,), (1,)), ((), ())), preferred_element_type=jnp.float32)
    for g in range(pred_ref.shape[0]):
        pred_ref[g:g + 1, :] = out[g:g + 1, :] + bias_ref[g]

    for d in away:
        frm = chip_at(d, -1)
        across(1, frm, frm).wait_recv()
        over(0, stage.at[frm], frm, core).start()
        across(2, frm, frm).wait_recv()
        over(1, ka.at[2 * frm + core], frm, core).start()

    def all_others(r):
        return lax.rem(c + r, chips)

    def settle(r, _):
        across(0, all_others(r), all_others(r)).wait_recv()
        for i in range(3):
            across(i, all_others(r), c).wait_send()
        return 0
    lax.fori_loop(1, chips, settle, 0)

    def settle_over(at, _):
        over(0, stage.at[at], at, 1 - core).wait()
        over(1, ka.at[2 * at + core], at, 1 - core).wait()
        return 0
    lax.fori_loop(0, chips, settle_over, 0)

    def f_copy(to, frm):
        cut = pl.ds(pl.multiple_of(to * feats, feats), feats)
        return remote(feat.at[:, cut], f_ref.at[frm], f_send.at[to], f_recv.at[frm], (2 * to + core, b))

    for d in away:
        f_copy(chip_at(d, 1), c).start()

    def sort(at, _):
        here = pl.ds(pl.multiple_of(at * rows, rows), rows)
        stored = inv[at]
        qs[here, :] = qa[stored]
        ks[here, :] = ka[stored]
        return 0
    lax.fori_loop(0, n, sort, 0)

    scale2 = math.log2(math.e) / math.sqrt(head)

    def done(i):
        for u in range(i * (tq // rows), (i + 1) * (tq // rows)):
            msort[u] = jnp.sum(acc_ref[u].T, axis=0, keepdims=True)

    attn_core(tq, sub, n * rows, scale2, limit_ref[...], qs, ks, bufs, acc_ref, done)

    def emit(at, _):
        mass_ref[at] = msort[order_ref[at]]
        return 0
    lax.fori_loop(0, n, emit, 0)

    def mass_copy(r, sender):
        to = lax.rem(s + r, n)
        return remote(mass_ref.at[to], mrecv.at[s], m_send.at[r], m_recv.at[s], (to, b))

    def mass_start(r, _):
        mass_copy(r, s).start()
        return 0
    lax.fori_loop(1, n, mass_start, 0)
    mrecv[s] = mass_ref[s]

    def f_wait(r, _):
        f_copy(all_others(r), all_others(r)).wait_recv()
        f_copy(all_others(r), c).wait_send()
        return 0
    lax.fori_loop(1, chips, f_wait, 0)
    for k in range(tokens // rows):
        ft[:, k * rows:(k + 1) * rows] = f_ref[k].T

    def mass_wait(r, _):
        frm = lax.rem(s + n - r, n)
        got = remote(mass_ref.at[frm], mrecv.at[frm], m_send.at[r], m_recv.at[frm], (frm, b))
        got.wait_recv()
        return 0
    lax.fori_loop(1, n, mass_wait, 0)

    heads = lab.shape[0]
    per = n // heads
    for g in range(heads):
        total = mrecv[per * g]
        for i in range(1, per):
            total = total + mrecv[per * g + i]
        lab[g:g + 1, :] = jnp.log1p(total)
    position = order_ref[s] * rows + lax.broadcasted_iota(jnp.int32, (1, rows), 1)
    live = jnp.where(position < limit_ref[...], 1.0, 0.0)
    resid_t = ((pred_ref[...] - lab[...]) * live * norm).astype(jnp.bfloat16)
    resid = resid_t.astype(jnp.float32).T.astype(jnp.bfloat16)
    back = jnp.dot(resid, w2t_ref[...], preferred_element_type=jnp.float32)
    delta = (back * slope_ref[...]).astype(jnp.bfloat16)
    here = pl.ds(pl.multiple_of(c * rows, rows), rows)
    for j in range(chunks):
        dl[j][here, :] = delta[:, begin[j]:begin[j + 1]]

    wide = rows // 2
    slot = {}

    def number(*key):
        return slot.setdefault(key, len(slot))

    def spot(half_id, a, e):
        return (a * nz + e) if half_id == 0 else (e * nz + a)

    def ring(v, d, size):
        return lax.rem(v + (d + size), size)

    def coords(half_id):
        return (y, z, ny, nz) if half_id == 0 else (z, y, nz, ny)

    def piece(j, block, half_id, quarter):
        r0 = half_id * wide + (quarter * (wide // 2) if quarter is not None else 0)
        size = wide // 2 if quarter is not None else wide
        return dl[j].at[pl.ds(pl.multiple_of(block * rows + r0, wide // 2), size), :]

    def neighbour(half_id, which, d):
        along_y = (half_id == 0) == (which == 0)
        to_y = ring(y, d, ny) if along_y else y
        to_z = z if along_y else ring(z, d, nz)
        return ((to_y * nz + to_z) * 2 + core, b)

    started = []

    def copy(j, half_id, which, da, de, quarter, d):
        a, e, na, ne = coords(half_id)
        block = spot(half_id, ring(a, da, na), ring(e, de, ne))
        ref = piece(j, block, half_id, quarter)
        m = number(j, half_id, which, da, de, quarter, d)
        return remote(ref, ref, g_send.at[m], g_recv.at[m], neighbour(half_id, which, d))

    def send(j, half_id, which, da, de, quarter, d):
        one = copy(j, half_id, which, da, de, quarter, d)
        one.start()
        started.append(one)

    def receive(j, half_id, which, da, de, quarter, d):
        a, e, na, ne = coords(half_id)
        back_a, back_e = (da - d, de) if which == 0 else (da, de - d)
        block = spot(half_id, ring(a, back_a, na), ring(e, back_e, ne))
        ref = piece(j, block, half_id, quarter)
        m = number(j, half_id, which, da, de, quarter, d)
        remote(ref, ref, g_send.at[m], g_recv.at[m], neighbour(half_id, which, -d)).wait_recv()

    def second(j, h, da):
        for d in (1, -1):
            send(j, h, 1, da, 0, None, d)

    def second_pass_on(j, h, da):
        receive(j, h, 1, da, 0, None, 1)
        send(j, h, 1, da, -1, 0, 1)
        receive(j, h, 1, da, 0, None, -1)
        send(j, h, 1, da, 1, 1, -1)

    def second_end(j, h, da):
        receive(j, h, 1, da, -1, 0, 1)
        receive(j, h, 1, da, 1, 1, -1)

    def stage0(j):
        for h in (0, 1):
            for d in (1, -1):
                send(j, h, 0, 0, 0, None, d)
        for h in (0, 1):
            second(j, h, 0)

    def stage1(j):
        for h in (0, 1):
            receive(j, h, 0, 0, 0, None, 1)
            send(j, h, 0, -1, 0, 0, 1)
            second(j, h, -1)
            receive(j, h, 0, 0, 0, None, -1)
            send(j, h, 0, 1, 0, 1, -1)
            second(j, h, 1)

    def stage2(j):
        for h in (0, 1):
            second_pass_on(j, h, 0)
        for h in (0, 1):
            receive(j, h, 0, -1, 0, 0, 1)
            receive(j, h, 0, 1, 0, 1, -1)
            second(j, h, 2)

    def stage3(j):
        for da in (-1, 1):
            for h in (0, 1):
                second_pass_on(j, h, da)

    def stage4(j):
        for h in (0, 1):
            second_pass_on(j, h, 2)

    def stage5(j):
        for da in (0, -1, 1, 2):
            for h in (0, 1):
                second_end(j, h, da)

    def multiply(j):
        part[j][...] = jnp.dot(ft[...], dl[j][...], preferred_element_type=jnp.float32)

    def pair_copy(j, of):
        ref = part[j].at[pl.ds(pl.multiple_of((1 - of) * half, half), half), :]
        return remote(ref, pair[j], p_send.at[j], p_recv.at[j], partner)

    def pair_start(j):
        one = pair_copy(j, core)
        one.start()
        started.append(one)

    def x_copy(j, r):
        to = lax.rem(b + r, nb)
        ref = pair[j].at[pl.ds(pl.multiple_of(to * own_rows, own_rows), own_rows), :]
        return remote(ref, xrecv[j].at[r - 1], x_send.at[j, r - 1], x_recv.at[j, r - 1], (s, to))

    def x_start(j):
        pair_copy(j, core).wait_recv()
        pair[j][...] = pair[j][...] + part[j][pl.ds(pl.multiple_of(core * half, half), half), :]
        for r in (2, 1, 3)[: nb - 1]:
            one = x_copy(j, r)
            one.start()
            started.append(one)

    def x_end(j):
        for r in range(1, nb):
            x_copy(j, r).wait_recv()
        own = pair[j][pl.ds(pl.multiple_of(b * own_rows, own_rows), own_rows), :]
        for r in range(1, nb):
            own = own + xrecv[j][r - 1]
        out_ref[:own_rows, begin[j]:begin[j + 1]] = own

    def small_start0():
        sw = sm.shape[2]
        out_term = jnp.dot(resid_t, act_ref[...], preferred_element_type=jnp.float32)
        sums = jnp.sum(delta.astype(jnp.float32), axis=0, keepdims=True)
        bias = jnp.sum(resid.astype(jnp.float32), axis=0, keepdims=True)
        lanes = 128
        cols = [out_term[:, k * lanes:(k + 1) * lanes] for k in range(hidden // lanes)]
        cols.append(jnp.concatenate([sums[:, k * lanes:(k + 1) * lanes] for k in range(hidden // lanes)], axis=0))
        cols.append(jnp.zeros((heads, lanes), jnp.float32))
        each = sw // lanes
        for k, value in enumerate(cols):
            sm[k // each, :, (k % each) * lanes:(k % each + 1) * lanes] = value
        at = (len(cols) - 1) % each * lanes
        sm[1, 0:1, at:at + heads] = bias
        one = remote(sm.at[1 - core], smr, s_send.at[0], s_recv.at[0], partner)
        one.start()
        started.append(one)

    def small_hop(level, value, buf, at, size, target):
        buf[at] = value
        for r in range(1, size):
            one = remote(buf.at[at], buf.at[at], s_send.at[level * 3 + r], s_recv.at[level * 3 + r], target(r))
            one.start()
            started.append(one)

    def small_sum(level, buf, at, size, target):
        for r in range(1, size):
            frm = lax.rem(at + size - r, size)
            remote(buf.at[frm], buf.at[frm], s_send.at[level * 3 + r], s_recv.at[level * 3 + r], target(r)).wait_recv()
        total = buf[0]
        for k in range(1, size):
            total = total + buf[k]
        return total

    to_z = lambda r: ((y * nz + lax.rem(z + r, nz)) * 2 + core, b)
    to_y = lambda r: ((lax.rem(y + r, ny) * nz + z) * 2 + core, b)
    to_x = lambda r: (s, lax.rem(b + r, nb))

    def small1():
        remote(sm.at[1 - core], smr, s_send.at[0], s_recv.at[0], partner).wait_recv()
        small_hop(0, sm[core] + smr[...], zs, z, nz, to_z)

    def small2():
        small_hop(1, small_sum(0, zs, z, nz, to_z), ys, y, ny, to_y)

    def small3():
        small_hop(2, small_sum(1, ys, y, ny, to_y), xs, b, nb, to_x)

    def small4():
        sm[core] = small_sum(2, xs, b, nb, to_x)
        one = remote(sm.at[core], small.at[core], s_send.at[10], s_recv.at[10], partner)
        one.start()
        started.append(one)
        small[core] = sm[core]

    def small5():
        remote(sm.at[1 - core], small.at[1 - core], s_send.at[10], s_recv.at[10], partner).wait_recv()
        sw = small.shape[2]
        out_ref[own_rows:own_rows + heads, :sw] = small[0]
        out_ref[own_rows:own_rows + heads, sw:] = small[1, :, :hidden - sw]
        base = own_rows + heads
        lanes = 128
        for k in range(hidden // lanes):
            out_ref[base:base + 1, k * lanes:(k + 1) * lanes] = small[1, k:k + 1, hidden - sw:hidden - sw + lanes]
        out_ref[base + 1:base + 2, :lanes] = small[1, 0:1, hidden - sw + lanes:hidden - sw + 2 * lanes]

    stage0(0)
    stage0(1)
    small_start0()
    stage1(0)
    stage2(0)
    stage1(1)
    small1()
    stage3(0)
    stage2(1)
    stage4(0)
    small2()
    stage3(1)
    stage5(0)
    multiply(0)
    pair_start(0)
    stage4(1)
    small3()
    x_start(0)
    stage5(1)
    multiply(1)
    pair_start(1)
    small4()
    x_start(1)
    x_end(0)
    small5()
    x_end(1)

    for one in started:
        one.wait_send()

    def mass_drain(r, _):
        mass_copy(r, s).wait_send()
        return 0
    lax.fori_loop(1, n, mass_drain, 0)


def whole(dims, norm, order, bias, limit, q, k, v, w_in, b_in, w2t, tq=512, sub=128, widths=(512, 512), slots=3, deep=512):
    ny, nz, nb = dims
    rows, hidden = q.shape[0], w_in.shape[1]
    heads = w2t.shape[0]
    size = k.shape[1] // heads
    chips = ny * nz
    n = 2 * chips
    tokens = chips * rows
    columns = w_in.shape[0]
    feats = columns // chips
    half = feats // 2
    chunks = len(widths)
    sw = (hidden + 256) // 2
    vm, dma = pltpu.VMEM, pltpu.SemaphoreType.DMA
    block = lambda space: pl.BlockSpec(memory_space=space)
    f32, bf16 = jnp.float32, jnp.bfloat16
    return pl.pallas_call(
        functools.partial(whole_body, dims, norm, q.shape[1] // k.shape[1], tq, sub),
        out_shape=jax.ShapeDtypeStruct((half // nb + 16, hidden), f32),
        in_specs=[block(pltpu.SMEM)] * 2 + [block(vm)] + [block(pltpu.HBM)] * 4 + [block(vm)] * 2,
        out_specs=block(vm),
        scratch_shapes=[
            vm((rows, columns), bf16),
            vm((n, rows, size), bf16),
            vm((n, rows, size), bf16),
            vm((chips, rows, size), bf16),
            vm((slots, deep, hidden), bf16),
            vm((rows, hidden), f32),
            vm((heads, rows), f32),
            vm((rows, hidden), f32),
            vm((rows, hidden), bf16),
            pltpu.SMEM((n,), jnp.int32),
            vm((n * rows, size), bf16),
            vm((n * rows, size), bf16),
            tuple(vm((n * rows, tq), f32) for _ in range(3)),
            vm((n, rows, 128), f32),
            vm((n, 1, rows), f32),
            vm((n, 1, rows), f32),
            vm((chips, rows, feats), bf16),
            vm((n, 1, rows), f32),
            vm((heads, rows), f32),
            tuple(vm((tokens, w), bf16) for w in widths),
            vm((feats, tokens), bf16),
            tuple(vm((feats, w), f32) for w in widths),
            tuple(vm((half, w), f32) for w in widths),
            tuple(vm((nb - 1, half // nb, w), f32) for w in widths),
            vm((2, heads, sw), f32),
            vm((2, heads, sw), f32),
            vm((heads, sw), f32),
            vm((nz, heads, sw), f32),
            vm((ny, heads, sw), f32),
            vm((nb, heads, sw), f32),
            dma((slots,)), dma((3,)),
            dma((3, chips)), dma((3, chips)),
            dma((2, chips)), dma((2, chips)),
            dma((chips,)), dma((chips,)),
            dma((n,)), dma((n,)),
            dma((chunks * 40,)), dma((chunks * 40,)),
            dma((chunks,)), dma((chunks,)),
            dma((chunks, nb - 1)), dma((chunks, nb - 1)),
            dma((12,)), dma((12,)),
        ],
        compiler_params=pltpu.CompilerParams(collective_id=1, has_side_effects=True, vmem_limit_bytes=60 * 2**20),
        name="whole",
    )(order, bias, limit, q, k, v, w_in, b_in, w2t)


def apart_body(own, heads, out_ref, grad_ref, ow_ref, gb_ref, bias_ref):
    grad_ref[...] = out_ref[:own]
    ow_ref[...] = out_ref[own:own + heads]
    gb_ref[...] = out_ref[own + heads:own + heads + 1]
    bias_ref[...] = out_ref[own + heads + 1:own + heads + 2, :heads]


def apart(own, heads, out):
    hidden = out.shape[1]
    shapes = ((own, hidden), (heads, hidden), (1, hidden), (1, heads))
    return pl.pallas_call(
        functools.partial(apart_body, own, heads),
        out_shape=tuple(jax.ShapeDtypeStruct(one, jnp.float32) for one in shapes),
        in_specs=[pl.BlockSpec(memory_space=pltpu.VMEM)],
        out_specs=[pl.BlockSpec(memory_space=pltpu.VMEM)] * 4,
        name="apart",
    )(out)


def on_device(dims, queries, keys, values, lengths, block_pos, w_in, b_in, output_weight, output_bias):
    hidden, heads = output_weight.shape
    total = lax.axis_size("seq") * queries.shape[1]
    norm = 1.0 / math.sqrt(lax.axis_size("batch") * total)
    out = whole(
        dims, norm, block_pos[0], output_bias, lengths[None, :], queries[0], keys[0], values[0], w_in, b_in[None, :], output_weight.T
    )
    own = out.shape[0] - 16
    grad, ow, gb, bias = apart(own, heads, out)
    return (grad, gb.reshape(hidden), ow.T, bias.reshape(heads))


def solution(mesh):
    nb = mesh.shape["batch"]
    ny = nz = math.isqrt(mesh.shape["seq"] // 2)
    return jax.shard_map(
        functools.partial(on_device, (ny, nz, nb)),
        mesh=mesh,
        in_specs=(
            P("batch", "seq", None),
            P("batch", "seq", None),
            P("batch", "seq", None),
            P("batch"),
            P("batch", None),
            P(),
            P(),
            P(),
            P(),
        ),
        out_specs=(P(("seq", "batch"), None), P(), P(), P()),
        check_vma=False,
    )
```

```python
import functools
import math

import jax
import jax.numpy as jnp
from jax import lax
from jax.experimental import pallas as pl
from jax.experimental.pallas import tpu as pltpu
from jax.sharding import PartitionSpec as P

NEG = -1e30
MESH = pl.DeviceIdType.MESH


def remote(src, dst, send_sem, recv_sem, device):
    return pltpu.make_async_remote_copy(
        src_ref=src, dst_ref=dst, send_sem=send_sem, recv_sem=recv_sem, device_id=device, device_id_type=MESH
    )


def attn_core(tq, sub, total, scale2, limit, qs, ks, bufs, acc_ref, done=None):
    lanes = 128
    groups = tq // lanes
    nt = total // tq
    eights = lambda x: x.reshape(x.shape[0] // 8, 8, tq)

    def at(j, n=tq):
        return pl.ds(pl.multiple_of(j * n, n), n)

    def scores(i, j, mx, masked):
        s = lax.dot_general(ks[at(j), :], qs[at(i), :], (((1,), (1,)), ((), ())), preferred_element_type=jnp.float32)
        if masked:
            kp = lax.broadcasted_iota(jnp.int32, (tq, tq), 0)
            qp = lax.broadcasted_iota(jnp.int32, (tq, tq), 1)
            s = jnp.where(kp <= qp, s, NEG)
        bufs[i % 3][at(j), :] = s
        return jnp.maximum(mx, jnp.max(eights(s), axis=0))

    def weights(i, j, l, top):
        buf = bufs[i % 3]
        for u in range(tq // sub):
            here = pl.ds(pl.multiple_of(j * tq + u * sub, sub), sub)
            w = jnp.exp2((eights(buf[here, :]) - top[None]) * scale2)
            buf[here, :] = w.reshape(sub, tq)
            l = l + jnp.sum(w, axis=0)
        return l

    def shares(i, j, rec):
        buf = bufs[i % 3]
        for u in range(tq // sub):
            here = pl.ds(pl.multiple_of(j * tq + u * sub, sub), sub)
            w = (eights(buf[here, :]) * rec[None]).reshape(sub, tq)
            tot = w[:, :lanes]
            for g in range(1, groups):
                tot = tot + w[:, g * lanes:(g + 1) * lanes]
            acc_ref[j * (tq // sub) + u] += tot

    def spread_top(mx):
        return jnp.broadcast_to(jnp.max(mx, axis=0, keepdims=True), (8, tq))

    def spread_rec(i, l):
        pos = i * tq + lax.broadcasted_iota(jnp.int32, (1, tq), 1)
        rec = jnp.where(pos < limit, 1.0 / jnp.sum(l, axis=0, keepdims=True), 0.0)
        return jnp.broadcast_to(rec, (8, tq))

    top = rec = None
    for i in range(nt - 1, -3, -1):
        first, second, third = i >= 0, 0 <= i + 1 < nt, i + 2 < nt

        def each(j, carry, i=i, first=first, second=second, third=third, top=top, rec=rec):
            mx, l = carry
            if first:
                mx = scores(i, j, mx, False)
            if second:
                l = weights(i + 1, j, l, top)
            if third:
                shares(i + 2, j, rec)
            return mx, l

        mx = jnp.full((8, tq), NEG, jnp.float32)
        l = jnp.zeros((8, tq), jnp.float32)
        if i > 0:
            mx, l = lax.fori_loop(0, i, each, (mx, l))
        if first:
            mx = scores(i, i, mx, True)
        for d in (0, 1, 2):
            if second and d < 2 and i + d >= 0:
                l = weights(i + 1, i + d, l, top)
            if third and i + d >= 0:
                shares(i + 2, i + d, rec)
        if third and done is not None:
            done(i + 2)
        top, rec = spread_top(mx), spread_rec(i + 1, l)


def whole_body(dims, norm, per, tq, sub, order_ref, bias_ref, limit_ref, q_hbm, k_hbm, v_hbm, w_hbm, bin_ref, w2t_ref, out_ref,
               feat, qa, ka, stage, wbuf, pre, pred_ref, slope_ref, act_ref, inv, qs, ks, bufs, acc_ref, msort, mass_ref, f_ref,
               mrecv, lab, dl, ft, part, pair, xrecv, sm, small, smr, zs, ys, xs,
               w_sem, in_sem, i_send, i_recv, d_send, d_recv, f_send, f_recv,
               m_send, m_recv, g_send, g_recv, p_send, p_recv, x_send, x_recv, s_send, s_recv):
    ny, nz, nb = dims
    chips = ny * nz
    n = chips * 2
    s, b = lax.axis_index("seq"), lax.axis_index("batch")
    core, c = lax.rem(s, 2), s // 2
    z, y = lax.rem(c, nz), c // nz
    rows, hidden = slope_ref.shape
    head = ka.shape[2]
    q_cols, k_cols = q_hbm.shape[1], k_hbm.shape[1]
    slots, deep = wbuf.shape[:2]
    steps = w_hbm.shape[0] // deep
    chunks, tokens = len(dl), dl[0].shape[0]
    feats = part[0].shape[0]
    begin = [sum(d.shape[1] for d in dl[:j]) for j in range(chunks + 1)]
    half = feats // 2
    own_rows = half // nb
    partner = (s + 1 - 2 * core, b)

    barrier = pltpu.get_barrier_semaphore()

    def greet(r, _):
        pl.semaphore_signal(barrier, inc=1, device_id=(lax.rem(s + r, n), b), device_id_type=MESH)
        return 0
    lax.fori_loop(1, n, greet, 0)
    for r in range(1, nb):
        pl.semaphore_signal(barrier, inc=1, device_id=(s, lax.rem(b + r, nb)), device_id_type=MESH)

    inputs = []
    at = 0
    for i, ref in enumerate((q_hbm, k_hbm, v_hbm)):
        inputs.append(pltpu.make_async_copy(ref, feat.at[:, at:at + ref.shape[1]], in_sem.at[i]))
        at += ref.shape[1]
    for one in inputs:
        one.start()

    def w_copy(i):
        at = lax.rem(i, slots)
        return pltpu.make_async_copy(w_hbm.at[pl.ds(pl.multiple_of(i * deep, deep), deep), :], wbuf.at[at], w_sem.at[at])

    for i in range(slots):
        w_copy(i).start()
    acc_ref[...] = jnp.zeros_like(acc_ref)
    pre[...] = jnp.broadcast_to(bin_ref[...], pre.shape)
    for one in inputs:
        one.wait()

    hops = lambda d: -min(d[0], ny - d[0]) - min(d[1], nz - d[1])
    away = sorted(((dy, dz) for dy in range(ny) for dz in range(nz) if dy or dz), key=hops)

    def chip_at(d, sign):
        dy, dz = d
        return lax.rem(y + sign * dy + ny, ny) * nz + lax.rem(z + sign * dz + nz, nz)

    def columns(i):
        return pl.ds(pl.multiple_of(i * head, head), head)

    def parts(to):
        return (columns(2 * to + core), columns(2 * to + 1 - core), columns(q_cols // head + (2 * to) // per))

    own_q, other_q, own_k = parts(c)
    qa[s] = feat[:, own_q]
    ka[s] = feat[:, own_k]
    mine = pl.ds(pl.multiple_of(c * feats, feats), feats)
    f_ref[c] = feat[:, mine]
    pl.semaphore_wait(barrier, n - 1 + nb - 1)

    def arrivals(frm):
        return (qa.at[2 * frm + core], stage.at[frm], ka.at[2 * frm + core])

    def across(i, to, frm):
        return remote(feat.at[:, parts(to)[i]], arrivals(frm)[i], i_send.at[i, to], i_recv.at[i, frm], (2 * to + core, b))

    for some in ((1,), (2,), (0,)):
        for d in away:
            for i in some:
                across(i, chip_at(d, 1), c).start()

    def over(i, src, at, whose):
        dst = (qa.at[2 * at + whose], ka.at[2 * at + whose])[i]
        return remote(src, dst, d_send.at[i, at], d_recv.at[i, at], partner)

    over(0, feat.at[:, other_q], c, core).start()
    over(1, feat.at[:, own_k], c, core).start()

    def find(at, _):
        stored = jnp.int32(0)
        for k in range(1, n):
            stored = stored + k * jnp.maximum(1 - jnp.abs(order_ref[k] - at), 0)
        inv[at] = jnp.minimum(stored, n - 1)
        return 0
    lax.fori_loop(0, n, find, 0)

    def step(i, _):
        w_copy(i).wait()
        x = feat[:, pl.ds(pl.multiple_of(i * deep, deep), deep)]
        pre[...] += jnp.dot(x, wbuf[lax.rem(i, slots)], preferred_element_type=jnp.float32)

        @pl.when(i + slots < steps)
        def _():
            w_copy(i + slots).start()
        return 0
    lax.fori_loop(0, steps, step, 0)
    p = pre[...]
    sig = jax.nn.sigmoid(p)
    act = (p * sig).astype(jnp.bfloat16)
    act_ref[...] = act
    slope_ref[...] = sig * (1.0 + p * (1.0 - sig))
    out = lax.dot_general(w2t_ref[...], act, (((1,), (1,)), ((), ())), preferred_element_type=jnp.float32)
    for g in range(pred_ref.shape[0]):
        pred_ref[g:g + 1, :] = out[g:g + 1, :] + bias_ref[g]

    for d in away:
        frm = chip_at(d, -1)
        across(1, frm, frm).wait_recv()
        over(0, stage.at[frm], frm, core).start()
        across(2, frm, frm).wait_recv()
        over(1, ka.at[2 * frm + core], frm, core).start()

    def all_others(r):
        return lax.rem(c + r, chips)

    def settle(r, _):
        across(0, all_others(r), all_others(r)).wait_recv()
        for i in range(3):
            across(i, all_others(r), c).wait_send()
        return 0
    lax.fori_loop(1, chips, settle, 0)

    def settle_over(at, _):
        over(0, stage.at[at], at, 1 - core).wait()
        over(1, ka.at[2 * at + core], at, 1 - core).wait()
        return 0
    lax.fori_loop(0, chips, settle_over, 0)

    def f_copy(to, frm):
        cut = pl.ds(pl.multiple_of(to * feats, feats), feats)
        return remote(feat.at[:, cut], f_ref.at[frm], f_send.at[to], f_recv.at[frm], (2 * to + core, b))

    for d in away:
        f_copy(chip_at(d, 1), c).start()

    def sort(at, _):
        here = pl.ds(pl.multiple_of(at * rows, rows), rows)
        stored = inv[at]
        qs[here, :] = qa[stored]
        ks[here, :] = ka[stored]
        return 0
    lax.fori_loop(0, n, sort, 0)

    scale2 = math.log2(math.e) / math.sqrt(head)

    def done(i):
        for u in range(i * (tq // rows), (i + 1) * (tq // rows)):
            msort[u] = jnp.sum(acc_ref[u].T, axis=0, keepdims=True)

    attn_core(tq, sub, n * rows, scale2, limit_ref[...], qs, ks, bufs, acc_ref, done)

    def emit(at, _):
        mass_ref[at] = msort[order_ref[at]]
        return 0
    lax.fori_loop(0, n, emit, 0)

    def mass_copy(r, sender):
        to = lax.rem(s + r, n)
        return remote(mass_ref.at[to], mrecv.at[s], m_send.at[r], m_recv.at[s], (to, b))

    def mass_start(r, _):
        mass_copy(r, s).start()
        return 0
    lax.fori_loop(1, n, mass_start, 0)
    mrecv[s] = mass_ref[s]

    def f_wait(r, _):
        f_copy(all_others(r), all_others(r)).wait_recv()
        f_copy(all_others(r), c).wait_send()
        return 0
    lax.fori_loop(1, chips, f_wait, 0)
    for k in range(tokens // rows):
        ft[:, k * rows:(k + 1) * rows] = f_ref[k].T

    def mass_wait(r, _):
        frm = lax.rem(s + n - r, n)
        got = remote(mass_ref.at[frm], mrecv.at[frm], m_send.at[r], m_recv.at[frm], (frm, b))
        got.wait_recv()
        return 0
    lax.fori_loop(1, n, mass_wait, 0)

    heads = lab.shape[0]
    per = n // heads
    for g in range(heads):
        total = mrecv[per * g]
        for i in range(1, per):
            total = total + mrecv[per * g + i]
        lab[g:g + 1, :] = jnp.log1p(total)
    position = order_ref[s] * rows + lax.broadcasted_iota(jnp.int32, (1, rows), 1)
    live = jnp.where(position < limit_ref[...], 1.0, 0.0)
    resid_t = ((pred_ref[...] - lab[...]) * live * norm).astype(jnp.bfloat16)
    resid = resid_t.astype(jnp.float32).T.astype(jnp.bfloat16)
    here = pl.ds(pl.multiple_of(c * rows, rows), rows)

    def make(j):
        cut = slice(begin[j], begin[j + 1])
        back = jnp.dot(resid, w2t_ref[:, cut], preferred_element_type=jnp.float32)
        dl[j][here, :] = (back * slope_ref[:, cut]).astype(jnp.bfloat16)

    wide = rows // 2
    slot = {}

    def number(*key):
        return slot.setdefault(key, len(slot))

    def spot(half_id, a, e):
        return (a * nz + e) if half_id == 0 else (e * nz + a)

    def ring(v, d, size):
        return lax.rem(v + (d + size), size)

    def coords(half_id):
        return (y, z, ny, nz) if half_id == 0 else (z, y, nz, ny)

    def piece(j, block, half_id, quarter):
        r0 = half_id * wide + (quarter * (wide // 2) if quarter is not None else 0)
        size = wide // 2 if quarter is not None else wide
        return dl[j].at[pl.ds(pl.multiple_of(block * rows + r0, wide // 2), size), :]

    def neighbour(half_id, which, d):
        along_y = (half_id == 0) == (which == 0)
        to_y = ring(y, d, ny) if along_y else y
        to_z = z if along_y else ring(z, d, nz)
        return ((to_y * nz + to_z) * 2 + core, b)

    started = []

    def copy(j, half_id, which, da, de, quarter, d):
        a, e, na, ne = coords(half_id)
        block = spot(half_id, ring(a, da, na), ring(e, de, ne))
        ref = piece(j, block, half_id, quarter)
        m = number(j, half_id, which, da, de, quarter, d)
        return remote(ref, ref, g_send.at[m], g_recv.at[m], neighbour(half_id, which, d))

    def send(j, half_id, which, da, de, quarter, d):
        one = copy(j, half_id, which, da, de, quarter, d)
        one.start()
        started.append(one)

    def receive(j, half_id, which, da, de, quarter, d):
        a, e, na, ne = coords(half_id)
        back_a, back_e = (da - d, de) if which == 0 else (da, de - d)
        block = spot(half_id, ring(a, back_a, na), ring(e, back_e, ne))
        ref = piece(j, block, half_id, quarter)
        m = number(j, half_id, which, da, de, quarter, d)
        remote(ref, ref, g_send.at[m], g_recv.at[m], neighbour(half_id, which, -d)).wait_recv()

    def second(j, h, da):
        for d in (1, -1):
            send(j, h, 1, da, 0, None, d)

    def second_pass_on(j, h, da):
        receive(j, h, 1, da, 0, None, 1)
        send(j, h, 1, da, -1, 0, 1)
        receive(j, h, 1, da, 0, None, -1)
        send(j, h, 1, da, 1, 1, -1)

    def second_end(j, h, da):
        receive(j, h, 1, da, -1, 0, 1)
        receive(j, h, 1, da, 1, 1, -1)

    def stage0(j):
        for h in (0, 1):
            for d in (1, -1):
                send(j, h, 0, 0, 0, None, d)
        for h in (0, 1):
            second(j, h, 0)

    def stage1(j):
        for h in (0, 1):
            receive(j, h, 0, 0, 0, None, 1)
            send(j, h, 0, -1, 0, 0, 1)
            second(j, h, -1)
            receive(j, h, 0, 0, 0, None, -1)
            send(j, h, 0, 1, 0, 1, -1)
            second(j, h, 1)

    def stage2(j):
        for h in (0, 1):
            second_pass_on(j, h, 0)
        for h in (0, 1):
            receive(j, h, 0, -1, 0, 0, 1)
            receive(j, h, 0, 1, 0, 1, -1)
            second(j, h, 2)

    def stage3(j):
        for da in (-1, 1):
            for h in (0, 1):
                second_pass_on(j, h, da)

    def stage4(j):
        for h in (0, 1):
            second_pass_on(j, h, 2)

    def stage5(j):
        for da in (0, -1, 1, 2):
            for h in (0, 1):
                second_end(j, h, da)

    def multiply(j):
        part[j][...] = jnp.dot(ft[...], dl[j][...], preferred_element_type=jnp.float32)

    def pair_copy(j, of):
        ref = part[j].at[pl.ds(pl.multiple_of((1 - of) * half, half), half), :]
        return remote(ref, pair[j], p_send.at[j], p_recv.at[j], partner)

    def pair_start(j):
        one = pair_copy(j, core)
        one.start()
        started.append(one)

    def x_copy(j, r):
        to = lax.rem(b + r, nb)
        ref = pair[j].at[pl.ds(pl.multiple_of(to * own_rows, own_rows), own_rows), :]
        return remote(ref, xrecv[j].at[r - 1], x_send.at[j, r - 1], x_recv.at[j, r - 1], (s, to))

    def x_start(j):
        pair_copy(j, core).wait_recv()
        pair[j][...] = pair[j][...] + part[j][pl.ds(pl.multiple_of(core * half, half), half), :]
        for r in (2, 1, 3)[: nb - 1]:
            one = x_copy(j, r)
            one.start()
            started.append(one)

    def x_end(j):
        for r in range(1, nb):
            x_copy(j, r).wait_recv()
        own = pair[j][pl.ds(pl.multiple_of(b * own_rows, own_rows), own_rows), :]
        for r in range(1, nb):
            own = own + xrecv[j][r - 1]
        out_ref[:own_rows, begin[j]:begin[j + 1]] = own

    def small_start0():
        sw = sm.shape[2]
        out_term = jnp.dot(resid_t, act_ref[...], preferred_element_type=jnp.float32)
        sums = jnp.concatenate(
            [jnp.sum(d[here, :].astype(jnp.float32), axis=0, keepdims=True) for d in dl], axis=1
        )
        bias = jnp.sum(resid.astype(jnp.float32), axis=0, keepdims=True)
        lanes = 128
        cols = [out_term[:, k * lanes:(k + 1) * lanes] for k in range(hidden // lanes)]
        cols.append(jnp.concatenate([sums[:, k * lanes:(k + 1) * lanes] for k in range(hidden // lanes)], axis=0))
        cols.append(jnp.zeros((heads, lanes), jnp.float32))
        each = sw // lanes
        for k, value in enumerate(cols):
            sm[k // each, :, (k % each) * lanes:(k % each + 1) * lanes] = value
        at = (len(cols) - 1) % each * lanes
        sm[1, 0:1, at:at + heads] = bias
        one = remote(sm.at[1 - core], smr, s_send.at[0], s_recv.at[0], partner)
        one.start()
        started.append(one)

    def small_hop(level, value, buf, at, size, target):
        buf[at] = value
        for r in range(1, size):
            one = remote(buf.at[at], buf.at[at], s_send.at[level * 3 + r], s_recv.at[level * 3 + r], target(r))
            one.start()
            started.append(one)

    def small_sum(level, buf, at, size, target):
        for r in range(1, size):
            frm = lax.rem(at + size - r, size)
            remote(buf.at[frm], buf.at[frm], s_send.at[level * 3 + r], s_recv.at[level * 3 + r], target(r)).wait_recv()
        total = buf[0]
        for k in range(1, size):
            total = total + buf[k]
        return total

    to_z = lambda r: ((y * nz + lax.rem(z + r, nz)) * 2 + core, b)
    to_y = lambda r: ((lax.rem(y + r, ny) * nz + z) * 2 + core, b)
    to_x = lambda r: (s, lax.rem(b + r, nb))

    def small1():
        remote(sm.at[1 - core], smr, s_send.at[0], s_recv.at[0], partner).wait_recv()
        small_hop(0, sm[core] + smr[...], zs, z, nz, to_z)

    def small2():
        small_hop(1, small_sum(0, zs, z, nz, to_z), ys, y, ny, to_y)

    def small3():
        small_hop(2, small_sum(1, ys, y, ny, to_y), xs, b, nb, to_x)

    def small4():
        sm[core] = small_sum(2, xs, b, nb, to_x)
        one = remote(sm.at[core], small.at[core], s_send.at[10], s_recv.at[10], partner)
        one.start()
        started.append(one)
        small[core] = sm[core]

    def small5():
        remote(sm.at[1 - core], small.at[1 - core], s_send.at[10], s_recv.at[10], partner).wait_recv()
        sw = small.shape[2]
        out_ref[own_rows:own_rows + heads, :sw] = small[0]
        out_ref[own_rows:own_rows + heads, sw:] = small[1, :, :hidden - sw]
        base = own_rows + heads
        lanes = 128
        for k in range(hidden // lanes):
            out_ref[base:base + 1, k * lanes:(k + 1) * lanes] = small[1, k:k + 1, hidden - sw:hidden - sw + lanes]
        out_ref[base + 1:base + 2, :lanes] = small[1, 0:1, hidden - sw + lanes:hidden - sw + 2 * lanes]

    make(0)
    stage0(0)
    make(1)
    stage0(1)
    small_start0()
    stage1(0)
    stage2(0)
    stage1(1)
    small1()
    stage3(0)
    stage2(1)
    stage4(0)
    small2()
    stage3(1)
    stage5(0)
    multiply(0)
    pair_start(0)
    stage4(1)
    small3()
    x_start(0)
    stage5(1)
    multiply(1)
    pair_start(1)
    small4()
    x_start(1)
    x_end(0)
    small5()
    x_end(1)

    for one in started:
        one.wait_send()

    def mass_drain(r, _):
        mass_copy(r, s).wait_send()
        return 0
    lax.fori_loop(1, n, mass_drain, 0)


def whole(dims, norm, order, bias, limit, q, k, v, w_in, b_in, w2t, tq=512, sub=128, widths=(512, 512), slots=3, deep=512):
    ny, nz, nb = dims
    rows, hidden = q.shape[0], w_in.shape[1]
    heads = w2t.shape[0]
    size = k.shape[1] // heads
    chips = ny * nz
    n = 2 * chips
    tokens = chips * rows
    columns = w_in.shape[0]
    feats = columns // chips
    half = feats // 2
    chunks = len(widths)
    sw = (hidden + 256) // 2
    vm, dma = pltpu.VMEM, pltpu.SemaphoreType.DMA
    block = lambda space: pl.BlockSpec(memory_space=space)
    f32, bf16 = jnp.float32, jnp.bfloat16
    return pl.pallas_call(
        functools.partial(whole_body, dims, norm, q.shape[1] // k.shape[1], tq, sub),
        out_shape=jax.ShapeDtypeStruct((half // nb + 16, hidden), f32),
        in_specs=[block(pltpu.SMEM)] * 2 + [block(vm)] + [block(pltpu.HBM)] * 4 + [block(vm)] * 2,
        out_specs=block(vm),
        scratch_shapes=[
            vm((rows, columns), bf16),
            vm((n, rows, size), bf16),
            vm((n, rows, size), bf16),
            vm((chips, rows, size), bf16),
            vm((slots, deep, hidden), bf16),
            vm((rows, hidden), f32),
            vm((heads, rows), f32),
            vm((rows, hidden), f32),
            vm((rows, hidden), bf16),
            pltpu.SMEM((n,), jnp.int32),
            vm((n * rows, size), bf16),
            vm((n * rows, size), bf16),
            tuple(vm((n * rows, tq), f32) for _ in range(3)),
            vm((n, rows, 128), f32),
            vm((n, 1, rows), f32),
            vm((n, 1, rows), f32),
            vm((chips, rows, feats), bf16),
            vm((n, 1, rows), f32),
            vm((heads, rows), f32),
            tuple(vm((tokens, w), bf16) for w in widths),
            vm((feats, tokens), bf16),
            tuple(vm((feats, w), f32) for w in widths),
            tuple(vm((half, w), f32) for w in widths),
            tuple(vm((nb - 1, half // nb, w), f32) for w in widths),
            vm((2, heads, sw), f32),
            vm((2, heads, sw), f32),
            vm((heads, sw), f32),
            vm((nz, heads, sw), f32),
            vm((ny, heads, sw), f32),
            vm((nb, heads, sw), f32),
            dma((slots,)), dma((3,)),
            dma((3, chips)), dma((3, chips)),
            dma((2, chips)), dma((2, chips)),
            dma((chips,)), dma((chips,)),
            dma((n,)), dma((n,)),
            dma((chunks * 40,)), dma((chunks * 40,)),
            dma((chunks,)), dma((chunks,)),
            dma((chunks, nb - 1)), dma((chunks, nb - 1)),
            dma((12,)), dma((12,)),
        ],
        compiler_params=pltpu.CompilerParams(collective_id=1, has_side_effects=True, vmem_limit_bytes=60 * 2**20),
        name="whole",
    )(order, bias, limit, q, k, v, w_in, b_in, w2t)


def apart_body(own, heads, out_ref, grad_ref, ow_ref, gb_ref, bias_ref):
    grad_ref[...] = out_ref[:own]
    ow_ref[...] = out_ref[own:own + heads]
    gb_ref[...] = out_ref[own + heads:own + heads + 1]
    bias_ref[...] = out_ref[own + heads + 1:own + heads + 2, :heads]


def apart(own, heads, out):
    hidden = out.shape[1]
    shapes = ((own, hidden), (heads, hidden), (1, hidden), (1, heads))
    return pl.pallas_call(
        functools.partial(apart_body, own, heads),
        out_shape=tuple(jax.ShapeDtypeStruct(one, jnp.float32) for one in shapes),
        in_specs=[pl.BlockSpec(memory_space=pltpu.VMEM)],
        out_specs=[pl.BlockSpec(memory_space=pltpu.VMEM)] * 4,
        name="apart",
    )(out)


def on_device(dims, queries, keys, values, lengths, block_pos, w_in, b_in, output_weight, output_bias):
    hidden, heads = output_weight.shape
    total = lax.axis_size("seq") * queries.shape[1]
    norm = 1.0 / math.sqrt(lax.axis_size("batch") * total)
    out = whole(
        dims, norm, block_pos[0], output_bias, lengths[None, :], queries[0], keys[0], values[0], w_in, b_in[None, :], output_weight.T
    )
    own = out.shape[0] - 16
    grad, ow, gb, bias = apart(own, heads, out)
    return (grad, gb.reshape(hidden), ow.T, bias.reshape(heads))


def solution(mesh):
    nb = mesh.shape["batch"]
    ny = nz = math.isqrt(mesh.shape["seq"] // 2)
    return jax.shard_map(
        functools.partial(on_device, (ny, nz, nb)),
        mesh=mesh,
        in_specs=(
            P("batch", "seq", None),
            P("batch", "seq", None),
            P("batch", "seq", None),
            P("batch"),
            P("batch", None),
            P(),
            P(),
            P(),
            P(),
        ),
        out_specs=(P(("seq", "batch"), None), P(), P(), P()),
        check_vma=False,
    )
```
